256 devices in a mesh: seq: 64 (over z_hi, x, y), heads: 4 (over z_lo, core).
Axes of the slice: x: 4, y: 4, z: 8 (z_hi: 4, z_lo: 2; z = z_hi * 2 + z_lo), core: 2. Of those that a mesh axis runs over, the one named last changes fastest.
Arguments:
- queries: bfloat16 [16384, 16, 128], P('seq', 'heads'), may hold values from -6 to 6
- key_vecs: bfloat16 [16384, 16, 128], P('seq', 'heads'), may hold values from -12 to 12
- values: bfloat16 [16384, 32, 128], P('seq', 'heads'), may hold values from -6 to 6
- strength: float32 [16384, 32], P('seq', 'heads'), may hold values from 0 to 1, as said below
- decay_rate: float32 [16384, 32], P('seq', 'heads'), may hold values from 0 to 0.15, as said below
- norm_gain: float32 [128], replicated, may hold values from 0.5 to 1.5
- w_out: bfloat16 [4096, 2048], P('heads'), may hold values from -0.09375 to 0.09375
Outputs:
- mixed: bfloat16 [16384, 2048], P(('seq', 'heads'))
The draws below stay inside these ranges and needn't reach their ends.
Inputs may be any that keep to these rules, and one draw needn't show every extreme that they name: Every write strength lies strictly between 0 and 1. `decay_rate`: every decay rate is positive.
All inputs are finite; a program needn't handle non-finite values.
Results may differ from the reference program's by a relative error of at most 0.0049.
Values sent between devices are 32-bit elements; how exact they have to be, the bound alone decides.
A program may use at most 192 MiB of HBM per device.

```python
import math
import jax
import jax.numpy as jnp
from jax import lax

D = 2048
DK = 128
DV = 128
HQK = 16
VALUE_HEADS = 32
BLOCK_TOKENS = 64
TOK_DEV = 256
SEQUENCE_TOKENS = 16384


def head_classes(key):
    head_order = jax.random.permutation(jax.random.fold_in(key, 11), VALUE_HEADS)
    fast_count = VALUE_HEADS // 2
    return head_order < fast_count


def logarithmic_uniform_draw(key, shape, low, high):
    return jnp.exp(jax.random.uniform(key, shape, jnp.float32, math.log(low), math.log(high)))


def draw_key_vecs(key, part):
    device_random_keys = jax.random.split(jax.random.fold_in(key, 41), 4)
    total_block_count = SEQUENCE_TOKENS // BLOCK_TOKENS
    base_noise = jnp.clip(jax.random.normal(device_random_keys[0], (SEQUENCE_TOKENS, HQK, DK), jnp.float32), -6.0, 6.0)
    shared = jnp.clip(jax.random.normal(device_random_keys[1], (HQK, DK), jnp.float32), -4.0, 4.0)
    block_signs = jnp.where(jax.random.bernoulli(device_random_keys[2], 0.5, (total_block_count, HQK)), 1.0, -1.0)
    block_weights = jax.random.uniform(device_random_keys[3], (total_block_count, HQK), jnp.float32, 0.8, 1.2)
    per_block = jnp.repeat(block_signs * block_weights, BLOCK_TOKENS, axis=0)
    return (base_noise + per_block[:, :, None] * shared[None, :, :]).astype(jnp.bfloat16)


def draw_strength(key, part):
    fast_heads = head_classes(key)
    device_random_keys = jax.random.split(jax.random.fold_in(key, 23), 6)
    total_block_count = SEQUENCE_TOKENS // BLOCK_TOKENS
    sudden_head_fraction = min(8.0 * BLOCK_TOKENS / SEQUENCE_TOKENS, 0.25)
    fast_level = logarithmic_uniform_draw(device_random_keys[0], (VALUE_HEADS,), 0.3, 0.9)
    gentle_decay_level = logarithmic_uniform_draw(device_random_keys[1], (VALUE_HEADS,), 0.1, 0.5) * (DK / SEQUENCE_TOKENS)
    rough_fast = jax.random.uniform(device_random_keys[2], (SEQUENCE_TOKENS, VALUE_HEADS), jnp.float32, 0.6, 1.1)
    noisy_gentle_decay = logarithmic_uniform_draw(device_random_keys[3], (SEQUENCE_TOKENS, VALUE_HEADS), 0.5, 2.0)
    sudden_decay_blocks = jax.random.bernoulli(device_random_keys[4], sudden_head_fraction, (total_block_count, VALUE_HEADS))
    sudden_decay_values = logarithmic_uniform_draw(device_random_keys[5], (SEQUENCE_TOKENS, VALUE_HEADS), 0.025, 0.048)
    sudden_decay_full = jnp.repeat(sudden_decay_blocks, BLOCK_TOKENS, axis=0)
    fast_vals = fast_level[None, :] * rough_fast
    gentle_decay_values = jnp.where(sudden_decay_full, sudden_decay_values, gentle_decay_level[None, :] * noisy_gentle_decay)
    return jnp.where(fast_heads[None, :], fast_vals, gentle_decay_values).astype(jnp.float32)


def draw_decay_rate(key, part):
    fast_heads = head_classes(key)
    device_random_keys = jax.random.split(jax.random.fold_in(key, 31), 4)
    fast_level = logarithmic_uniform_draw(device_random_keys[0], (VALUE_HEADS,), min(1.0 / TOK_DEV, 1.0 / 80.0), 1.0 / 40.0)
    gentle_decay_level = logarithmic_uniform_draw(device_random_keys[1], (VALUE_HEADS,), 0.1, 0.5) / SEQUENCE_TOKENS
    rough = logarithmic_uniform_draw(device_random_keys[2], (SEQUENCE_TOKENS, VALUE_HEADS), 0.5, 2.0)
    segment = logarithmic_uniform_draw(device_random_keys[3], (SEQUENCE_TOKENS // TOK_DEV, VALUE_HEADS), 0.5, 2.0)
    segment_full = jnp.repeat(segment, TOK_DEV, axis=0)
    head_level = jnp.where(fast_heads, fast_level, gentle_decay_level)
    return (head_level[None, :] * rough * segment_full).astype(jnp.float32)


def levels(stream_key, extent, cuts, smallest, largest):
    def one(axis_at, shards_of):
        draws = jax.random.uniform(jax.random.fold_in(jax.random.fold_in(stream_key, 6), axis_at), (shards_of,), jnp.float32, smallest / len(cuts), largest / len(cuts))
        return jnp.repeat(jnp.exp(draws), extent[axis_at] // shards_of).reshape((-1,) + (1,) * (len(extent) - axis_at - 1))

    loudness = one(*cuts[0])
    for cut in cuts[1:]:
        loudness = loudness * one(*cut)
    return loudness


def noise(rng, dims, width, bound, shards=(), kind=jnp.bfloat16):
    drawn = width * jax.random.normal(rng, dims, jnp.float32)
    if shards:
        drawn = drawn * levels(rng, dims, shards, -0.22, 0.18)
    return jnp.clip(drawn, -bound, bound).astype(kind)


def setup_inputs(seed: int = 0) -> dict:
    splits = jax.random.split(jax.random.key(seed), 8)
    return {
        "queries": noise(splits[0], (SEQUENCE_TOKENS, HQK, DK), 1.0, 6.0, ((0, 64), (1, 4))),
        "key_vecs": draw_key_vecs(jax.random.fold_in(splits[7], 71), 0),
        "values": noise(splits[2], (SEQUENCE_TOKENS, VALUE_HEADS, DV), 1.0, 6.0, ((0, 64), (1, 4))),
        "strength": draw_strength(jax.random.fold_in(splits[7], 71), 0),
        "decay_rate": draw_decay_rate(jax.random.fold_in(splits[7], 71), 0),
        "norm_gain": jnp.clip(1.0 + 0.1 * jax.random.normal(splits[5], (DV,), jnp.float32), 0.5, 1.5),
        "w_out": noise(splits[6], (VALUE_HEADS * DV, D), (VALUE_HEADS * DV) ** -0.5, 0.09375, ((0, 4),)),
    }


strict_precision = lax.Precision.HIGHEST
norm_eps = 1e-12
unit_eps = 1e-06

def unit_rows(matrix):
    matrix = matrix.astype(jnp.float32)
    return matrix / jnp.sqrt(lax.optimization_barrier(jnp.sum(matrix * matrix, axis=-1, keepdims=True)) + unit_eps)

def prepare(query_blk, key_blk, value_blk, strength_blk, decay_blk):
    group_size = value_blk.shape[1] // query_blk.shape[1]
    normalized_queries = jnp.repeat(jnp.transpose(unit_rows(query_blk), (1, 0, 2)), group_size, axis=0)
    keys_n = jnp.repeat(jnp.transpose(unit_rows(key_blk), (1, 0, 2)), group_size, axis=0)
    values_f = jnp.transpose(value_blk.astype(jnp.float32), (1, 0, 2))
    writes = jnp.transpose(strength_blk)
    decay_logarithm = -jnp.cumsum(jnp.transpose(decay_blk), axis=1)
    return (normalized_queries, keys_n, values_f, writes, decay_logarithm)

def block_parts(normalized_queries, keys_n, values_f, writes, decay_logarithm):
    key_width = keys_n.shape[2]
    length = keys_n.shape[1]
    row_ids = lax.broadcasted_iota(jnp.int32, (length, length), 0)
    col_ids = lax.broadcasted_iota(jnp.int32, (length, length), 1)
    ratios = jnp.exp(jnp.minimum(decay_logarithm[:, :, None] - decay_logarithm[:, None, :], 0.0))
    key_dots = jnp.einsum('hik,hjk->hij', keys_n, keys_n, precision=strict_precision)
    query_dots = jnp.einsum('hik,hjk->hij', normalized_queries, keys_n, precision=strict_precision)
    system = jnp.where(row_ids > col_ids, writes[:, :, None] * ratios * key_dots, 0.0)
    system = system + jnp.eye(length, dtype=jnp.float32)
    scaled = writes * jnp.exp(decay_logarithm)
    right_side = jnp.concatenate([scaled[:, :, None] * keys_n, writes[:, :, None] * values_f], axis=2)
    solved = jax.scipy.linalg.solve_triangular(system, right_side, lower=True, unit_diagonal=True)
    weighted_key_rows = solved[:, :, :key_width]
    corrected_values = solved[:, :, key_width:]
    mixing = jnp.where(row_ids >= col_ids, ratios * query_dots, 0.0)
    trailing_keys = jnp.exp(decay_logarithm[:, -1:] - decay_logarithm)[:, :, None] * keys_n
    return (weighted_key_rows, corrected_values, mixing, trailing_keys)

def block_apply(memory_state, normalized_queries, decay_logarithm, weighted_key_rows, corrected_values, mixing, trailing_keys):
    state_increment = corrected_values - jnp.einsum('qjl,qlo->qjo', weighted_key_rows, memory_state, precision=strict_precision)
    output_rows = jnp.exp(decay_logarithm)[:, :, None] * jnp.einsum('qjl,qlo->qjo', normalized_queries, memory_state, precision=strict_precision)
    output_rows = output_rows + jnp.einsum('hij,hjv->hiv', mixing, state_increment, precision=strict_precision)
    updated_state = jnp.exp(decay_logarithm[:, -1])[:, None, None] * memory_state
    updated_state = updated_state + jnp.einsum('oqm,oqy->omy', trailing_keys, state_increment, precision=strict_precision)
    return (updated_state, output_rows)

def normalize(output_rows, norm_gain):
    mean_sq = lax.optimization_barrier(jnp.mean(output_rows * output_rows, axis=-1, keepdims=True))
    return (output_rows / jnp.sqrt(mean_sq + norm_eps) * norm_gain).astype(jnp.bfloat16)

def reference(queries, key_vecs, values, strength, decay_rate, norm_gain, w_out):
    total_len = queries.shape[0]
    block_count = total_len // BLOCK_TOKENS
    heads_v = values.shape[1]
    blocks = (queries.reshape(block_count, BLOCK_TOKENS, HQK, DK), key_vecs.reshape(block_count, BLOCK_TOKENS, HQK, DK), values.reshape(block_count, BLOCK_TOKENS, heads_v, DV), strength.reshape(block_count, BLOCK_TOKENS, heads_v), decay_rate.reshape(block_count, BLOCK_TOKENS, heads_v))

    def advance(memory_state, pieces):
        prepared = prepare(pieces[0], pieces[1], pieces[2], pieces[3], pieces[4])
        weighted_key_rows, corrected_values, mixing, trailing_keys = block_parts(*prepared)
        updated_state, output_rows = block_apply(memory_state, prepared[0], prepared[4], weighted_key_rows, corrected_values, mixing, trailing_keys)
        return (updated_state, normalize(jnp.transpose(output_rows, (1, 0, 2)), norm_gain))
    start_state = jnp.zeros((heads_v, DK, DV), jnp.float32)
    _, normed = lax.scan(advance, start_state, blocks)
    flat = normed.reshape(total_len, heads_v * DV)
    mixed = jnp.dot(flat.astype(jnp.float32), w_out.astype(jnp.float32), precision=strict_precision)
    return mixed.astype(jnp.bfloat16)
```

```python
import functools

import jax
import jax.numpy as jnp
from jax import lax
from jax.experimental import pallas as pl
from jax.experimental.pallas import tpu as pltpu
from jax.sharding import Mesh
from jax.sharding import PartitionSpec as P

SEQ = ("seq_0", "seq_1", "seq_2")
SEQ_HEADS = ("seq_0", "seq_1", "seq_2", "heads")
F32 = jnp.float32
BF16 = jnp.bfloat16
HIGHEST = lax.Precision.HIGHEST
norm_eps = 1e-12
unit_eps = 1e-06

NN = (((1,), (0,)), ((), ()))
NT = (((1,), (1,)), ((), ()))
TN = (((0,), (0,)), ((), ()))


def dot(a, b, dims=NN):
    return lax.dot_general(a, b, dims, preferred_element_type=F32)


def split(x):
    high = x.astype(BF16)
    low = (x - high.astype(F32)).astype(BF16)
    return high, low


def dot_split(a, b, dims=NN):
    return dot(a[0], b[0], dims) + (dot(a[0], b[1], dims) + dot(a[1], b[0], dims))


def spread(parts):
    half = parts[0].shape[0]
    out = []
    for part in parts:
        zero = jnp.zeros((half, half), part.dtype)
        top = jnp.concatenate([part[:, :half], zero], axis=1)
        bottom = jnp.concatenate([zero, part[:, half:]], axis=1)
        out.append(jnp.concatenate([top, bottom], axis=0))
    return tuple(out)


def unit_lower_inverse(lower, row, col):
    size = lower.shape[0]
    half = size // 2
    compact = jnp.concatenate([lower[:half, :half], lower[half:, half:]], axis=1)
    r = row[:half, :]
    c = col[:half, :] % half
    base = 8
    diag = jnp.where(r // base == c // base, compact, 0.0)
    s1 = split(diag)
    d2 = dot_split(s1, spread(s1))
    s2 = split(d2)
    f2 = spread(s2)
    d3 = dot_split(s1, f2)
    d4 = dot_split(s2, f2)
    inv = jnp.where(r == c, 1.0, 0.0) - diag + d2 - d3
    inv = inv + dot_split(split(inv), spread(split(d4)))
    width = base
    while width < half:
        across = (r // (2 * width) == c // (2 * width)) & (r // width != c // width)
        off = split(jnp.where(across, compact, 0.0))
        si = split(inv)
        step = split(dot_split(si, spread(off)))
        inv = inv - dot_split(step, spread(si))
        width *= 2
    top, bottom = inv[:, :half], inv[:, half:]
    corner = split(dot_split(split(bottom), split(lower[half:, :half])))
    corner = -dot_split(corner, split(top))
    return jnp.concatenate(
        [
            jnp.concatenate([top, jnp.zeros((half, half), F32)], axis=1),
            jnp.concatenate([corner, bottom], axis=1),
        ],
        axis=0,
    )


def local_kernel(q_ref, k_ref, v_ref, w_ref, d_ref, maps_ref, own_ref, reach_ref, rows, cols):
    size, width = k_ref.shape
    group = maps_ref.shape[0]
    pair = pl.program_id(0)
    row = lax.broadcasted_iota(jnp.int32, (size, size), 0)
    col = lax.broadcasted_iota(jnp.int32, (size, size), 1)

    @pl.when(pair == 0)
    def _():
        tri = jnp.where(row >= col, 1.0, 0.0).astype(F32)
        eye = jnp.where(row == col, 1.0, 0.0).astype(F32)
        rate = d_ref[...]
        cols[...] = lax.dot_general(tri, rate, NN, precision=HIGHEST, preferred_element_type=F32)
        rows[0] = lax.dot_general(
            rate, tri, (((0,), (1,)), ((), ())), precision=HIGHEST, preferred_element_type=F32
        )
        rows[1] = lax.dot_general(
            w_ref[...], eye, TN, precision=HIGHEST, preferred_element_type=F32
        )

    q = q_ref[...]
    k = k_ref[...]
    kf = k.astype(F32)
    qf = q.astype(F32)
    k2 = kf * kf
    rk_col = lax.rsqrt(jnp.sum(k2, axis=1, keepdims=True) + unit_eps)
    rq_col = lax.rsqrt(jnp.sum(qf * qf, axis=1, keepdims=True) + unit_eps)
    ones = jnp.ones((8, width), F32)
    k2_row = lax.dot_general(ones, k2, NT, precision=HIGHEST, preferred_element_type=F32)
    rk_row = lax.rsqrt(k2_row[0:1, :] + unit_eps)
    key_dots = dot(k, k, NT) * rk_col * rk_row
    query_dots = dot(q, k, NT) * rq_col * rk_row
    unit_q = qf * rq_col
    heads = w_ref.shape[1]
    lane = lax.broadcasted_iota(jnp.int32, (size, heads), 1)
    eye_k = jnp.where(
        lax.broadcasted_iota(jnp.int32, (width, width), 0)
        == lax.broadcasted_iota(jnp.int32, (width, width), 1),
        1.0,
        0.0,
    )
    for member in range(group):
        head = pair * group + member
        g_col = -jnp.sum(jnp.where(lane == head, cols[...], 0.0), axis=1, keepdims=True)
        w_col = jnp.sum(jnp.where(lane == head, w_ref[...], 0.0), axis=1, keepdims=True)
        g_row = -rows[0, pl.ds(head, 1), :]
        w_row = rows[1, pl.ds(head, 1), :]
        ratios = jnp.exp(jnp.minimum(g_col - g_row, 0.0))
        lower = jnp.where(row > col, w_col * ratios * key_dots, 0.0)
        mixing = split(jnp.where(row >= col, ratios * query_dots, 0.0))
        inv = unit_lower_inverse(lower, row, col)
        g_end = g_row[:, size - 1 : size]
        gamma_col = jnp.exp(g_col)
        trail = jnp.exp(g_end - g_col) * rk_col
        on_keys = split(inv * (w_row * jnp.exp(g_row) * rk_row))
        on_values = split(inv * w_row)
        v = v_ref[:, member * width : (member + 1) * width]
        solved = jnp.concatenate(
            [
                dot(on_keys[0], k) + dot(on_keys[1], k),
                dot(on_values[0], v) + dot(on_values[1], v),
            ],
            axis=1,
        )
        mixed = dot_split(mixing, split(solved))
        tail = split(trail * solved)
        moved = dot(k, tail[0], TN) + dot(k, tail[1], TN)
        maps_ref[member, :, :width] = jnp.exp(g_end) * eye_k - moved[:, :width]
        maps_ref[member, :, width:] = moved[:, width:]
        reach_ref[member] = gamma_col * unit_q - mixed[:, :width]
        own_ref[member] = mixed[:, width:]


def local_work(queries, key_vecs, values, strength, decay_rate):
    size, pairs, width = queries.shape
    heads = values.shape[1]
    group = heads // pairs
    flat_q = queries.reshape(size, pairs * width)
    flat_k = key_vecs.reshape(size, pairs * width)
    flat_v = values.reshape(size, heads * width)
    one = pl.BlockSpec((size, width), lambda i: (0, i))
    small = pl.BlockSpec((size, heads), lambda i: (0, 0))
    return pl.pallas_call(
        local_kernel,
        grid=(pairs,),
        in_specs=[one, one, pl.BlockSpec((size, group * width), lambda i: (0, i)), small, small],
        out_specs=[
            pl.BlockSpec((group, width, 2 * width), lambda i: (i, 0, 0)),
            pl.BlockSpec((group, size, width), lambda i: (i, 0, 0)),
            pl.BlockSpec((group, size, width), lambda i: (i, 0, 0)),
        ],
        out_shape=[
            jax.ShapeDtypeStruct((heads, width, 2 * width), F32),
            jax.ShapeDtypeStruct((heads, size, width), F32),
            jax.ShapeDtypeStruct((heads, size, width), F32),
        ],
        scratch_shapes=[pltpu.VMEM((2, heads, size), F32), pltpu.VMEM((size, heads), F32)],
        compiler_params=pltpu.CompilerParams(dimension_semantics=("arbitrary",)),
        name="local_work",
    )(flat_q, flat_k, flat_v, strength, decay_rate)


def remote(src, dst, send, recv, target):
    return pltpu.make_async_remote_copy(
        src_ref=src,
        dst_ref=dst,
        send_sem=send,
        recv_sem=recv,
        device_id=target,
        device_id_type=pl.DeviceIdType.MESH,
    )


def prefix_kernel(
    maps_ref, out_ref, arrived, prefix, lower_map, plane, states, incoming, passing,
    send_maps, recv_maps, send_pair, recv_pair, send_chain, recv_chain, send_down, recv_down,
):
    width = maps_ref.shape[1]
    z = lax.axis_index("seq_0")
    x = lax.axis_index("seq_1")
    y = lax.axis_index("seq_2")
    upper = x // 2
    side = x % 2
    place = side * 4 + y
    mine = ((side + upper) % 2) * 4 + y
    mirror = 3 - x

    def peer(step):
        p = (place + step) % 8
        target = {"seq_1": upper * 2 + p // 4, "seq_2": p % 4}
        head = ((p // 4 + upper) % 2) * 4 + p % 4
        return p, target, head

    def beside(dz, at):
        return {"seq_0": (z + dz + 4) % 4, "seq_1": at}

    barrier = pltpu.get_barrier_semaphore()
    greeted = [peer(step)[1] for step in range(1, 8)]
    greeted += [{"seq_1": mirror}]
    greeted += [beside(dz, at) for dz in (1, -1) for at in (x, mirror)]
    for target in greeted:
        pl.semaphore_signal(barrier, inc=1, device_id=target, device_id_type=pl.DeviceIdType.MESH)
    pl.semaphore_wait(barrier, len(greeted))

    for step in range(1, 8):
        p, target, head = peer(step)
        remote(
            maps_ref.at[head], arrived.at[place], send_maps.at[step], recv_maps.at[place], target
        ).start()
    arrived[place] = maps_ref[mine]

    def wait_map(s):
        @pl.when(place != s)
        def _():
            remote(
                maps_ref.at[0], arrived.at[s], send_maps.at[0], recv_maps.at[s], {"seq_1": mirror}
            ).wait_recv()

    def then(later, running):
        moved = dot_split(split(later[:, :width]), split(running))
        return jnp.concatenate([moved[:, :width], moved[:, width:] + later[:, width:]], axis=1)

    wait_map(0)
    running = arrived[0]
    prefix[0] = running
    for s in range(1, 8):
        wait_map(s)
        running = then(arrived[s], running)
        prefix[s] = running

    pair = remote(prefix.at[7], lower_map, send_pair, recv_pair, {"seq_1": mirror})

    @pl.when(upper == 0)
    def _():
        pair.start()

    @pl.when(upper == 1)
    def _():
        pair.wait_recv()
        plane[...] = then(prefix[7], lower_map[...])

    chain = [
        remote(passing, incoming, send_chain.at[i], recv_chain, beside(1, at))
        for i, at in enumerate((x, mirror))
    ]

    @pl.when(z == 0)
    def _():
        incoming[...] = jnp.zeros_like(incoming)

    @pl.when(z > 0)
    def _():
        chain[0].wait_recv()

    before = split(incoming[...])

    @pl.when((upper == 1) & (z < 3))
    def _():
        passing[...] = dot_split(split(plane[:, :width]), before) + plane[:, width:]
        for copy in chain:
            copy.start()

    @pl.when(upper == 0)
    def _():
        states[0] = incoming[...]

    @pl.when(upper == 1)
    def _():
        states[0] = dot_split(split(lower_map[:, :width]), before) + lower_map[:, width:]

    ahead = split(states[0])
    for s in range(1, 8):
        states[s] = dot_split(split(prefix[s - 1, :, :width]), ahead) + prefix[s - 1, :, width:]

    for step in range(1, 8):
        p, target, head = peer(step)
        remote(
            states.at[p], out_ref.at[mine], send_down.at[step], recv_down.at[mine], target
        ).start()
    out_ref[mine] = states[place]
    for s in range(8):
        @pl.when(mine != s)
        def _():
            remote(
                states.at[0], out_ref.at[s], send_down.at[0], recv_down.at[s], {"seq_1": mirror}
            ).wait_recv()

    for step in range(1, 8):
        p, target, head = peer(step)
        remote(
            maps_ref.at[head], arrived.at[place], send_maps.at[step], recv_maps.at[place], target
        ).wait_send()
        remote(
            states.at[p], out_ref.at[mine], send_down.at[step], recv_down.at[mine], target
        ).wait_send()

    @pl.when(upper == 0)
    def _():
        pair.wait_send()

    @pl.when((upper == 1) & (z < 3))
    def _():
        for copy in chain:
            copy.wait_send()


def prefix_states(maps):
    heads, width, _ = maps.shape
    dma = pltpu.SemaphoreType.DMA
    vmem = pl.BlockSpec(memory_space=pltpu.VMEM)
    return pl.pallas_call(
        prefix_kernel,
        out_shape=jax.ShapeDtypeStruct((heads, width, width), F32),
        in_specs=[vmem],
        out_specs=vmem,
        scratch_shapes=[
            pltpu.VMEM((8, width, 2 * width), F32),
            pltpu.VMEM((8, width, 2 * width), F32),
            pltpu.VMEM((width, 2 * width), F32),
            pltpu.VMEM((width, 2 * width), F32),
            pltpu.VMEM((8, width, width), F32),
            pltpu.VMEM((width, width), F32),
            pltpu.VMEM((width, width), F32),
            dma((8,)),
            dma((8,)),
            dma,
            dma,
            dma((2,)),
            dma,
            dma((8,)),
            dma((8,)),
        ],
        compiler_params=pltpu.CompilerParams(collective_id=0, has_side_effects=True),
        name="prefix_states",
    )(maps)


def output_kernel(
    own_ref, reach_ref, state_ref, gain_ref, weight_hbm, out_ref,
    weight, flat, to_core, from_core, to_chip, from_chip, local,
    load_sem, send_core, recv_core, send_chip, recv_chip,
):
    heads, size, width = own_ref.shape
    rows = size // 4
    chunks, _, span = to_chip.shape
    me = lax.axis_index("heads")
    chip = me // 2
    core = me % 2
    other_core = {"heads": chip * 2 + 1 - core}
    other_chip = {"heads": (1 - chip) * 2 + core}

    load = pltpu.make_async_copy(weight_hbm, weight, load_sem)
    load.start()
    barrier = pltpu.get_barrier_semaphore()
    for target in (other_core, other_chip):
        pl.semaphore_signal(barrier, inc=1, device_id=target, device_id_type=pl.DeviceIdType.MESH)
    pl.semaphore_wait(barrier, 2)

    for head in range(heads):
        value = own_ref[head] + dot_split(split(reach_ref[head]), split(state_ref[head]))
        mean = jnp.mean(value * value, axis=1, keepdims=True)
        normed = value * lax.rsqrt(mean + norm_eps) * gain_ref[...]
        flat[:, head * width : (head + 1) * width] = normed.astype(BF16)
    load.wait()

    def rows_of(owner):
        return pl.ds(pl.multiple_of(owner * rows, rows), rows)

    def core_copy(c):
        return remote(
            to_core.at[c], from_core.at[c], send_core.at[c], recv_core.at[c], other_core
        )

    def chip_copy(c):
        return remote(
            to_chip.at[c], from_chip.at[c], send_chip.at[c], recv_chip.at[c], other_chip
        )

    far_mine = flat[rows_of((1 - chip) * 2 + core), :]
    far_theirs = flat[rows_of((1 - chip) * 2 + 1 - core), :]
    near_mine = flat[rows_of(me), :]
    near_theirs = flat[rows_of(chip * 2 + 1 - core), :]
    far = jnp.concatenate([far_theirs, far_mine], axis=0)
    near = jnp.concatenate([near_theirs, near_mine], axis=0)

    for c in range(chunks):
        part = dot(far, weight[:, c * span : (c + 1) * span])
        to_core[c] = part[:rows]
        core_copy(c).start()
        to_chip[c] = part[rows:]
    for c in range(chunks):
        core_copy(c).wait_recv()
        to_chip[c] = to_chip[c] + from_core[c]
        chip_copy(c).start()
    for c in range(chunks):
        part = dot(near, weight[:, c * span : (c + 1) * span])
        to_core[chunks + c] = part[:rows]
        core_copy(chunks + c).start()
        local[c] = part[rows:]
    for c in range(chunks):
        core_copy(chunks + c).wait_recv()
        local[c] = local[c] + from_core[chunks + c]
    for c in range(chunks):
        chip_copy(c).wait_recv()
        total = local[c] + from_chip[c]
        out_ref[:, c * span : (c + 1) * span] = total.astype(BF16)
    for c in range(chunks):
        core_copy(c).wait_send()
        core_copy(chunks + c).wait_send()
        chip_copy(c).wait_send()


def outputs(own, reach, states, norm_gain, w_out):
    heads, size, width = own.shape
    depth, model = w_out.shape
    chunks = 4
    span = model // chunks
    rows = size // 4
    dma = pltpu.SemaphoreType.DMA
    vmem = pl.BlockSpec(memory_space=pltpu.VMEM)
    return pl.pallas_call(
        output_kernel,
        out_shape=jax.ShapeDtypeStruct((rows, model), BF16),
        in_specs=[vmem, vmem, vmem, vmem, pl.BlockSpec(memory_space=pl.ANY)],
        out_specs=vmem,
        scratch_shapes=[
            pltpu.VMEM((depth, model), BF16),
            pltpu.VMEM((size, depth), BF16),
            pltpu.VMEM((2 * chunks, rows, span), F32),
            pltpu.VMEM((2 * chunks, rows, span), F32),
            pltpu.VMEM((chunks, rows, span), F32),
            pltpu.VMEM((chunks, rows, span), F32),
            pltpu.VMEM((chunks, rows, span), F32),
            dma,
            dma((2 * chunks,)),
            dma((2 * chunks,)),
            dma((chunks,)),
            dma((chunks,)),
        ],
        compiler_params=pltpu.CompilerParams(collective_id=1, has_side_effects=True),
        name="outputs",
    )(own, reach, states, norm_gain.reshape(1, width), w_out)


def body(queries, key_vecs, values, strength, decay_rate, norm_gain, w_out):
    maps, own, reach = local_work(queries, key_vecs, values, strength, decay_rate)
    states = prefix_states(maps)
    return outputs(own, reach, states, norm_gain, w_out)


def solution(mesh):
    finer = Mesh(
        mesh.devices.reshape(4, 4, 4, mesh.shape["heads"]), ("seq_0", "seq_1", "seq_2", "heads")
    )
    placed = (
        P(SEQ, "heads", None),
        P(SEQ, "heads", None),
        P(SEQ, "heads", None),
        P(SEQ, "heads"),
        P(SEQ, "heads"),
        P(),
        P("heads", None),
    )
    return jax.shard_map(
        body, mesh=finer, in_specs=placed, out_specs=P(SEQ_HEADS, None), check_vma=False
    )
```

```python
import functools

import jax
import jax.numpy as jnp
from jax import lax
from jax.experimental import pallas as pl
from jax.experimental.pallas import tpu as pltpu
from jax.sharding import Mesh
from jax.sharding import PartitionSpec as P

SEQ = ("seq_0", "seq_1", "seq_2")
SEQ_HEADS = ("seq_0", "seq_1", "seq_2", "heads")
F32 = jnp.float32
BF16 = jnp.bfloat16
HIGHEST = lax.Precision.HIGHEST
norm_eps = 1e-12
unit_eps = 1e-06

NN = (((1,), (0,)), ((), ()))
NT = (((1,), (1,)), ((), ()))
TN = (((0,), (0,)), ((), ()))


def dot(a, b, dims=NN):
    return lax.dot_general(a, b, dims, preferred_element_type=F32)


def split(x):
    high = x.astype(BF16)
    low = (x - high.astype(F32)).astype(BF16)
    return high, low


def dot_split(a, b, dims=NN):
    return dot(a[0], b[0], dims) + (dot(a[0], b[1], dims) + dot(a[1], b[0], dims))


def spread(part):
    half = part.shape[0]
    zero = jnp.zeros((half, half), part.dtype)
    top = jnp.concatenate([part[:, :half], zero], axis=1)
    bottom = jnp.concatenate([zero, part[:, half:]], axis=1)
    return jnp.concatenate([top, bottom], axis=0)


def unit_lower_inverse(lower, row, col):
    size = lower.shape[0]
    half = size // 2
    compact = jnp.concatenate([lower[:half, :half], lower[half:, half:]], axis=1)
    r = row[:half, :]
    c = col[:half, :] % half
    base = 8
    diag = jnp.where(r // base == c // base, compact, 0.0)
    s1 = diag.astype(BF16)
    d2 = dot(s1, spread(s1))
    s2 = d2.astype(BF16)
    f2 = spread(s2)
    d3 = dot(s1, f2)
    d4 = dot(s2, f2)
    inv = jnp.where(r == c, 1.0, 0.0) - diag + d2 - d3
    inv = inv + dot(inv.astype(BF16), spread(d4.astype(BF16)))
    width = base
    while width < half:
        across = (r // (2 * width) == c // (2 * width)) & (r // width != c // width)
        off = jnp.where(across, compact, 0.0).astype(BF16)
        si = inv.astype(BF16)
        step = dot(si, spread(off)).astype(BF16)
        inv = inv - dot(step, spread(si))
        width *= 2
    si = inv.astype(BF16)
    top, bottom = si[:, :half], si[:, half:]
    high, low = split(lower)
    corner = dot(bottom, high[half:, :half]).astype(BF16)
    corner = -dot(corner, top)
    rough = jnp.concatenate(
        [
            jnp.concatenate([top, jnp.zeros((half, half), BF16)], axis=1),
            jnp.concatenate([corner.astype(BF16), bottom], axis=1),
        ],
        axis=0,
    )
    eye = jnp.where(row == col, 1.0, 0.0)
    known = rough.astype(F32)
    residual = (eye - known) - (dot(high, rough) + dot(low, rough))
    short = residual.astype(BF16)
    series = (residual + dot(short, short)).astype(BF16)
    return known + dot(rough, series)


def column(table, head):
    lane = lax.broadcasted_iota(jnp.int32, table.shape, 1)
    return jnp.sum(jnp.where(lane == head, table, 0.0), axis=1, keepdims=True)


def unpack_inputs(q_ref, k_ref, v_ref, w_ref, d_ref, q32, k32, v32, rows, cols):
    q32[...] = q_ref[...].astype(F32)
    k32[...] = k_ref[...].astype(F32)
    v32[...] = v_ref[...].astype(F32)
    size = d_ref.shape[1]
    row = lax.broadcasted_iota(jnp.int32, (size, size), 0)
    col = lax.broadcasted_iota(jnp.int32, (size, size), 1)
    tri = jnp.where(row >= col, 1.0, 0.0).astype(F32)
    summed = lax.dot_general(d_ref[...], tri, NT, precision=HIGHEST, preferred_element_type=F32)
    rows[0] = -summed
    rows[1] = w_ref[...]
    cols[0] = rows[0].T
    cols[1] = rows[1].T


def key_parts(k32, pair, pairs, size):
    kf = k32[pl.ds(pair, size, stride=pairs), :]
    k2 = kf * kf
    rk_col = lax.rsqrt(jnp.sum(k2, axis=1, keepdims=True) + unit_eps)
    ones = jnp.ones((8, kf.shape[1]), BF16)
    high, low = split(k2)
    total = dot(ones, high, NT) + dot(ones, low, NT)
    rk_row = lax.rsqrt(total[0:1, :] + unit_eps)
    return kf, kf.astype(BF16), rk_col, rk_row


def decay_ratios(rows, cols, head):
    g_row = rows[0, pl.ds(head, 1), :]
    g_col = column(cols[0], head)
    return g_row, g_col, jnp.exp(jnp.minimum(g_col - g_row, 0.0))


def pair_maps(pair, k32, v32, rows, cols, maps_ref, solved_ref):
    heads, width, _ = maps_ref.shape
    size = rows.shape[2]
    pairs = k32.shape[0] // size
    group = heads // pairs
    row = lax.broadcasted_iota(jnp.int32, (size, size), 0)
    col = lax.broadcasted_iota(jnp.int32, (size, size), 1)
    eye_k = jnp.where(row[:width, :width] == col[:width, :width], 1.0, 0.0)
    kf, k, rk_col, rk_row = key_parts(k32, pair, pairs, size)
    k_t = kf.T.astype(BF16)
    key_dots = dot(k, k, NT) * rk_col * rk_row
    for member in range(group):
        head = pair * group + member
        g_row, g_col, ratios = decay_ratios(rows, cols, head)
        w_row = rows[1, pl.ds(head, 1), :]
        w_col = column(cols[1], head)
        lower = jnp.where(row > col, w_col * ratios * key_dots, 0.0)
        inv = split(unit_lower_inverse(lower, row, col) * w_row)
        g_end = g_row[:, size - 1 : size]
        keys = split(kf * (jnp.exp(g_col) * rk_col))
        v = v32[pl.ds(head, size, stride=heads), :].astype(BF16)
        right = jnp.concatenate([keys[0], v], axis=1)
        both = dot(inv[0], right) + dot(inv[1], right)
        on_keys = both[:, :width] + dot(inv[0], keys[1])
        solved = jnp.concatenate([on_keys, both[:, width:]], axis=1)
        solved_ref[head] = solved
        tail = split((jnp.exp(g_end - g_col) * rk_col) * solved)
        moved = dot(k_t, tail[0]) + dot(k_t, tail[1])
        maps_ref[head, :, :width] = jnp.exp(g_end) * eye_k - moved[:, :width]
        maps_ref[head, :, width:] = moved[:, width:]


def pair_outputs(pair, q32, k32, rows, cols, solved_ref, own_ref, reach_ref):
    heads, size, width = own_ref.shape
    pairs = k32.shape[0] // size
    group = heads // pairs
    row = lax.broadcasted_iota(jnp.int32, (size, size), 0)
    col = lax.broadcasted_iota(jnp.int32, (size, size), 1)
    kf, k, rk_col, rk_row = key_parts(k32, pair, pairs, size)
    qf = q32[pl.ds(pair, size, stride=pairs), :]
    rq_col = lax.rsqrt(jnp.sum(qf * qf, axis=1, keepdims=True) + unit_eps)
    query_dots = dot(qf.astype(BF16), k, NT) * rq_col * rk_row
    unit_q = qf * rq_col
    for member in range(group):
        head = pair * group + member
        g_row, g_col, ratios = decay_ratios(rows, cols, head)
        mixing = split(jnp.where(row >= col, ratios * query_dots, 0.0))
        mixed = dot_split(mixing, split(solved_ref[head]))
        reach_ref[head] = jnp.exp(g_col) * unit_q - mixed[:, :width]
        own_ref[head] = mixed[:, width:]


def remote(src, dst, send, recv, target):
    return pltpu.make_async_remote_copy(
        src_ref=src,
        dst_ref=dst,
        send_sem=send,
        recv_sem=recv,
        device_id=target,
        device_id_type=pl.DeviceIdType.MESH,
    )


def front_kernel(
    q_ref, k_ref, v_ref, w_ref, d_ref, own_ref, reach_ref, out_ref,
    q32, k32, v32, rows, cols, maps_ref, solved_ref,
    arrived, prefix, lower_map, plane, states, incoming, passing,
    send_maps, recv_maps, send_pair, recv_pair, send_chain, recv_chain, send_down, recv_down,
):
    width = maps_ref.shape[1]
    z = lax.axis_index("seq_0")
    x = lax.axis_index("seq_1")
    y = lax.axis_index("seq_2")
    upper = x // 2
    side = x % 2
    place = side * 4 + y
    mine = ((side + upper) % 2) * 4 + y
    mirror = 3 - x

    def peer(step):
        p = (place + step) % 8
        target = {"seq_1": upper * 2 + p // 4, "seq_2": p % 4}
        head = ((p // 4 + upper) % 2) * 4 + p % 4
        return p, target, head

    def beside(dz, at):
        return {"seq_0": (z + dz + 4) % 4, "seq_1": at}

    barrier = pltpu.get_barrier_semaphore()
    greeted = [peer(step)[1] for step in range(1, 8)]
    greeted += [{"seq_1": mirror}]
    greeted += [beside(dz, at) for dz in (1, -1) for at in (x, mirror)]
    for target in greeted:
        pl.semaphore_signal(barrier, inc=1, device_id=target, device_id_type=pl.DeviceIdType.MESH)

    unpack_inputs(q_ref, k_ref, v_ref, w_ref, d_ref, q32, k32, v32, rows, cols)

    def send_map(head):
        p = ((head // 4 + upper) % 2) * 4 + head % 4
        target = {"seq_1": upper * 2 + p // 4, "seq_2": p % 4}
        return remote(
            maps_ref.at[head], arrived.at[place], send_maps.at[head], recv_maps.at[place], target
        )

    def one_pair(step, carry):
        pair = (mine // 2 + step) % 4
        pair_maps(pair, k32, v32, rows, cols, maps_ref, solved_ref)

        @pl.when(step == 1)
        def _():
            pl.semaphore_wait(barrier, len(greeted))

        for member in range(2):
            head = pair * 2 + member

            @pl.when(head != mine)
            def _():
                send_map(head).start()

        return carry

    lax.fori_loop(1, 5, one_pair, 0)
    arrived[place] = maps_ref[mine]

    def one_output(pair, carry):
        pair_outputs(pair, q32, k32, rows, cols, solved_ref, own_ref, reach_ref)
        return carry

    lax.fori_loop(0, 4, one_output, 0)

    def wait_map(s):
        @pl.when(place != s)
        def _():
            remote(
                maps_ref.at[0], arrived.at[s], send_maps.at[0], recv_maps.at[s], {"seq_1": mirror}
            ).wait_recv()

    def then(later, running):
        moved = dot_split(split(later[:, :width]), split(running))
        return jnp.concatenate([moved[:, :width], moved[:, width:] + later[:, width:]], axis=1)

    wait_map(0)
    running = arrived[0]
    prefix[0] = running
    for s in range(1, 8):
        wait_map(s)
        running = then(arrived[s], running)
        prefix[s] = running

    pair = remote(prefix.at[7], lower_map, send_pair, recv_pair, {"seq_1": mirror})

    @pl.when(upper == 0)
    def _():
        pair.start()

    @pl.when(upper == 1)
    def _():
        pair.wait_recv()
        plane[...] = then(prefix[7], lower_map[...])

    chain = [
        remote(passing, incoming, send_chain.at[i], recv_chain, beside(1, at))
        for i, at in enumerate((x, mirror))
    ]

    @pl.when(z == 0)
    def _():
        incoming[...] = jnp.zeros_like(incoming)

    @pl.when(z > 0)
    def _():
        chain[0].wait_recv()

    before = split(incoming[...])

    @pl.when((upper == 1) & (z < 3))
    def _():
        passing[...] = dot_split(split(plane[:, :width]), before) + plane[:, width:]
        for copy in chain:
            copy.start()

    @pl.when(upper == 0)
    def _():
        states[0] = incoming[...]

    @pl.when(upper == 1)
    def _():
        states[0] = dot_split(split(lower_map[:, :width]), before) + lower_map[:, width:]

    ahead = split(states[0])
    for s in range(1, 8):
        states[s] = dot_split(split(prefix[s - 1, :, :width]), ahead) + prefix[s - 1, :, width:]

    for step in range(1, 8):
        p, target, head = peer(step)
        remote(
            states.at[p], out_ref.at[mine], send_down.at[step], recv_down.at[mine], target
        ).start()
    out_ref[mine] = states[place]
    for s in range(8):
        @pl.when(mine != s)
        def _():
            remote(
                states.at[0], out_ref.at[s], send_down.at[0], recv_down.at[s], {"seq_1": mirror}
            ).wait_recv()

    for step in range(1, 8):
        p, target, head = peer(step)
        send_map(head).wait_send()
        remote(
            states.at[p], out_ref.at[mine], send_down.at[step], recv_down.at[mine], target
        ).wait_send()

    @pl.when(upper == 0)
    def _():
        pair.wait_send()

    @pl.when((upper == 1) & (z < 3))
    def _():
        for copy in chain:
            copy.wait_send()


def front(queries, key_vecs, values, strength, decay_rate):
    size, pairs, width = queries.shape
    heads = values.shape[1]
    dma = pltpu.SemaphoreType.DMA
    vmem = pl.BlockSpec(memory_space=pltpu.VMEM)
    return pl.pallas_call(
        front_kernel,
        out_shape=[
            jax.ShapeDtypeStruct((heads, size, width), F32),
            jax.ShapeDtypeStruct((heads, size, width), F32),
            jax.ShapeDtypeStruct((heads, width, width), F32),
        ],
        in_specs=[vmem] * 5,
        out_specs=[vmem] * 3,
        scratch_shapes=[
            pltpu.VMEM((size * pairs, width), F32),
            pltpu.VMEM((size * pairs, width), F32),
            pltpu.VMEM((size * heads, width), F32),
            pltpu.VMEM((2, heads, size), F32),
            pltpu.VMEM((2, size, heads), F32),
            pltpu.VMEM((heads, width, 2 * width), F32),
            pltpu.VMEM((heads, size, 2 * width), F32),
            pltpu.VMEM((8, width, 2 * width), F32),
            pltpu.VMEM((8, width, 2 * width), F32),
            pltpu.VMEM((width, 2 * width), F32),
            pltpu.VMEM((width, 2 * width), F32),
            pltpu.VMEM((8, width, width), F32),
            pltpu.VMEM((width, width), F32),
            pltpu.VMEM((width, width), F32),
            dma((8,)),
            dma((8,)),
            dma,
            dma,
            dma((2,)),
            dma,
            dma((8,)),
            dma((8,)),
        ],
        compiler_params=pltpu.CompilerParams(collective_id=0, has_side_effects=True),
        name="front",
    )(
        queries.reshape(size * pairs, width),
        key_vecs.reshape(size * pairs, width),
        values.reshape(size * heads, width),
        strength.T,
        decay_rate.T,
    )


def output_kernel(
    own_ref, reach_ref, state_ref, gain_ref, weight_hbm, out_ref,
    weight, flat, to_core, from_core, to_chip, from_chip, local,
    load_sem, send_core, recv_core, send_chip, recv_chip,
):
    heads, size, width = own_ref.shape
    rows = size // 4
    chunks, _, span = to_chip.shape
    me = lax.axis_index("heads")
    chip = me // 2
    core = me % 2
    other_core = {"heads": chip * 2 + 1 - core}
    other_chip = {"heads": (1 - chip) * 2 + core}

    load = pltpu.make_async_copy(weight_hbm, weight, load_sem)
    load.start()
    barrier = pltpu.get_barrier_semaphore()
    for target in (other_core, other_chip):
        pl.semaphore_signal(barrier, inc=1, device_id=target, device_id_type=pl.DeviceIdType.MESH)
    pl.semaphore_wait(barrier, 2)

    for head in range(heads):
        value = own_ref[head] + dot_split(split(reach_ref[head]), split(state_ref[head]))
        mean = jnp.mean(value * value, axis=1, keepdims=True)
        normed = value * lax.rsqrt(mean + norm_eps) * gain_ref[...]
        flat[:, head * width : (head + 1) * width] = normed.astype(BF16)
    load.wait()

    def rows_of(owner):
        return pl.ds(pl.multiple_of(owner * rows, rows), rows)

    def core_copy(c):
        return remote(
            to_core.at[c], from_core.at[c], send_core.at[c], recv_core.at[c], other_core
        )

    def chip_copy(c):
        return remote(
            to_chip.at[c], from_chip.at[c], send_chip.at[c], recv_chip.at[c], other_chip
        )

    far_mine = flat[rows_of((1 - chip) * 2 + core), :]
    far_theirs = flat[rows_of((1 - chip) * 2 + 1 - core), :]
    near_mine = flat[rows_of(me), :]
    near_theirs = flat[rows_of(chip * 2 + 1 - core), :]
    far = jnp.concatenate([far_theirs, far_mine], axis=0)
    near = jnp.concatenate([near_theirs, near_mine], axis=0)

    for c in range(chunks):
        part = dot(far, weight[:, c * span : (c + 1) * span])
        to_core[c] = part[:rows]
        core_copy(c).start()
        to_chip[c] = part[rows:]
    for c in range(chunks):
        core_copy(c).wait_recv()
        to_chip[c] = to_chip[c] + from_core[c]
        chip_copy(c).start()
    for c in range(chunks):
        part = dot(near, weight[:, c * span : (c + 1) * span])
        to_core[chunks + c] = part[:rows]
        core_copy(chunks + c).start()
        local[c] = part[rows:]
    for c in range(chunks):
        core_copy(chunks + c).wait_recv()
        local[c] = local[c] + from_core[chunks + c]
    for c in range(chunks):
        chip_copy(c).wait_recv()
        total = local[c] + from_chip[c]
        out_ref[:, c * span : (c + 1) * span] = total.astype(BF16)
    for c in range(chunks):
        core_copy(c).wait_send()
        core_copy(chunks + c).wait_send()
        chip_copy(c).wait_send()


def outputs(own, reach, states, norm_gain, w_out):
    heads, size, width = own.shape
    depth, model = w_out.shape
    chunks = 4
    span = model // chunks
    rows = size // 4
    dma = pltpu.SemaphoreType.DMA
    vmem = pl.BlockSpec(memory_space=pltpu.VMEM)
    return pl.pallas_call(
        output_kernel,
        out_shape=jax.ShapeDtypeStruct((rows, model), BF16),
        in_specs=[vmem, vmem, vmem, vmem, pl.BlockSpec(memory_space=pl.ANY)],
        out_specs=vmem,
        scratch_shapes=[
            pltpu.VMEM((depth, model), BF16),
            pltpu.VMEM((size, depth), BF16),
            pltpu.VMEM((2 * chunks, rows, span), F32),
            pltpu.VMEM((2 * chunks, rows, span), F32),
            pltpu.VMEM((chunks, rows, span), F32),
            pltpu.VMEM((chunks, rows, span), F32),
            pltpu.VMEM((chunks, rows, span), F32),
            dma,
            dma((2 * chunks,)),
            dma((2 * chunks,)),
            dma((chunks,)),
            dma((chunks,)),
        ],
        compiler_params=pltpu.CompilerParams(collective_id=1, has_side_effects=True),
        name="outputs",
    )(own, reach, states, norm_gain.reshape(1, width), w_out)


def body(queries, key_vecs, values, strength, decay_rate, norm_gain, w_out):
    own, reach, states = front(queries, key_vecs, values, strength, decay_rate)
    return outputs(own, reach, states, norm_gain, w_out)


def solution(mesh):
    finer = Mesh(
        mesh.devices.reshape(4, 4, 4, mesh.shape["heads"]), ("seq_0", "seq_1", "seq_2", "heads")
    )
    placed = (
        P(SEQ, "heads", None),
        P(SEQ, "heads", None),
        P(SEQ, "heads", None),
        P(SEQ, "heads"),
        P(SEQ, "heads"),
        P(),
        P("heads", None),
    )
    return jax.shard_map(
        body, mesh=finer, in_specs=placed, out_specs=P(SEQ_HEADS, None), check_vma=False
    )
```

```python
import functools

import jax
import jax.numpy as jnp
from jax import lax
from jax.experimental import pallas as pl
from jax.experimental.pallas import tpu as pltpu
from jax.sharding import Mesh
from jax.sharding import PartitionSpec as P

SEQ = ("seq_0", "seq_1", "seq_2")
SEQ_HEADS = ("seq_0", "seq_1", "seq_2", "heads")
F32 = jnp.float32
BF16 = jnp.bfloat16
HIGHEST = lax.Precision.HIGHEST
norm_eps = 1e-12
unit_eps = 1e-06

NN = (((1,), (0,)), ((), ()))
NT = (((1,), (1,)), ((), ()))
TN = (((0,), (0,)), ((), ()))


def dot(a, b, dims=NN):
    return lax.dot_general(a, b, dims, preferred_element_type=F32)


def split(x):
    high = x.astype(BF16)
    low = (x - high.astype(F32)).astype(BF16)
    return high, low


def dot_split(a, b, dims=NN):
    return dot(a[0], b[0], dims) + (dot(a[0], b[1], dims) + dot(a[1], b[0], dims))


def spread(part):
    half = part.shape[0]
    zero = jnp.zeros((half, half), part.dtype)
    top = jnp.concatenate([part[:, :half], zero], axis=1)
    bottom = jnp.concatenate([zero, part[:, half:]], axis=1)
    return jnp.concatenate([top, bottom], axis=0)


def unit_lower_inverses(lowers, row, col):
    size = row.shape[0]
    half = size // 2
    r = row[:half, :]
    c = col[:half, :] % half
    base = 8
    unit = jnp.where(r == c, 1.0, 0.0)
    compact = [jnp.concatenate([x[:half, :half], x[half:, half:]], axis=1) for x in lowers]
    diag = [jnp.where(r // base == c // base, x, 0.0) for x in compact]
    s1 = [x.astype(BF16) for x in diag]
    d2 = [dot(x, spread(x)) for x in s1]
    s2 = [x.astype(BF16) for x in d2]
    d3 = [dot(x, spread(y)) for x, y in zip(s1, s2)]
    d4 = [dot(x, spread(x)).astype(BF16) for x in s2]
    inv = [unit - x + y - z for x, y, z in zip(diag, d2, d3)]
    inv = [x + dot(x.astype(BF16), spread(y)) for x, y in zip(inv, d4)]
    width = base
    while width < half:
        across = (r // (2 * width) == c // (2 * width)) & (r // width != c // width)
        off = [jnp.where(across, x, 0.0).astype(BF16) for x in compact]
        si = [x.astype(BF16) for x in inv]
        step = [dot(x, spread(y)).astype(BF16) for x, y in zip(si, off)]
        inv = [x - dot(y, spread(z)) for x, y, z in zip(inv, step, si)]
        width *= 2
    si = [x.astype(BF16) for x in inv]
    parts = [split(x) for x in lowers]
    corner = [dot(x[:, half:], y[0][half:, :half]).astype(BF16) for x, y in zip(si, parts)]
    corner = [(-dot(x, y[:, :half])).astype(BF16) for x, y in zip(corner, si)]
    zero = jnp.zeros((half, half), BF16)
    rough = [
        jnp.concatenate(
            [
                jnp.concatenate([x[:, :half], zero], axis=1),
                jnp.concatenate([y, x[:, half:]], axis=1),
            ],
            axis=0,
        )
        for x, y in zip(si, corner)
    ]
    eye = jnp.where(row == col, 1.0, 0.0)
    residual = [
        (eye - x.astype(F32)) - (dot(y[0], x) + dot(y[1], x)) for x, y in zip(rough, parts)
    ]
    short = [x.astype(BF16) for x in residual]
    series = [(x + dot(y, y)).astype(BF16) for x, y in zip(residual, short)]
    return [x.astype(F32) + dot(x, y) for x, y in zip(rough, series)]


def column(table, head):
    lane = lax.broadcasted_iota(jnp.int32, table.shape, 1)
    return jnp.sum(jnp.where(lane == head, table, 0.0), axis=1, keepdims=True)


def unpack_inputs(q_ref, k_ref, v_ref, w_ref, d_ref, q32, k32, v32, rows, cols):
    q32[...] = q_ref[...].astype(F32)
    k32[...] = k_ref[...].astype(F32)
    v32[...] = v_ref[...].astype(F32)
    size = d_ref.shape[1]
    row = lax.broadcasted_iota(jnp.int32, (size, size), 0)
    col = lax.broadcasted_iota(jnp.int32, (size, size), 1)
    tri = jnp.where(row >= col, 1.0, 0.0).astype(F32)
    summed = lax.dot_general(d_ref[...], tri, NT, precision=HIGHEST, preferred_element_type=F32)
    rows[0] = -summed
    rows[1] = w_ref[...]
    cols[0] = rows[0].T
    cols[1] = rows[1].T


def key_parts(k32, pair, pairs, size):
    kf = k32[pl.ds(pair, size, stride=pairs), :]
    k2 = kf * kf
    rk_col = lax.rsqrt(jnp.sum(k2, axis=1, keepdims=True) + unit_eps)
    ones = jnp.ones((8, kf.shape[1]), BF16)
    high, low = split(k2)
    total = dot(ones, high, NT) + dot(ones, low, NT)
    rk_row = lax.rsqrt(total[0:1, :] + unit_eps)
    return kf, kf.astype(BF16), rk_col, rk_row


def decay_ratios(rows, cols, head):
    g_row = rows[0, pl.ds(head, 1), :]
    g_col = column(cols[0], head)
    return g_row, g_col, jnp.exp(jnp.minimum(g_col - g_row, 0.0))


def state_maps(chosen, k32, v32, rows, cols, maps_ref, solved_ref):
    heads, width, _ = maps_ref.shape
    size = rows.shape[2]
    pairs = k32.shape[0] // size
    group = heads // pairs
    row = lax.broadcasted_iota(jnp.int32, (size, size), 0)
    col = lax.broadcasted_iota(jnp.int32, (size, size), 1)
    eye_k = jnp.where(row[:width, :width] == col[:width, :width], 1.0, 0.0)
    keyed = [key_parts(k32, pair, pairs, size) for pair in chosen]
    dots = [dot(k, k, NT) * rk_col * rk_row for _, k, rk_col, rk_row in keyed]
    todo = [(pair * group + member, n) for n, pair in enumerate(chosen) for member in range(group)]
    lowers = []
    for head, n in todo:
        _, _, ratios = decay_ratios(rows, cols, head)
        lowers.append(jnp.where(row > col, column(cols[1], head) * ratios * dots[n], 0.0))
    inverses = unit_lower_inverses(lowers, row, col)
    scaled = [split(x * rows[1, pl.ds(head, 1), :]) for x, (head, _) in zip(inverses, todo)]
    tails = []
    for inv, (head, n) in zip(scaled, todo):
        kf, _, rk_col, _ = keyed[n]
        g_col = column(cols[0], head)
        keys = split(kf * (jnp.exp(g_col) * rk_col))
        v = v32[pl.ds(head, size, stride=heads), :].astype(BF16)
        right = jnp.concatenate([keys[0], v], axis=1)
        both = dot(inv[0], right) + dot(inv[1], right)
        on_keys = both[:, :width] + dot(inv[0], keys[1])
        solved = jnp.concatenate([on_keys, both[:, width:]], axis=1)
        solved_ref[head] = solved
        g_end = rows[0, pl.ds(head, 1), :][:, size - 1 : size]
        tails.append((g_end, split((jnp.exp(g_end - g_col) * rk_col) * solved)))
    turned = [kf.T.astype(BF16) for kf, _, _, _ in keyed]
    for (g_end, tail), (head, n) in zip(tails, todo):
        moved = dot(turned[n], tail[0]) + dot(turned[n], tail[1])
        maps_ref[head, :, :width] = jnp.exp(g_end) * eye_k - moved[:, :width]
        maps_ref[head, :, width:] = moved[:, width:]


def pair_outputs(pair, q32, k32, rows, cols, solved_ref, own_ref, reach_ref):
    heads, size, width = own_ref.shape
    pairs = k32.shape[0] // size
    group = heads // pairs
    row = lax.broadcasted_iota(jnp.int32, (size, size), 0)
    col = lax.broadcasted_iota(jnp.int32, (size, size), 1)
    kf, k, rk_col, rk_row = key_parts(k32, pair, pairs, size)
    qf = q32[pl.ds(pair, size, stride=pairs), :]
    rq_col = lax.rsqrt(jnp.sum(qf * qf, axis=1, keepdims=True) + unit_eps)
    query_dots = dot(qf.astype(BF16), k, NT) * rq_col * rk_row
    unit_q = qf * rq_col
    for member in range(group):
        head = pair * group + member
        g_row, g_col, ratios = decay_ratios(rows, cols, head)
        mixing = split(jnp.where(row >= col, ratios * query_dots, 0.0))
        mixed = dot_split(mixing, split(solved_ref[head]))
        reach_ref[head] = jnp.exp(g_col) * unit_q - mixed[:, :width]
        own_ref[head] = mixed[:, width:]


def remote(src, dst, send, recv, target):
    return pltpu.make_async_remote_copy(
        src_ref=src,
        dst_ref=dst,
        send_sem=send,
        recv_sem=recv,
        device_id=target,
        device_id_type=pl.DeviceIdType.MESH,
    )


def front_kernel(
    q_ref, k_ref, v_ref, w_ref, d_ref, own_ref, reach_ref, out_ref,
    q32, k32, v32, rows, cols, maps_ref, solved_ref,
    arrived, prefix, lower_map, plane, states, incoming, passing,
    send_maps, recv_maps, send_pair, recv_pair, send_chain, recv_chain, send_down, recv_down,
):
    width = maps_ref.shape[1]
    z = lax.axis_index("seq_0")
    x = lax.axis_index("seq_1")
    y = lax.axis_index("seq_2")
    upper = x // 2
    side = x % 2
    place = side * 4 + y
    mine = ((side + upper) % 2) * 4 + y
    mirror = 3 - x

    def peer(step):
        p = (place + step) % 8
        target = {"seq_1": upper * 2 + p // 4, "seq_2": p % 4}
        head = ((p // 4 + upper) % 2) * 4 + p % 4
        return p, target, head

    def beside(dz, at):
        return {"seq_0": (z + dz + 4) % 4, "seq_1": at}

    barrier = pltpu.get_barrier_semaphore()
    greeted = [peer(step)[1] for step in range(1, 8)]
    greeted += [{"seq_1": mirror}]
    greeted += [beside(dz, at) for dz in (1, -1) for at in (x, mirror)]
    for target in greeted:
        pl.semaphore_signal(barrier, inc=1, device_id=target, device_id_type=pl.DeviceIdType.MESH)

    unpack_inputs(q_ref, k_ref, v_ref, w_ref, d_ref, q32, k32, v32, rows, cols)

    def send_map(head):
        p = ((head // 4 + upper) % 2) * 4 + head % 4
        target = {"seq_1": upper * 2 + p // 4, "seq_2": p % 4}
        return remote(
            maps_ref.at[head], arrived.at[place], send_maps.at[head], recv_maps.at[place], target
        )

    def some_heads(step, carry):
        part = (mine // 4 + step) % 2
        state_maps([part * 2, part * 2 + 1], k32, v32, rows, cols, maps_ref, solved_ref)

        @pl.when(step == 1)
        def _():
            pl.semaphore_wait(barrier, len(greeted))

        for member in range(4):
            head = part * 4 + (mine + 1 + member) % 4

            @pl.when(head != mine)
            def _():
                send_map(head).start()

        return carry

    lax.fori_loop(1, 3, some_heads, 0)
    arrived[place] = maps_ref[mine]

    def one_output(pair, carry):
        pair_outputs(pair, q32, k32, rows, cols, solved_ref, own_ref, reach_ref)
        return carry

    lax.fori_loop(0, 4, one_output, 0)

    def wait_map(s):
        @pl.when(place != s)
        def _():
            remote(
                maps_ref.at[0], arrived.at[s], send_maps.at[0], recv_maps.at[s], {"seq_1": mirror}
            ).wait_recv()

    def then(later, running):
        moved = dot_split(split(later[:, :width]), split(running))
        return jnp.concatenate([moved[:, :width], moved[:, width:] + later[:, width:]], axis=1)

    wait_map(0)
    running = arrived[0]
    prefix[0] = running
    for s in range(1, 8):
        wait_map(s)
        running = then(arrived[s], running)
        prefix[s] = running

    pair = [
        remote(
            prefix.at[7, :, pl.ds(part * width, width)],
            lower_map.at[:, pl.ds(part * width, width)],
            send_pair.at[part],
            recv_pair.at[part],
            {"seq_1": mirror},
        )
        for part in (1, 0)
    ]
    chain = [
        remote(passing, incoming, send_chain.at[i], recv_chain, beside(1, at))
        for i, at in enumerate((x, mirror))
    ]

    @pl.when(upper == 0)
    def _():
        for copy in pair:
            copy.start()

    @pl.when(upper == 1)
    def _():
        pair[0].wait_recv()

    @pl.when((upper == 1) & (z == 0))
    def _():
        passing[...] = (
            dot_split(split(prefix[7, :, :width]), split(lower_map[:, width:]))
            + prefix[7, :, width:]
        )
        for copy in chain:
            copy.start()

    @pl.when(upper == 1)
    def _():
        pair[1].wait_recv()

    @pl.when((upper == 1) & (z > 0))
    def _():
        plane[...] = then(prefix[7], lower_map[...])

    @pl.when(z == 0)
    def _():
        incoming[...] = jnp.zeros_like(incoming)

    @pl.when(z > 0)
    def _():
        chain[0].wait_recv()

    before = split(incoming[...])

    @pl.when((upper == 1) & (z > 0) & (z < 3))
    def _():
        passing[...] = dot_split(split(plane[:, :width]), before) + plane[:, width:]
        for copy in chain:
            copy.start()

    @pl.when(upper == 0)
    def _():
        states[0] = incoming[...]

    @pl.when(upper == 1)
    def _():
        states[0] = dot_split(split(lower_map[:, :width]), before) + lower_map[:, width:]

    ahead = split(states[0])
    for s in range(1, 8):
        states[s] = dot_split(split(prefix[s - 1, :, :width]), ahead) + prefix[s - 1, :, width:]

    for step in range(1, 8):
        p, target, head = peer(step)
        remote(
            states.at[p], out_ref.at[mine], send_down.at[step], recv_down.at[mine], target
        ).start()
    out_ref[mine] = states[place]
    for s in range(8):
        @pl.when(mine != s)
        def _():
            remote(
                states.at[0], out_ref.at[s], send_down.at[0], recv_down.at[s], {"seq_1": mirror}
            ).wait_recv()

    for step in range(1, 8):
        p, target, head = peer(step)
        send_map(head).wait_send()
        remote(
            states.at[p], out_ref.at[mine], send_down.at[step], recv_down.at[mine], target
        ).wait_send()

    @pl.when(upper == 0)
    def _():
        for copy in pair:
            copy.wait_send()

    @pl.when((upper == 1) & (z < 3))
    def _():
        for copy in chain:
            copy.wait_send()


def front(queries, key_vecs, values, strength, decay_rate):
    size, pairs, width = queries.shape
    heads = values.shape[1]
    dma = pltpu.SemaphoreType.DMA
    vmem = pl.BlockSpec(memory_space=pltpu.VMEM)
    return pl.pallas_call(
        front_kernel,
        out_shape=[
            jax.ShapeDtypeStruct((heads, size, width), F32),
            jax.ShapeDtypeStruct((heads, size, width), F32),
            jax.ShapeDtypeStruct((heads, width, width), F32),
        ],
        in_specs=[vmem] * 5,
        out_specs=[vmem] * 3,
        scratch_shapes=[
            pltpu.VMEM((size * pairs, width), F32),
            pltpu.VMEM((size * pairs, width), F32),
            pltpu.VMEM((size * heads, width), F32),
            pltpu.VMEM((2, heads, size), F32),
            pltpu.VMEM((2, size, heads), F32),
            pltpu.VMEM((heads, width, 2 * width), F32),
            pltpu.VMEM((heads, size, 2 * width), F32),
            pltpu.VMEM((8, width, 2 * width), F32),
            pltpu.VMEM((8, width, 2 * width), F32),
            pltpu.VMEM((width, 2 * width), F32),
            pltpu.VMEM((width, 2 * width), F32),
            pltpu.VMEM((8, width, width), F32),
            pltpu.VMEM((width, width), F32),
            pltpu.VMEM((width, width), F32),
            dma((8,)),
            dma((8,)),
            dma((2,)),
            dma((2,)),
            dma((2,)),
            dma,
            dma((8,)),
            dma((8,)),
        ],
        compiler_params=pltpu.CompilerParams(collective_id=0, has_side_effects=True),
        name="front",
    )(
        queries.reshape(size * pairs, width),
        key_vecs.reshape(size * pairs, width),
        values.reshape(size * heads, width),
        strength.T,
        decay_rate.T,
    )


def output_kernel(
    own_ref, reach_ref, state_ref, gain_ref, weight_hbm, out_ref,
    weight, flat, to_core, from_core, to_chip, from_chip, local,
    load_sem, send_core, recv_core, send_chip, recv_chip,
):
    heads, size, width = own_ref.shape
    rows = size // 4
    chunks, _, span = to_chip.shape
    me = lax.axis_index("heads")
    chip = me // 2
    core = me % 2
    other_core = {"heads": chip * 2 + 1 - core}
    other_chip = {"heads": (1 - chip) * 2 + core}

    load = pltpu.make_async_copy(weight_hbm, weight, load_sem)
    load.start()
    barrier = pltpu.get_barrier_semaphore()
    for target in (other_core, other_chip):
        pl.semaphore_signal(barrier, inc=1, device_id=target, device_id_type=pl.DeviceIdType.MESH)
    pl.semaphore_wait(barrier, 2)

    for head in range(heads):
        value = own_ref[head] + dot_split(split(reach_ref[head]), split(state_ref[head]))
        mean = jnp.mean(value * value, axis=1, keepdims=True)
        normed = value * lax.rsqrt(mean + norm_eps) * gain_ref[...]
        flat[:, head * width : (head + 1) * width] = normed.astype(BF16)
    load.wait()

    def rows_of(owner):
        return pl.ds(pl.multiple_of(owner * rows, rows), rows)

    def core_copy(c):
        return remote(
            to_core.at[c], from_core.at[c], send_core.at[c], recv_core.at[c], other_core
        )

    def chip_copy(c):
        return remote(
            to_chip.at[c], from_chip.at[c], send_chip.at[c], recv_chip.at[c], other_chip
        )

    far_mine = flat[rows_of((1 - chip) * 2 + core), :]
    far_theirs = flat[rows_of((1 - chip) * 2 + 1 - core), :]
    near_mine = flat[rows_of(me), :]
    near_theirs = flat[rows_of(chip * 2 + 1 - core), :]
    far = jnp.concatenate([far_theirs, far_mine], axis=0)
    near = jnp.concatenate([near_theirs, near_mine], axis=0)

    for c in range(chunks):
        part = dot(far, weight[:, c * span : (c + 1) * span])
        to_core[c] = part[:rows]
        core_copy(c).start()
        to_chip[c] = part[rows:]
    for c in range(chunks):
        core_copy(c).wait_recv()
        to_chip[c] = to_chip[c] + from_core[c]
        chip_copy(c).start()
    for c in range(chunks):
        part = dot(near, weight[:, c * span : (c + 1) * span])
        to_core[chunks + c] = part[:rows]
        core_copy(chunks + c).start()
        local[c] = part[rows:]
    for c in range(chunks):
        core_copy(chunks + c).wait_recv()
        local[c] = local[c] + from_core[chunks + c]
    for c in range(chunks):
        chip_copy(c).wait_recv()
        total = local[c] + from_chip[c]
        out_ref[:, c * span : (c + 1) * span] = total.astype(BF16)
    for c in range(chunks):
        core_copy(c).wait_send()
        core_copy(chunks + c).wait_send()
        chip_copy(c).wait_send()


def outputs(own, reach, states, norm_gain, w_out):
    heads, size, width = own.shape
    depth, model = w_out.shape
    chunks = 4
    span = model // chunks
    rows = size // 4
    dma = pltpu.SemaphoreType.DMA
    vmem = pl.BlockSpec(memory_space=pltpu.VMEM)
    return pl.pallas_call(
        output_kernel,
        out_shape=jax.ShapeDtypeStruct((rows, model), BF16),
        in_specs=[vmem, vmem, vmem, vmem, pl.BlockSpec(memory_space=pl.ANY)],
        out_specs=vmem,
        scratch_shapes=[
            pltpu.VMEM((depth, model), BF16),
            pltpu.VMEM((size, depth), BF16),
            pltpu.VMEM((2 * chunks, rows, span), F32),
            pltpu.VMEM((2 * chunks, rows, span), F32),
            pltpu.VMEM((chunks, rows, span), F32),
            pltpu.VMEM((chunks, rows, span), F32),
            pltpu.VMEM((chunks, rows, span), F32),
            dma,
            dma((2 * chunks,)),
            dma((2 * chunks,)),
            dma((chunks,)),
            dma((chunks,)),
        ],
        compiler_params=pltpu.CompilerParams(collective_id=1, has_side_effects=True),
        name="outputs",
    )(own, reach, states, norm_gain.reshape(1, width), w_out)


def body(queries, key_vecs, values, strength, decay_rate, norm_gain, w_out):
    own, reach, states = front(queries, key_vecs, values, strength, decay_rate)
    return outputs(own, reach, states, norm_gain, w_out)


def solution(mesh):
    finer = Mesh(
        mesh.devices.reshape(4, 4, 4, mesh.shape["heads"]), ("seq_0", "seq_1", "seq_2", "heads")
    )
    placed = (
        P(SEQ, "heads", None),
        P(SEQ, "heads", None),
        P(SEQ, "heads", None),
        P(SEQ, "heads"),
        P(SEQ, "heads"),
        P(),
        P("heads", None),
    )
    return jax.shard_map(
        body, mesh=finer, in_specs=placed, out_specs=P(SEQ_HEADS, None), check_vma=False
    )
```

```python
import jax
import jax.numpy as jnp
from jax import lax
from jax.experimental import pallas as pl
from jax.experimental.pallas import tpu as pltpu
from jax.sharding import Mesh
from jax.sharding import PartitionSpec as P

SEQ = ("seq_0", "seq_1", "seq_2")
SEQ_HEADS = ("seq_0", "seq_1", "seq_2", "heads")
F32 = jnp.float32
BF16 = jnp.bfloat16
HIGHEST = lax.Precision.HIGHEST
norm_eps = 1e-12
unit_eps = 1e-06

NN = (((1,), (0,)), ((), ()))
NT = (((1,), (1,)), ((), ()))
TN = (((0,), (0,)), ((), ()))


def dot(a, b, dims=NN):
    return lax.dot_general(a, b, dims, preferred_element_type=F32)


def split(x):
    high = x.astype(BF16)
    low = (x - high.astype(F32)).astype(BF16)
    return high, low


def dot_split(a, b, dims=NN):
    return dot(a[0], b[0], dims) + (dot(a[0], b[1], dims) + dot(a[1], b[0], dims))


def spread(part):
    half = part.shape[0]
    zero = jnp.zeros((half, half), part.dtype)
    top = jnp.concatenate([part[:, :half], zero], axis=1)
    bottom = jnp.concatenate([zero, part[:, half:]], axis=1)
    return jnp.concatenate([top, bottom], axis=0)


def unit_lower_inverses(lowers, row, col):
    size = row.shape[0]
    half = size // 2
    r = row[:half, :]
    c = col[:half, :] % half
    base = 8
    unit = jnp.where(r == c, 1.0, 0.0)
    compact = [jnp.concatenate([x[:half, :half], x[half:, half:]], axis=1) for x in lowers]
    diag = [jnp.where(r // base == c // base, x, 0.0) for x in compact]
    s1 = [x.astype(BF16) for x in diag]
    d2 = [dot(x, spread(x)) for x in s1]
    s2 = [x.astype(BF16) for x in d2]
    d3 = [dot(x, spread(y)) for x, y in zip(s1, s2)]
    d4 = [dot(x, spread(x)).astype(BF16) for x in s2]
    inv = [unit - x + y - z for x, y, z in zip(diag, d2, d3)]
    inv = [x + dot(x.astype(BF16), spread(y)) for x, y in zip(inv, d4)]
    width = base
    while width < half:
        across = (r // (2 * width) == c // (2 * width)) & (r // width != c // width)
        off = [jnp.where(across, x, 0.0).astype(BF16) for x in compact]
        si = [x.astype(BF16) for x in inv]
        step = [dot(x, spread(y)).astype(BF16) for x, y in zip(si, off)]
        inv = [x - dot(y, spread(z)) for x, y, z in zip(inv, step, si)]
        width *= 2
    si = [x.astype(BF16) for x in inv]
    parts = [split(x) for x in lowers]
    corner = [dot(x[:, half:], y[0][half:, :half]).astype(BF16) for x, y in zip(si, parts)]
    corner = [(-dot(x, y[:, :half])).astype(BF16) for x, y in zip(corner, si)]
    zero = jnp.zeros((half, half), BF16)
    rough = [
        jnp.concatenate(
            [
                jnp.concatenate([x[:, :half], zero], axis=1),
                jnp.concatenate([y, x[:, half:]], axis=1),
            ],
            axis=0,
        )
        for x, y in zip(si, corner)
    ]
    eye = jnp.where(row == col, 1.0, 0.0)
    residual = [
        (eye - x.astype(F32)) - (dot(y[0], x) + dot(y[1], x)) for x, y in zip(rough, parts)
    ]
    short = [x.astype(BF16) for x in residual]
    series = [(x + dot(y, y)).astype(BF16) for x, y in zip(residual, short)]
    return [x.astype(F32) + dot(x, y) for x, y in zip(rough, series)]


def column(table, head):
    lane = lax.broadcasted_iota(jnp.int32, table.shape, 1)
    return jnp.sum(jnp.where(lane == head, table, 0.0), axis=1, keepdims=True)


def unpack_inputs(q_ref, k_ref, v_ref, w_ref, d_ref, q32, k32, v32, rows, cols):
    q32[...] = q_ref[...].astype(F32)
    k32[...] = k_ref[...].astype(F32)
    v32[...] = v_ref[...].astype(F32)
    size = d_ref.shape[1]
    row = lax.broadcasted_iota(jnp.int32, (size, size), 0)
    col = lax.broadcasted_iota(jnp.int32, (size, size), 1)
    tri = jnp.where(row >= col, 1.0, 0.0).astype(F32)
    summed = lax.dot_general(d_ref[...], tri, NT, precision=HIGHEST, preferred_element_type=F32)
    rows[0] = -summed
    rows[1] = w_ref[...]
    cols[0] = rows[0].T
    cols[1] = rows[1].T


def key_parts(k32, pair, pairs, size):
    kf = k32[pl.ds(pair, size, stride=pairs), :]
    k2 = kf * kf
    rk_col = lax.rsqrt(jnp.sum(k2, axis=1, keepdims=True) + unit_eps)
    ones = jnp.ones((8, kf.shape[1]), BF16)
    high, low = split(k2)
    total = dot(ones, high, NT) + dot(ones, low, NT)
    rk_row = lax.rsqrt(total[0:1, :] + unit_eps)
    return kf, kf.astype(BF16), rk_col, rk_row


def decay_ratios(rows, cols, head):
    g_row = rows[0, pl.ds(head, 1), :]
    g_col = column(cols[0], head)
    return g_row, g_col, jnp.exp(jnp.minimum(g_col - g_row, 0.0))


def state_maps(chosen, k32, v32, rows, cols, maps_ref, solved_ref):
    heads, width, _ = maps_ref.shape
    size = rows.shape[2]
    pairs = k32.shape[0] // size
    group = heads // pairs
    row = lax.broadcasted_iota(jnp.int32, (size, size), 0)
    col = lax.broadcasted_iota(jnp.int32, (size, size), 1)
    eye_k = jnp.where(row[:width, :width] == col[:width, :width], 1.0, 0.0)
    keyed = [key_parts(k32, pair, pairs, size) for pair in chosen]
    dots = [dot(k, k, NT) * rk_col * rk_row for _, k, rk_col, rk_row in keyed]
    todo = [(pair * group + member, n) for n, pair in enumerate(chosen) for member in range(group)]
    lowers = []
    for head, n in todo:
        _, _, ratios = decay_ratios(rows, cols, head)
        lowers.append(jnp.where(row > col, column(cols[1], head) * ratios * dots[n], 0.0))
    inverses = unit_lower_inverses(lowers, row, col)
    scaled = [split(x * rows[1, pl.ds(head, 1), :]) for x, (head, _) in zip(inverses, todo)]
    tails = []
    for inv, (head, n) in zip(scaled, todo):
        kf, _, rk_col, _ = keyed[n]
        g_col = column(cols[0], head)
        keys = split(kf * (jnp.exp(g_col) * rk_col))
        v = v32[pl.ds(head, size, stride=heads), :].astype(BF16)
        right = jnp.concatenate([keys[0], v], axis=1)
        both = dot(inv[0], right) + dot(inv[1], right)
        on_keys = both[:, :width] + dot(inv[0], keys[1])
        solved = jnp.concatenate([on_keys, both[:, width:]], axis=1)
        solved_ref[head] = solved
        g_end = rows[0, pl.ds(head, 1), :][:, size - 1 : size]
        tails.append((g_end, split((jnp.exp(g_end - g_col) * rk_col) * solved)))
    turned = [kf.T.astype(BF16) for kf, _, _, _ in keyed]
    for (g_end, tail), (head, n) in zip(tails, todo):
        moved = dot(turned[n], tail[0]) + dot(turned[n], tail[1])
        maps_ref[head, :, :width] = jnp.exp(g_end) * eye_k - moved[:, :width]
        maps_ref[head, :, width:] = moved[:, width:]


def pair_outputs(pair, q32, k32, rows, cols, solved_ref, own_ref, reach_ref):
    heads, size, width = own_ref.shape
    pairs = k32.shape[0] // size
    group = heads // pairs
    row = lax.broadcasted_iota(jnp.int32, (size, size), 0)
    col = lax.broadcasted_iota(jnp.int32, (size, size), 1)
    kf, k, rk_col, rk_row = key_parts(k32, pair, pairs, size)
    qf = q32[pl.ds(pair, size, stride=pairs), :]
    rq_col = lax.rsqrt(jnp.sum(qf * qf, axis=1, keepdims=True) + unit_eps)
    query_dots = dot(qf.astype(BF16), k, NT) * rq_col * rk_row
    unit_q = qf * rq_col
    for member in range(group):
        head = pair * group + member
        g_row, g_col, ratios = decay_ratios(rows, cols, head)
        mixing = split(jnp.where(row >= col, ratios * query_dots, 0.0))
        mixed = dot_split(mixing, split(solved_ref[head]))
        reach_ref[head] = jnp.exp(g_col) * unit_q - mixed[:, :width]
        own_ref[head] = mixed[:, width:]


def remote(src, dst, send, recv, target):
    return pltpu.make_async_remote_copy(
        src_ref=src,
        dst_ref=dst,
        send_sem=send,
        recv_sem=recv,
        device_id=target,
        device_id_type=pl.DeviceIdType.MESH,
    )


def layer_kernel(
    q_ref, k_ref, v_ref, w_ref, d_ref, gain_ref, weight_hbm, out_ref,
    q32, k32, v32, rows, cols, maps_ref, solved_ref, own_ref, reach_ref,
    arrived, prefix, lower_map, plane, states, incoming, passing, entering,
    weight, flat, parts, from_core, to_chip, from_chip,
    send_maps, recv_maps, send_pair, recv_pair, send_chain, recv_chain, send_down, recv_down,
    load_sem, send_core, recv_core, send_chip, recv_chip,
):
    load = pltpu.make_async_copy(weight_hbm, weight, load_sem)
    load.start()
    width = maps_ref.shape[1]
    z = lax.axis_index("seq_0")
    x = lax.axis_index("seq_1")
    y = lax.axis_index("seq_2")
    upper = x // 2
    side = x % 2
    place = side * 4 + y
    mine = ((side + upper) % 2) * 4 + y
    mirror = 3 - x
    me = lax.axis_index("heads")
    chip = me // 2
    core = me % 2
    other_core = {"heads": chip * 2 + 1 - core}
    other_chip = {"heads": (1 - chip) * 2 + core}

    def peer(step):
        p = (place + step) % 8
        target = {"seq_1": upper * 2 + p // 4, "seq_2": p % 4}
        head = ((p // 4 + upper) % 2) * 4 + p % 4
        return p, target, head

    def beside(dz, at):
        return {"seq_0": (z + dz + 4) % 4, "seq_1": at}

    barrier = pltpu.get_barrier_semaphore()
    greeted = [peer(step)[1] for step in range(1, 8)]
    greeted += [{"seq_1": mirror}]
    greeted += [beside(dz, at) for dz in (1, -1) for at in (x, mirror)]
    greeted += [other_core, other_chip]
    for target in greeted:
        pl.semaphore_signal(barrier, inc=1, device_id=target, device_id_type=pl.DeviceIdType.MESH)

    unpack_inputs(q_ref, k_ref, v_ref, w_ref, d_ref, q32, k32, v32, rows, cols)

    def send_map(head):
        p = ((head // 4 + upper) % 2) * 4 + head % 4
        target = {"seq_1": upper * 2 + p // 4, "seq_2": p % 4}
        return remote(
            maps_ref.at[head], arrived.at[place], send_maps.at[head], recv_maps.at[place], target
        )

    def some_heads(step, carry):
        part = (mine // 4 + step) % 2
        state_maps([part * 2, part * 2 + 1], k32, v32, rows, cols, maps_ref, solved_ref)

        @pl.when(step == 1)
        def _():
            pl.semaphore_wait(barrier, len(greeted))

        for member in range(4):
            head = part * 4 + (mine + 1 + member) % 4

            @pl.when(head != mine)
            def _():
                send_map(head).start()

        return carry

    lax.fori_loop(1, 3, some_heads, 0)
    arrived[place] = maps_ref[mine]

    def one_output(pair, carry):
        pair_outputs(pair, q32, k32, rows, cols, solved_ref, own_ref, reach_ref)
        return carry

    lax.fori_loop(0, 4, one_output, 0)

    def wait_map(s):
        @pl.when(place != s)
        def _():
            remote(
                maps_ref.at[0], arrived.at[s], send_maps.at[0], recv_maps.at[s], {"seq_1": mirror}
            ).wait_recv()

    def then(later, running):
        moved = dot_split(split(later[:, :width]), split(running))
        return jnp.concatenate([moved[:, :width], moved[:, width:] + later[:, width:]], axis=1)

    wait_map(0)
    running = arrived[0]
    prefix[0] = running
    for s in range(1, 8):
        wait_map(s)
        running = then(arrived[s], running)
        prefix[s] = running

    pair = [
        remote(
            prefix.at[7, :, pl.ds(part * width, width)],
            lower_map.at[:, pl.ds(part * width, width)],
            send_pair.at[part],
            recv_pair.at[part],
            {"seq_1": mirror},
        )
        for part in (1, 0)
    ]
    chain = [
        remote(passing, incoming, send_chain.at[i], recv_chain, beside(1, at))
        for i, at in enumerate((x, mirror))
    ]

    @pl.when(upper == 0)
    def _():
        for copy in pair:
            copy.start()

    @pl.when(upper == 1)
    def _():
        pair[0].wait_recv()

    @pl.when((upper == 1) & (z == 0))
    def _():
        passing[...] = (
            dot_split(split(prefix[7, :, :width]), split(lower_map[:, width:]))
            + prefix[7, :, width:]
        )
        for copy in chain:
            copy.start()

    @pl.when(upper == 1)
    def _():
        pair[1].wait_recv()

    @pl.when((upper == 1) & (z > 0))
    def _():
        plane[...] = then(prefix[7], lower_map[...])

    @pl.when(z == 0)
    def _():
        incoming[...] = jnp.zeros_like(incoming)

    @pl.when(z > 0)
    def _():
        chain[0].wait_recv()

    before = split(incoming[...])

    @pl.when((upper == 1) & (z > 0) & (z < 3))
    def _():
        passing[...] = dot_split(split(plane[:, :width]), before) + plane[:, width:]
        for copy in chain:
            copy.start()

    @pl.when(upper == 0)
    def _():
        states[0] = incoming[...]

    @pl.when(upper == 1)
    def _():
        states[0] = dot_split(split(lower_map[:, :width]), before) + lower_map[:, width:]

    ahead = split(states[0])
    for s in range(1, 8):
        states[s] = dot_split(split(prefix[s - 1, :, :width]), ahead) + prefix[s - 1, :, width:]

    def send_state(step):
        p, target, head = peer(step)
        return remote(
            states.at[p], entering.at[mine], send_down.at[step], recv_down.at[mine], target
        )

    for step in range(1, 8):
        send_state(step).start()
    entering[mine] = states[place]
    for head in range(8):
        @pl.when(mine != head)
        def _():
            remote(
                states.at[0],
                entering.at[head],
                send_down.at[0],
                recv_down.at[head],
                {"seq_1": mirror},
            ).wait_recv()

    heads, size, _ = own_ref.shape
    half = size // 2
    quarter = size // 4
    chunks, _, span = to_chip.shape

    def emit(side):
        here = pl.ds(pl.multiple_of(side * half, half), half)
        entry = [split(entering[head]) for head in range(heads)]
        value = [
            own_ref[head, here, :] + dot_split(split(reach_ref[head, here, :]), entry[head])
            for head in range(heads)
        ]
        mean = [jnp.mean(x * x, axis=1, keepdims=True) for x in value]
        normed = [x * lax.rsqrt(m + norm_eps) * gain_ref[...] for x, m in zip(value, mean)]
        for head in range(heads):
            flat[:, head * width : (head + 1) * width] = normed[head].astype(BF16)

    def core_copy(way, c):
        return remote(
            parts.at[way, c, 1 - core],
            from_core.at[way, c],
            send_core.at[way, c],
            recv_core.at[way, c],
            other_core,
        )

    def chip_copy(c):
        return remote(
            to_chip.at[c], from_chip.at[c], send_chip.at[c], recv_chip.at[c], other_chip
        )

    def project(way):
        for c in range(chunks):
            part = dot(flat[...], weight[:, c * span : (c + 1) * span])
            parts[way, c, 0] = part[:quarter]
            parts[way, c, 1] = part[quarter:]
            core_copy(way, c).start()

    emit(1 - chip)
    load.wait()
    project(0)
    for c in range(chunks):
        core_copy(0, c).wait_recv()
        to_chip[c] = parts[0, c, core] + from_core[0, c]
        chip_copy(c).start()
    emit(chip)
    project(1)
    for c in range(chunks):
        core_copy(1, c).wait_recv()
    for c in range(chunks):
        chip_copy(c).wait_recv()
        total = parts[1, c, core] + from_core[1, c] + from_chip[c]
        out_ref[:, c * span : (c + 1) * span] = total.astype(BF16)

    for step in range(1, 8):
        p, target, head = peer(step)
        send_map(head).wait_send()
        send_state(step).wait_send()

    @pl.when(upper == 0)
    def _():
        for copy in pair:
            copy.wait_send()

    @pl.when((upper == 1) & (z < 3))
    def _():
        for copy in chain:
            copy.wait_send()

    for c in range(chunks):
        core_copy(0, c).wait_send()
        core_copy(1, c).wait_send()
        chip_copy(c).wait_send()


def body(queries, key_vecs, values, strength, decay_rate, norm_gain, w_out):
    size, pairs, width = queries.shape
    heads = values.shape[1]
    depth, model = w_out.shape
    chunks = 8
    span = model // chunks
    quarter = size // 4
    dma = pltpu.SemaphoreType.DMA
    vmem = pl.BlockSpec(memory_space=pltpu.VMEM)
    return pl.pallas_call(
        layer_kernel,
        out_shape=jax.ShapeDtypeStruct((quarter, model), BF16),
        in_specs=[vmem] * 6 + [pl.BlockSpec(memory_space=pl.ANY)],
        out_specs=vmem,
        scratch_shapes=[
            pltpu.VMEM((size * pairs, width), F32),
            pltpu.VMEM((size * pairs, width), F32),
            pltpu.VMEM((size * heads, width), F32),
            pltpu.VMEM((2, heads, size), F32),
            pltpu.VMEM((2, size, heads), F32),
            pltpu.VMEM((heads, width, 2 * width), F32),
            pltpu.VMEM((heads, size, 2 * width), F32),
            pltpu.VMEM((heads, size, width), F32),
            pltpu.VMEM((heads, size, width), F32),
            pltpu.VMEM((8, width, 2 * width), F32),
            pltpu.VMEM((8, width, 2 * width), F32),
            pltpu.VMEM((width, 2 * width), F32),
            pltpu.VMEM((width, 2 * width), F32),
            pltpu.VMEM((8, width, width), F32),
            pltpu.VMEM((width, width), F32),
            pltpu.VMEM((width, width), F32),
            pltpu.VMEM((heads, width, width), F32),
            pltpu.VMEM((depth, model), BF16),
            pltpu.VMEM((size // 2, depth), BF16),
            pltpu.VMEM((2, chunks, 2, quarter, span), F32),
            pltpu.VMEM((2, chunks, quarter, span), F32),
            pltpu.VMEM((chunks, quarter, span), F32),
            pltpu.VMEM((chunks, quarter, span), F32),
            dma((8,)),
            dma((8,)),
            dma((2,)),
            dma((2,)),
            dma((2,)),
            dma,
            dma((8,)),
            dma((8,)),
            dma,
            dma((2, chunks)),
            dma((2, chunks)),
            dma((chunks,)),
            dma((chunks,)),
        ],
        compiler_params=pltpu.CompilerParams(collective_id=0, has_side_effects=True),
        name="layer",
    )(
        queries.reshape(size * pairs, width),
        key_vecs.reshape(size * pairs, width),
        values.reshape(size * heads, width),
        strength.T,
        decay_rate.T,
        norm_gain.reshape(1, width),
        w_out,
    )


def solution(mesh):
    finer = Mesh(
        mesh.devices.reshape(4, 4, 4, mesh.shape["heads"]), ("seq_0", "seq_1", "seq_2", "heads")
    )
    placed = (
        P(SEQ, "heads", None),
        P(SEQ, "heads", None),
        P(SEQ, "heads", None),
        P(SEQ, "heads"),
        P(SEQ, "heads"),
        P(),
        P("heads", None),
    )
    return jax.shard_map(
        body, mesh=finer, in_specs=placed, out_specs=P(SEQ_HEADS, None), check_vma=False
    )
```

```python
import jax
import jax.numpy as jnp
from jax import lax
from jax.experimental import pallas as pl
from jax.experimental.pallas import tpu as pltpu
from jax.sharding import Mesh
from jax.sharding import PartitionSpec as P

SEQ = ("seq_0", "seq_1", "seq_2")
SEQ_HEADS = ("seq_0", "seq_1", "seq_2", "heads")
F32 = jnp.float32
BF16 = jnp.bfloat16
norm_eps = 1e-12
unit_eps = 1e-06

NN = (((1,), (0,)), ((), ()))
NT = (((1,), (1,)), ((), ()))
TN = (((0,), (0,)), ((), ()))


def dot(a, b, dims=NN):
    return lax.dot_general(a, b, dims, preferred_element_type=F32)


def split(x):
    high = x.astype(BF16)
    low = (x - high.astype(F32)).astype(BF16)
    return high, low


def dot_split(a, b, dims=NN):
    return dot(a[0], b[0], dims) + (dot(a[0], b[1], dims) + dot(a[1], b[0], dims))


def spread(part):
    half = part.shape[0]
    zero = jnp.zeros((half, half), part.dtype)
    top = jnp.concatenate([part[:, :half], zero], axis=1)
    bottom = jnp.concatenate([zero, part[:, half:]], axis=1)
    return jnp.concatenate([top, bottom], axis=0)


def unit_lower_inverses(lowers, row, col):
    size = row.shape[0]
    half = size // 2
    r = row[:half, :]
    c = col[:half, :] % half
    base = 8
    unit = jnp.where(r == c, 1.0, 0.0)
    compact = [jnp.concatenate([x[:half, :half], x[half:, half:]], axis=1) for x in lowers]
    diag = [jnp.where(r // base == c // base, x, 0.0) for x in compact]
    s1 = [x.astype(BF16) for x in diag]
    d2 = [dot(x, spread(x)) for x in s1]
    s2 = [x.astype(BF16) for x in d2]
    d3 = [dot(x, spread(y)) for x, y in zip(s1, s2)]
    d4 = [dot(x, spread(x)).astype(BF16) for x in s2]
    inv = [unit - x + y - z for x, y, z in zip(diag, d2, d3)]
    inv = [x + dot(x.astype(BF16), spread(y)) for x, y in zip(inv, d4)]
    width = base
    while width < half:
        across = (r // (2 * width) == c // (2 * width)) & (r // width != c // width)
        off = [jnp.where(across, x, 0.0).astype(BF16) for x in compact]
        si = [x.astype(BF16) for x in inv]
        step = [dot(x, spread(y)).astype(BF16) for x, y in zip(si, off)]
        inv = [x - dot(y, spread(z)) for x, y, z in zip(inv, step, si)]
        width *= 2
    si = [x.astype(BF16) for x in inv]
    parts = [split(x) for x in lowers]
    corner = [dot(x[:, half:], y[0][half:, :half]).astype(BF16) for x, y in zip(si, parts)]
    corner = [(-dot(x, y[:, :half])).astype(BF16) for x, y in zip(corner, si)]
    zero = jnp.zeros((half, half), BF16)
    rough = [
        jnp.concatenate(
            [
                jnp.concatenate([x[:, :half], zero], axis=1),
                jnp.concatenate([y, x[:, half:]], axis=1),
            ],
            axis=0,
        )
        for x, y in zip(si, corner)
    ]
    eye = jnp.where(row == col, 1.0, 0.0)
    residual = [
        (eye - x.astype(F32)) - (dot(y[0], x) + dot(y[1], x)) for x, y in zip(rough, parts)
    ]
    short = [x.astype(BF16) for x in residual]
    series = [(x + dot(y, y)).astype(BF16) for x, y in zip(residual, short)]
    return [x.astype(F32) + dot(x, y) for x, y in zip(rough, series)]


def column(table, head):
    lane = lax.broadcasted_iota(jnp.int32, table.shape, 1)
    return jnp.sum(jnp.where(lane == head, table, 0.0), axis=1, keepdims=True)


def unpack_inputs(k_ref, v_ref, w_ref, d_ref, k32, v32, rows, cols):
    k32[...] = k_ref[...].astype(F32)
    v32[...] = v_ref[...].astype(F32)
    size = d_ref.shape[1]
    row = lax.broadcasted_iota(jnp.int32, (size, size), 0)
    col = lax.broadcasted_iota(jnp.int32, (size, size), 1)
    tri = jnp.where(row <= col, 1.0, 0.0).astype(BF16)
    rest = d_ref[...]
    summed = jnp.zeros_like(rest)
    for _ in range(3):
        part = rest.astype(BF16)
        summed = summed + dot(part, tri)
        rest = rest - part.astype(F32)
    rows[0] = -summed
    rows[1] = w_ref[...]
    cols[0] = rows[0].T
    cols[1] = rows[1].T


def key_parts(k32, pair, pairs, size):
    kf = k32[pl.ds(pair, size, stride=pairs), :]
    k2 = kf * kf
    rk_col = lax.rsqrt(jnp.sum(k2, axis=1, keepdims=True) + unit_eps)
    ones = jnp.ones((8, kf.shape[1]), BF16)
    high, low = split(k2)
    total = dot(ones, high, NT) + dot(ones, low, NT)
    rk_row = lax.rsqrt(total[0:1, :] + unit_eps)
    return kf, kf.astype(BF16), rk_col, rk_row


def decay_ratios(rows, cols, head):
    g_row = rows[0, pl.ds(head, 1), :]
    g_col = column(cols[0], head)
    return g_row, g_col, jnp.exp(jnp.minimum(g_col - g_row, 0.0))


def state_maps(chosen, k32, v32, rows, cols, maps_ref, solved_ref):
    heads, width, _ = maps_ref.shape
    size = rows.shape[2]
    pairs = k32.shape[0] // size
    group = heads // pairs
    row = lax.broadcasted_iota(jnp.int32, (size, size), 0)
    col = lax.broadcasted_iota(jnp.int32, (size, size), 1)
    eye_k = jnp.where(row[:width, :width] == col[:width, :width], 1.0, 0.0)
    keyed = [key_parts(k32, pair, pairs, size) for pair in chosen]
    dots = [dot(k, k, NT) * rk_col * rk_row for _, k, rk_col, rk_row in keyed]
    todo = [(pair * group + member, n) for n, pair in enumerate(chosen) for member in range(group)]
    lowers = []
    for head, n in todo:
        _, _, ratios = decay_ratios(rows, cols, head)
        lowers.append(jnp.where(row > col, column(cols[1], head) * ratios * dots[n], 0.0))
    inverses = unit_lower_inverses(lowers, row, col)
    scaled = [split(x * rows[1, pl.ds(head, 1), :]) for x, (head, _) in zip(inverses, todo)]
    tails = []
    for inv, (head, n) in zip(scaled, todo):
        kf, _, rk_col, _ = keyed[n]
        g_col = column(cols[0], head)
        keys = split(kf * (jnp.exp(g_col) * rk_col))
        v = v32[pl.ds(head, size, stride=heads), :].astype(BF16)
        right = jnp.concatenate([keys[0], v], axis=1)
        both = dot(inv[0], right) + dot(inv[1], right)
        on_keys = both[:, :width] + dot(inv[0], keys[1])
        solved = jnp.concatenate([on_keys, both[:, width:]], axis=1)
        solved_ref[head] = solved
        g_end = rows[0, pl.ds(head, 1), :][:, size - 1 : size]
        tails.append((g_end, split((jnp.exp(g_end - g_col) * rk_col) * solved)))
    turned = [kf.T.astype(BF16) for kf, _, _, _ in keyed]
    for (g_end, tail), (head, n) in zip(tails, todo):
        moved = dot(turned[n], tail[0]) + dot(turned[n], tail[1])
        maps_ref[head, :, :width] = jnp.exp(g_end) * eye_k - moved[:, :width]
        maps_ref[head, :, width:] = moved[:, width:]


def pair_outputs(pair, q32, k32, rows, cols, solved_ref, own_ref, reach_ref):
    heads, size, width = own_ref.shape
    pairs = k32.shape[0] // size
    group = heads // pairs
    row = lax.broadcasted_iota(jnp.int32, (size, size), 0)
    col = lax.broadcasted_iota(jnp.int32, (size, size), 1)
    kf, k, rk_col, rk_row = key_parts(k32, pair, pairs, size)
    qf = q32[pl.ds(pair, size, stride=pairs), :]
    rq_col = lax.rsqrt(jnp.sum(qf * qf, axis=1, keepdims=True) + unit_eps)
    query_dots = dot(qf.astype(BF16), k, NT) * rq_col * rk_row
    unit_q = qf * rq_col
    for member in range(group):
        head = pair * group + member
        g_row, g_col, ratios = decay_ratios(rows, cols, head)
        mixing = split(jnp.where(row >= col, ratios * query_dots, 0.0))
        mixed = dot_split(mixing, split(solved_ref[head]))
        reach_ref[head] = jnp.exp(g_col) * unit_q - mixed[:, :width]
        own_ref[head] = mixed[:, width:]


def remote(src, dst, send, recv, target):
    return pltpu.make_async_remote_copy(
        src_ref=src,
        dst_ref=dst,
        send_sem=send,
        recv_sem=recv,
        device_id=target,
        device_id_type=pl.DeviceIdType.MESH,
    )


def layer_kernel(
    q_ref, k_ref, v_ref, w_ref, d_ref, gain_ref, weight_hbm, out_ref,
    q32, k32, v32, rows, cols, maps_ref, solved_ref, own_ref, reach_ref,
    arrived, prefix, lower_map, plane, lent, states, incoming, passing, entering,
    weight, flat, parts, from_core, to_chip, from_chip, result,
    send_maps, recv_maps, send_pair, recv_pair, send_chain, recv_chain, send_lent, recv_lent, send_down, recv_down,
    load_sem, send_core, recv_core, send_chip, recv_chip, store_sem,
):
    load = pltpu.make_async_copy(weight_hbm, weight, load_sem)
    load.start()
    width = maps_ref.shape[1]
    z = lax.axis_index("seq_0")
    x = lax.axis_index("seq_1")
    y = lax.axis_index("seq_2")
    upper = x // 2
    side = x % 2
    place = side * 4 + y
    mine = ((side + upper) % 2) * 4 + y
    mirror = 3 - x
    me = lax.axis_index("heads")
    chip = me // 2
    core = me % 2
    other_core = {"heads": chip * 2 + 1 - core}
    other_chip = {"heads": (1 - chip) * 2 + core}

    def peer(step):
        p = (place + step) % 8
        target = {"seq_1": upper * 2 + p // 4, "seq_2": p % 4}
        head = ((p // 4 + upper) % 2) * 4 + p % 4
        return p, target, head

    def beside(dz, at):
        return {"seq_0": (z + dz + 4) % 4, "seq_1": at}

    barrier = pltpu.get_barrier_semaphore()
    greeted = [peer(step)[1] for step in range(1, 8)]
    greeted += [{"seq_1": mirror}]
    greeted += [beside(dz, at) for dz in (1, -1) for at in (x, mirror)]
    greeted += [beside(2, x), other_core, other_chip]
    for target in greeted:
        pl.semaphore_signal(barrier, inc=1, device_id=target, device_id_type=pl.DeviceIdType.MESH)

    unpack_inputs(k_ref, v_ref, w_ref, d_ref, k32, v32, rows, cols)

    def send_map(head):
        p = ((head // 4 + upper) % 2) * 4 + head % 4
        target = {"seq_1": upper * 2 + p // 4, "seq_2": p % 4}
        return remote(
            maps_ref.at[head], arrived.at[place], send_maps.at[head], recv_maps.at[place], target
        )

    def some_heads(step, carry):
        part = (mine // 4 + step) % 2
        state_maps([part * 2, part * 2 + 1], k32, v32, rows, cols, maps_ref, solved_ref)

        @pl.when(step == 1)
        def _():
            pl.semaphore_wait(barrier, len(greeted))

        for member in range(4):
            head = part * 4 + (mine + 1 + member) % 4

            @pl.when(head != mine)
            def _():
                send_map(head).start()

        return carry

    lax.fori_loop(1, 3, some_heads, 0)
    arrived[place] = maps_ref[mine]

    q32[...] = q_ref[...].astype(F32)

    def one_output(pair, carry):
        pair_outputs(pair, q32, k32, rows, cols, solved_ref, own_ref, reach_ref)
        return carry

    lax.fori_loop(0, 4, one_output, 0)

    def wait_map(s):
        @pl.when(place != s)
        def _():
            remote(
                maps_ref.at[0], arrived.at[s], send_maps.at[0], recv_maps.at[s], {"seq_1": mirror}
            ).wait_recv()

    def then(later, running):
        moved = dot_split(split(later[:, :width]), split(running))
        return jnp.concatenate([moved[:, :width], moved[:, width:] + later[:, width:]], axis=1)

    pairs_of = []
    for s in range(0, 8, 2):
        wait_map(s)
        wait_map(s + 1)
        pairs_of.append(then(arrived[s + 1], arrived[s]))
    low_half = then(pairs_of[1], pairs_of[0])
    high_half = then(pairs_of[3], pairs_of[2])
    prefix[7] = then(high_half, low_half)
    prefix[1] = pairs_of[0]
    prefix[3] = low_half

    pair = [
        remote(
            prefix.at[7, :, pl.ds(part * width, width)],
            lower_map.at[:, pl.ds(part * width, width)],
            send_pair.at[part],
            recv_pair.at[part],
            {"seq_1": mirror},
        )
        for part in (1, 0)
    ]
    chain = [
        remote(passing, incoming, send_chain.at[i], recv_chain, beside(dz, at))
        for i, (dz, at) in enumerate(((1, x), (2, x), (1, mirror)))
    ]
    lend = remote(plane, lent, send_lent, recv_lent, beside(1, x))

    @pl.when(upper == 0)
    def _():
        for copy in pair:
            copy.start()

    def rest_of_prefixes():
        prefix[0] = arrived[0]
        prefix[2] = then(arrived[2], prefix[1])
        prefix[4] = then(arrived[4], prefix[3])
        prefix[5] = then(arrived[5], prefix[4])
        prefix[6] = then(arrived[6], prefix[5])

    rest_of_prefixes()

    @pl.when(upper == 1)
    def _():
        pair[0].wait_recv()

    @pl.when((upper == 1) & (z == 0))
    def _():
        passing[...] = (
            dot_split(split(prefix[7, :, :width]), split(lower_map[:, width:]))
            + prefix[7, :, width:]
        )
        chain[0].start()
        chain[2].start()

    @pl.when(upper == 1)
    def _():
        pair[1].wait_recv()

    @pl.when((upper == 1) & (z > 0))
    def _():
        plane[...] = then(prefix[7], lower_map[...])

    @pl.when((upper == 1) & (z == 2))
    def _():
        lend.start()

    @pl.when(z == 0)
    def _():
        incoming[...] = jnp.zeros_like(incoming)

    @pl.when(z > 0)
    def _():
        chain[0].wait_recv()

    @pl.when((upper == 1) & (z == 3))
    def _():
        lend.wait_recv()
        incoming[...] = (
            dot_split(split(lent[:, :width]), split(incoming[...])) + lent[:, width:]
        )

    before = split(incoming[...])

    @pl.when((upper == 1) & (z > 0) & (z < 3))
    def _():
        passing[...] = dot_split(split(plane[:, :width]), before) + plane[:, width:]

        @pl.when(z == 1)
        def _():
            chain[0].start()
            chain[1].start()

        chain[2].start()

    @pl.when(upper == 0)
    def _():
        states[0] = incoming[...]

    @pl.when(upper == 1)
    def _():
        states[0] = dot_split(split(lower_map[:, :width]), before) + lower_map[:, width:]

    ahead = split(states[0])
    for s in range(1, 8):
        states[s] = dot_split(split(prefix[s - 1, :, :width]), ahead) + prefix[s - 1, :, width:]

    def send_state(step):
        p, target, head = peer(step)
        return remote(
            states.at[p], entering.at[mine], send_down.at[step], recv_down.at[mine], target
        )

    for step in range(1, 8):
        send_state(step).start()
    entering[mine] = states[place]
    heads, size, _ = own_ref.shape
    half = size // 2
    quarter = size // 4
    chunks, _, span = to_chip.shape

    def emit(side, head):
        here = pl.ds(pl.multiple_of(side * half, half), half)
        value = own_ref[head, here, :] + dot_split(
            split(reach_ref[head, here, :]), split(entering[head])
        )
        mean = jnp.mean(value * value, axis=1, keepdims=True)
        normed = value * lax.rsqrt(mean + norm_eps) * gain_ref[...]
        flat[:, pl.ds(pl.multiple_of(head * width, width), width)] = normed.astype(BF16)

    def core_copy(way, c):
        return remote(
            parts.at[way, c, 1 - core],
            from_core.at[way, c],
            send_core.at[way, c],
            recv_core.at[way, c],
            other_core,
        )

    def chip_copy(c):
        return remote(
            to_chip.at[c], from_chip.at[c], send_chip.at[c], recv_chip.at[c], other_chip
        )

    def store_copy(c):
        return pltpu.make_async_copy(
            result.at[c], out_ref.at[:, pl.ds(c * span, span)], store_sem.at[c]
        )

    def project(way):
        for c in range(chunks):
            part = dot(flat[...], weight[:, c * span : (c + 1) * span])
            parts[way, c, 0] = part[:quarter]
            parts[way, c, 1] = part[quarter:]
            core_copy(way, c).start()

    emit(1 - chip, mine)
    for step in range(1, 8):
        p = (place + 8 - step) % 8
        head = ((p // 4 + upper) % 2) * 4 + p % 4
        remote(
            states.at[0], entering.at[head], send_down.at[0], recv_down.at[head], {"seq_1": mirror}
        ).wait_recv()
        emit(1 - chip, head)
    load.wait()
    project(0)
    for c in range(chunks):
        core_copy(0, c).wait_recv()
        to_chip[c] = parts[0, c, core] + from_core[0, c]
        chip_copy(c).start()
    for head in range(heads):
        emit(chip, head)
    project(1)
    for c in range(chunks):
        core_copy(1, c).wait_recv()
    for c in range(chunks):
        chip_copy(c).wait_recv()
        total = parts[1, c, core] + from_core[1, c] + from_chip[c]
        result[c] = total.astype(BF16)
        store_copy(c).start()

    for step in range(1, 8):
        p, target, head = peer(step)
        send_map(head).wait_send()
        send_state(step).wait_send()

    @pl.when(upper == 0)
    def _():
        for copy in pair:
            copy.wait_send()

    @pl.when((upper == 1) & (z < 3))
    def _():
        chain[2].wait_send()

        @pl.when(z < 2)
        def _():
            chain[0].wait_send()

        @pl.when(z == 1)
        def _():
            chain[1].wait_send()

        @pl.when(z == 2)
        def _():
            lend.wait_send()

    for c in range(chunks):
        core_copy(0, c).wait_send()
        core_copy(1, c).wait_send()
        chip_copy(c).wait_send()
        store_copy(c).wait()


def body(queries, key_vecs, values, strength, decay_rate, norm_gain, w_out):
    size, pairs, width = queries.shape
    heads = values.shape[1]
    depth, model = w_out.shape
    chunks = 8
    span = model // chunks
    quarter = size // 4
    dma = pltpu.SemaphoreType.DMA
    vmem = pl.BlockSpec(memory_space=pltpu.VMEM)
    return pl.pallas_call(
        layer_kernel,
        out_shape=jax.ShapeDtypeStruct((quarter, model), BF16),
        in_specs=[vmem] * 6 + [pl.BlockSpec(memory_space=pl.ANY)],
        out_specs=pl.BlockSpec(memory_space=pl.ANY),
        scratch_shapes=[
            pltpu.VMEM((size * pairs, width), F32),
            pltpu.VMEM((size * pairs, width), F32),
            pltpu.VMEM((size * heads, width), F32),
            pltpu.VMEM((2, heads, size), F32),
            pltpu.VMEM((2, size, heads), F32),
            pltpu.VMEM((heads, width, 2 * width), F32),
            pltpu.VMEM((heads, size, 2 * width), F32),
            pltpu.VMEM((heads, size, width), F32),
            pltpu.VMEM((heads, size, width), F32),
            pltpu.VMEM((8, width, 2 * width), F32),
            pltpu.VMEM((8, width, 2 * width), F32),
            pltpu.VMEM((width, 2 * width), F32),
            pltpu.VMEM((width, 2 * width), F32),
            pltpu.VMEM((width, 2 * width), F32),
            pltpu.VMEM((8, width, width), F32),
            pltpu.VMEM((width, width), F32),
            pltpu.VMEM((width, width), F32),
            pltpu.VMEM((heads, width, width), F32),
            pltpu.VMEM((depth, model), BF16),
            pltpu.VMEM((size // 2, depth), BF16),
            pltpu.VMEM((2, chunks, 2, quarter, span), F32),
            pltpu.VMEM((2, chunks, quarter, span), F32),
            pltpu.VMEM((chunks, quarter, span), F32),
            pltpu.VMEM((chunks, quarter, span), F32),
            pltpu.VMEM((chunks, quarter, span), BF16),
            dma((8,)),
            dma((8,)),
            dma((2,)),
            dma((2,)),
            dma((3,)),
            dma,
            dma,
            dma,
            dma((8,)),
            dma((8,)),
            dma,
            dma((2, chunks)),
            dma((2, chunks)),
            dma((chunks,)),
            dma((chunks,)),
            dma((chunks,)),
        ],
        compiler_params=pltpu.CompilerParams(collective_id=0, has_side_effects=True),
        name="layer",
    )(
        queries.reshape(size * pairs, width),
        key_vecs.reshape(size * pairs, width),
        values.reshape(size * heads, width),
        strength.T,
        decay_rate.T,
        norm_gain.reshape(1, width),
        w_out,
    )


def solution(mesh):
    finer = Mesh(
        mesh.devices.reshape(4, 4, 4, mesh.shape["heads"]), ("seq_0", "seq_1", "seq_2", "heads")
    )
    placed = (
        P(SEQ, "heads", None),
        P(SEQ, "heads", None),
        P(SEQ, "heads", None),
        P(SEQ, "heads"),
        P(SEQ, "heads"),
        P(),
        P("heads", None),
    )
    return jax.shard_map(
        body, mesh=finer, in_specs=placed, out_specs=P(SEQ_HEADS, None), check_vma=False
    )
```

```python
import jax
import jax.numpy as jnp
from jax import lax
from jax.experimental import pallas as pl
from jax.experimental.pallas import tpu as pltpu
from jax.sharding import Mesh
from jax.sharding import PartitionSpec as P

SEQ = ("seq_0", "seq_1", "seq_2")
SEQ_HEADS = ("seq_0", "seq_1", "seq_2", "heads")
F32 = jnp.float32
BF16 = jnp.bfloat16
norm_eps = 1e-12
unit_eps = 1e-06

NN = (((1,), (0,)), ((), ()))
NT = (((1,), (1,)), ((), ()))
TN = (((0,), (0,)), ((), ()))


def dot(a, b, dims=NN):
    return lax.dot_general(a, b, dims, preferred_element_type=F32)


def split(x):
    high = x.astype(BF16)
    low = (x - high.astype(F32)).astype(BF16)
    return high, low


def dot_split(a, b, dims=NN):
    return dot(a[0], b[0], dims) + (dot(a[0], b[1], dims) + dot(a[1], b[0], dims))


def spread(part):
    half = part.shape[0]
    zero = jnp.zeros((half, half), part.dtype)
    top = jnp.concatenate([part[:, :half], zero], axis=1)
    bottom = jnp.concatenate([zero, part[:, half:]], axis=1)
    return jnp.concatenate([top, bottom], axis=0)


def unit_lower_inverses(lowers, row, col):
    size = row.shape[0]
    half = size // 2
    r = row[:half, :]
    c = col[:half, :] % half
    base = 8
    unit = jnp.where(r == c, 1.0, 0.0)
    compact = [jnp.concatenate([x[:half, :half], x[half:, half:]], axis=1) for x in lowers]
    diag = [jnp.where(r // base == c // base, x, 0.0) for x in compact]
    s1 = [x.astype(BF16) for x in diag]
    d2 = [dot(x, spread(x)) for x in s1]
    s2 = [x.astype(BF16) for x in d2]
    d3 = [dot(x, spread(y)) for x, y in zip(s1, s2)]
    d4 = [dot(x, spread(x)).astype(BF16) for x in s2]
    inv = [unit - x + y - z for x, y, z in zip(diag, d2, d3)]
    inv = [x + dot(x.astype(BF16), spread(y)) for x, y in zip(inv, d4)]
    width = base
    while width < half:
        across = (r // (2 * width) == c // (2 * width)) & (r // width != c // width)
        off = [jnp.where(across, x, 0.0).astype(BF16) for x in compact]
        si = [x.astype(BF16) for x in inv]
        step = [dot(x, spread(y)).astype(BF16) for x, y in zip(si, off)]
        inv = [x - dot(y, spread(z)) for x, y, z in zip(inv, step, si)]
        width *= 2
    si = [x.astype(BF16) for x in inv]
    parts = [split(x) for x in lowers]
    corner = [dot(x[:, half:], y[0][half:, :half]).astype(BF16) for x, y in zip(si, parts)]
    corner = [(-dot(x, y[:, :half])).astype(BF16) for x, y in zip(corner, si)]
    zero = jnp.zeros((half, half), BF16)
    rough = [
        jnp.concatenate(
            [
                jnp.concatenate([x[:, :half], zero], axis=1),
                jnp.concatenate([y, x[:, half:]], axis=1),
            ],
            axis=0,
        )
        for x, y in zip(si, corner)
    ]
    eye = jnp.where(row == col, 1.0, 0.0)
    residual = [
        (eye - x.astype(F32)) - (dot(y[0], x) + dot(y[1], x)) for x, y in zip(rough, parts)
    ]
    short = [x.astype(BF16) for x in residual]
    series = [(x + dot(y, y)).astype(BF16) for x, y in zip(residual, short)]
    return [x.astype(F32) + dot(x, y) for x, y in zip(rough, series)]


def column(table, head):
    lane = lax.broadcasted_iota(jnp.int32, table.shape, 1)
    return jnp.sum(jnp.where(lane == head, table, 0.0), axis=1, keepdims=True)


def unpack_inputs(k_ref, v_ref, w_ref, d_ref, k32, v32, rows, cols):
    k32[...] = k_ref[...].astype(F32)
    v32[...] = v_ref[...].astype(F32)
    size = d_ref.shape[1]
    row = lax.broadcasted_iota(jnp.int32, (size, size), 0)
    col = lax.broadcasted_iota(jnp.int32, (size, size), 1)
    tri = jnp.where(row <= col, 1.0, 0.0).astype(BF16)
    rest = d_ref[...]
    summed = jnp.zeros_like(rest)
    for _ in range(3):
        part = rest.astype(BF16)
        summed = summed + dot(part, tri)
        rest = rest - part.astype(F32)
    rows[0] = -summed
    rows[1] = w_ref[...]
    cols[0] = rows[0].T
    cols[1] = rows[1].T


def key_parts(k32, pair, pairs, size):
    kf = k32[pl.ds(pair, size, stride=pairs), :]
    k2 = kf * kf
    rk_col = lax.rsqrt(jnp.sum(k2, axis=1, keepdims=True) + unit_eps)
    ones = jnp.ones((8, kf.shape[1]), BF16)
    high, low = split(k2)
    total = dot(ones, high, NT) + dot(ones, low, NT)
    rk_row = lax.rsqrt(total[0:1, :] + unit_eps)
    return kf, kf.astype(BF16), rk_col, rk_row


def decay_ratios(rows, cols, head):
    g_row = rows[0, pl.ds(head, 1), :]
    g_col = column(cols[0], head)
    return g_row, g_col, jnp.exp(jnp.minimum(g_col - g_row, 0.0))


def state_maps(chosen, k32, v32, rows, cols, maps_ref, solved_ref):
    heads, width, _ = maps_ref.shape
    size = rows.shape[2]
    pairs = k32.shape[0] // size
    group = heads // pairs
    row = lax.broadcasted_iota(jnp.int32, (size, size), 0)
    col = lax.broadcasted_iota(jnp.int32, (size, size), 1)
    eye_k = jnp.where(row[:width, :width] == col[:width, :width], 1.0, 0.0)
    keyed = [key_parts(k32, pair, pairs, size) for pair in chosen]
    dots = [dot(k, k, NT) * rk_col * rk_row for _, k, rk_col, rk_row in keyed]
    todo = [(pair * group + member, n) for n, pair in enumerate(chosen) for member in range(group)]
    lowers = []
    for head, n in todo:
        _, _, ratios = decay_ratios(rows, cols, head)
        lowers.append(jnp.where(row > col, column(cols[1], head) * ratios * dots[n], 0.0))
    inverses = unit_lower_inverses(lowers, row, col)
    scaled = [split(x * rows[1, pl.ds(head, 1), :]) for x, (head, _) in zip(inverses, todo)]
    tails = []
    for inv, (head, n) in zip(scaled, todo):
        kf, _, rk_col, _ = keyed[n]
        g_col = column(cols[0], head)
        keys = split(kf * (jnp.exp(g_col) * rk_col))
        v = v32[pl.ds(head, size, stride=heads), :].astype(BF16)
        right = jnp.concatenate([keys[0], v], axis=1)
        both = dot(inv[0], right) + dot(inv[1], right)
        on_keys = both[:, :width] + dot(inv[0], keys[1])
        solved = jnp.concatenate([on_keys, both[:, width:]], axis=1)
        solved_ref[head] = solved
        g_end = rows[0, pl.ds(head, 1), :][:, size - 1 : size]
        tails.append((g_end, split((jnp.exp(g_end - g_col) * rk_col) * solved)))
    turned = [kf.T.astype(BF16) for kf, _, _, _ in keyed]
    for (g_end, tail), (head, n) in zip(tails, todo):
        moved = dot(turned[n], tail[0]) + dot(turned[n], tail[1])
        maps_ref[head, :, :width] = jnp.exp(g_end) * eye_k - moved[:, :width]
        maps_ref[head, :, width:] = moved[:, width:]


def pair_outputs(pair, q32, k32, rows, cols, solved_ref, own_ref, reach_ref):
    heads, size, width = own_ref.shape
    pairs = k32.shape[0] // size
    group = heads // pairs
    row = lax.broadcasted_iota(jnp.int32, (size, size), 0)
    col = lax.broadcasted_iota(jnp.int32, (size, size), 1)
    kf, k, rk_col, rk_row = key_parts(k32, pair, pairs, size)
    qf = q32[pl.ds(pair, size, stride=pairs), :]
    rq_col = lax.rsqrt(jnp.sum(qf * qf, axis=1, keepdims=True) + unit_eps)
    query_dots = dot(qf.astype(BF16), k, NT) * rq_col * rk_row
    unit_q = qf * rq_col
    for member in range(group):
        head = pair * group + member
        g_row, g_col, ratios = decay_ratios(rows, cols, head)
        mixing = split(jnp.where(row >= col, ratios * query_dots, 0.0))
        mixed = dot_split(mixing, split(solved_ref[head]))
        reach_ref[head] = jnp.exp(g_col) * unit_q - mixed[:, :width]
        own_ref[head] = mixed[:, width:]


def remote(src, dst, send, recv, target):
    return pltpu.make_async_remote_copy(
        src_ref=src,
        dst_ref=dst,
        send_sem=send,
        recv_sem=recv,
        device_id=target,
        device_id_type=pl.DeviceIdType.MESH,
    )


def layer_kernel(
    q_ref, k_ref, v_ref, w_ref, d_ref, gain_ref, weight_hbm, out_ref,
    q32, k32, v32, rows, cols, maps_ref, solved_ref, own_ref, reach_ref,
    arrived, prefix, lower_map, plane, lent, states, incoming, passing, entering,
    weight, flat, parts, from_core, to_chip, from_chip, result,
    send_maps, recv_maps, send_pair, recv_pair, send_chain, recv_chain, send_lent, recv_lent, send_down, recv_down,
    load_sem, send_core, recv_core, send_chip, recv_chip, store_sem,
):
    load = pltpu.make_async_copy(weight_hbm, weight, load_sem)
    load.start()
    width = maps_ref.shape[1]
    z = lax.axis_index("seq_0")
    x = lax.axis_index("seq_1")
    y = lax.axis_index("seq_2")
    upper = x // 2
    side = x % 2
    place = side * 4 + y
    mine = ((side + upper) % 2) * 4 + y
    mirror = 3 - x
    me = lax.axis_index("heads")
    chip = me // 2
    core = me % 2
    other_core = {"heads": chip * 2 + 1 - core}
    other_chip = {"heads": (1 - chip) * 2 + core}

    def peer(step):
        p = (place + step) % 8
        target = {"seq_1": upper * 2 + p // 4, "seq_2": p % 4}
        head = ((p // 4 + upper) % 2) * 4 + p % 4
        return p, target, head

    def beside(dz, at):
        return {"seq_0": (z + dz + 4) % 4, "seq_1": at}

    barrier = pltpu.get_barrier_semaphore()
    greeted = [peer(step)[1] for step in range(1, 8)]
    greeted += [{"seq_1": mirror}]
    greeted += [beside(dz, at) for dz in (1, -1) for at in (x, mirror)]
    greeted += [beside(2, x), other_core, other_chip]
    for target in greeted:
        pl.semaphore_signal(barrier, inc=1, device_id=target, device_id_type=pl.DeviceIdType.MESH)

    unpack_inputs(k_ref, v_ref, w_ref, d_ref, k32, v32, rows, cols)

    def send_map(head):
        p = ((head // 4 + upper) % 2) * 4 + head % 4
        target = {"seq_1": upper * 2 + p // 4, "seq_2": p % 4}
        return remote(
            maps_ref.at[head], arrived.at[place], send_maps.at[head], recv_maps.at[place], target
        )

    def some_heads(step, carry):
        part = (mine // 4 + step) % 2
        state_maps([part * 2, part * 2 + 1], k32, v32, rows, cols, maps_ref, solved_ref)

        @pl.when(step == 1)
        def _():
            pl.semaphore_wait(barrier, len(greeted))

        for member in range(4):
            head = part * 4 + (mine + 1 + member) % 4

            @pl.when(head != mine)
            def _():
                send_map(head).start()

        return carry

    lax.fori_loop(1, 3, some_heads, 0)
    arrived[place] = maps_ref[mine]

    q32[...] = q_ref[...].astype(F32)

    def one_output(pair, carry):
        pair_outputs(pair, q32, k32, rows, cols, solved_ref, own_ref, reach_ref)
        return carry

    lax.fori_loop(0, 4, one_output, 0)

    def wait_map(s):
        @pl.when(place != s)
        def _():
            remote(
                maps_ref.at[0], arrived.at[s], send_maps.at[0], recv_maps.at[s], {"seq_1": mirror}
            ).wait_recv()

    def then(later, running):
        moved = dot_split(split(later[:, :width]), split(running))
        return jnp.concatenate([moved[:, :width], moved[:, width:] + later[:, width:]], axis=1)

    pairs_of = []
    for s in range(0, 8, 2):
        wait_map(s)
        wait_map(s + 1)
        pairs_of.append(then(arrived[s + 1], arrived[s]))
    low_half = then(pairs_of[1], pairs_of[0])
    high_half = then(pairs_of[3], pairs_of[2])
    prefix[7] = then(high_half, low_half)
    prefix[1] = pairs_of[0]
    prefix[3] = low_half

    pair = [
        remote(
            prefix.at[7, :, pl.ds(part * width, width)],
            lower_map.at[:, pl.ds(part * width, width)],
            send_pair.at[part],
            recv_pair.at[part],
            {"seq_1": mirror},
        )
        for part in (1, 0)
    ]
    chain = [
        remote(passing, incoming, send_chain.at[i], recv_chain, beside(dz, at))
        for i, (dz, at) in enumerate(((1, x), (2, x), (1, mirror)))
    ]
    lend = remote(plane, lent, send_lent, recv_lent, beside(1, x))
    across = remote(passing, incoming, send_chain.at[0], recv_chain, {"seq_1": mirror})

    @pl.when(upper == 0)
    def _():
        for copy in pair:
            copy.start()

    def rest_of_prefixes():
        prefix[0] = arrived[0]
        prefix[2] = then(arrived[2], prefix[1])
        prefix[4] = then(arrived[4], prefix[3])
        prefix[5] = then(arrived[5], prefix[4])
        prefix[6] = then(arrived[6], prefix[5])

    rest_of_prefixes()

    @pl.when(upper == 1)
    def _():
        pair[0].wait_recv()

    @pl.when((upper == 1) & (z == 0))
    def _():
        passing[...] = (
            dot_split(split(prefix[7, :, :width]), split(lower_map[:, width:]))
            + prefix[7, :, width:]
        )
        chain[0].start()
        chain[2].start()

    @pl.when(upper == 1)
    def _():
        pair[1].wait_recv()

    @pl.when((upper == 1) & (z > 0) & (z < 3))
    def _():
        plane[...] = then(prefix[7], lower_map[...])

    @pl.when((upper == 1) & (z == 2))
    def _():
        lend.start()

    @pl.when(z == 0)
    def _():
        incoming[...] = jnp.zeros_like(incoming)

    @pl.when(z > 0)
    def _():
        chain[0].wait_recv()

    @pl.when((upper == 1) & (z == 3))
    def _():
        lend.wait_recv()
        passing[...] = (
            dot_split(split(lent[:, :width]), split(incoming[...])) + lent[:, width:]
        )
        across.start()
        incoming[...] = passing[...]

    before = split(incoming[...])

    @pl.when((upper == 1) & (z == 1))
    def _():
        passing[...] = dot_split(split(plane[:, :width]), before) + plane[:, width:]
        for copy in (chain[1], chain[0], chain[2]):
            copy.start()

    @pl.when(upper == 0)
    def _():
        states[0] = incoming[...]

    @pl.when(upper == 1)
    def _():
        states[0] = dot_split(split(lower_map[:, :width]), before) + lower_map[:, width:]

    ahead = split(states[0])
    for s in range(1, 8):
        states[s] = dot_split(split(prefix[s - 1, :, :width]), ahead) + prefix[s - 1, :, width:]

    def send_state(step):
        p, target, head = peer(step)
        return remote(
            states.at[p], entering.at[mine], send_down.at[step], recv_down.at[mine], target
        )

    for step in range(1, 8):
        send_state(step).start()
    entering[mine] = states[place]
    heads, size, _ = own_ref.shape
    half = size // 2
    quarter = size // 4
    chunks, _, span = to_chip.shape

    def emit(side):
        here = pl.ds(pl.multiple_of(side * half, half), half)
        value = [
            own_ref[head, here, :]
            + dot_split(split(reach_ref[head, here, :]), split(entering[head]))
            for head in range(heads)
        ]
        mean = [jnp.mean(x * x, axis=1, keepdims=True) for x in value]
        for head in range(heads):
            normed = value[head] * lax.rsqrt(mean[head] + norm_eps) * gain_ref[...]
            flat[:, head * width : (head + 1) * width] = normed.astype(BF16)

    def core_copy(way, c):
        return remote(
            parts.at[way, c, 1 - core],
            from_core.at[way, c],
            send_core.at[way, c],
            recv_core.at[way, c],
            other_core,
        )

    def chip_copy(c):
        return remote(
            to_chip.at[c], from_chip.at[c], send_chip.at[c], recv_chip.at[c], other_chip
        )

    def store_copy(c):
        return pltpu.make_async_copy(
            result.at[c], out_ref.at[:, pl.ds(c * span, span)], store_sem.at[c]
        )

    def project(way):
        for c in range(chunks):
            part = dot(flat[...], weight[:, c * span : (c + 1) * span])
            parts[way, c, 0] = part[:quarter]
            parts[way, c, 1] = part[quarter:]
            core_copy(way, c).start()

    for step in range(1, 8):
        p = (place + 8 - step) % 8
        head = ((p // 4 + upper) % 2) * 4 + p % 4
        remote(
            states.at[0], entering.at[head], send_down.at[0], recv_down.at[head], {"seq_1": mirror}
        ).wait_recv()
    emit(1 - chip)
    load.wait()
    project(0)
    for c in range(chunks):
        core_copy(0, c).wait_recv()
        to_chip[c] = parts[0, c, core] + from_core[0, c]
        chip_copy(c).start()
    emit(chip)
    project(1)
    for c in range(chunks):
        core_copy(1, c).wait_recv()
    for c in range(chunks):
        chip_copy(c).wait_recv()
        total = parts[1, c, core] + from_core[1, c] + from_chip[c]
        result[c] = total.astype(BF16)
        store_copy(c).start()

    for step in range(1, 8):
        p, target, head = peer(step)
        send_map(head).wait_send()
        send_state(step).wait_send()

    @pl.when(upper == 0)
    def _():
        for copy in pair:
            copy.wait_send()

    @pl.when((upper == 1) & (z < 2))
    def _():
        chain[0].wait_send()
        chain[2].wait_send()

    @pl.when((upper == 1) & (z == 1))
    def _():
        chain[1].wait_send()

    @pl.when((upper == 1) & (z == 2))
    def _():
        lend.wait_send()

    @pl.when((upper == 1) & (z == 3))
    def _():
        across.wait_send()

    for c in range(chunks):
        core_copy(0, c).wait_send()
        core_copy(1, c).wait_send()
        chip_copy(c).wait_send()
        store_copy(c).wait()


def body(queries, key_vecs, values, strength, decay_rate, norm_gain, w_out):
    size, pairs, width = queries.shape
    heads = values.shape[1]
    depth, model = w_out.shape
    chunks = 8
    span = model // chunks
    quarter = size // 4
    dma = pltpu.SemaphoreType.DMA
    vmem = pl.BlockSpec(memory_space=pltpu.VMEM)
    return pl.pallas_call(
        layer_kernel,
        out_shape=jax.ShapeDtypeStruct((quarter, model), BF16),
        in_specs=[vmem] * 6 + [pl.BlockSpec(memory_space=pl.ANY)],
        out_specs=pl.BlockSpec(memory_space=pl.ANY),
        scratch_shapes=[
            pltpu.VMEM((size * pairs, width), F32),
            pltpu.VMEM((size * pairs, width), F32),
            pltpu.VMEM((size * heads, width), F32),
            pltpu.VMEM((2, heads, size), F32),
            pltpu.VMEM((2, size, heads), F32),
            pltpu.VMEM((heads, width, 2 * width), F32),
            pltpu.VMEM((heads, size, 2 * width), F32),
            pltpu.VMEM((heads, size, width), F32),
            pltpu.VMEM((heads, size, width), F32),
            pltpu.VMEM((8, width, 2 * width), F32),
            pltpu.VMEM((8, width, 2 * width), F32),
            pltpu.VMEM((width, 2 * width), F32),
            pltpu.VMEM((width, 2 * width), F32),
            pltpu.VMEM((width, 2 * width), F32),
            pltpu.VMEM((8, width, width), F32),
            pltpu.VMEM((width, width), F32),
            pltpu.VMEM((width, width), F32),
            pltpu.VMEM((heads, width, width), F32),
            pltpu.VMEM((depth, model), BF16),
            pltpu.VMEM((size // 2, depth), BF16),
            pltpu.VMEM((2, chunks, 2, quarter, span), F32),
            pltpu.VMEM((2, chunks, quarter, span), F32),
            pltpu.VMEM((chunks, quarter, span), F32),
            pltpu.VMEM((chunks, quarter, span), F32),
            pltpu.VMEM((chunks, quarter, span), BF16),
            dma((8,)),
            dma((8,)),
            dma((2,)),
            dma((2,)),
            dma((3,)),
            dma,
            dma,
            dma,
            dma((8,)),
            dma((8,)),
            dma,
            dma((2, chunks)),
            dma((2, chunks)),
            dma((chunks,)),
            dma((chunks,)),
            dma((chunks,)),
        ],
        compiler_params=pltpu.CompilerParams(collective_id=0, has_side_effects=True),
        name="layer",
    )(
        queries.reshape(size * pairs, width),
        key_vecs.reshape(size * pairs, width),
        values.reshape(size * heads, width),
        strength.T,
        decay_rate.T,
        norm_gain.reshape(1, width),
        w_out,
    )


def solution(mesh):
    finer = Mesh(
        mesh.devices.reshape(4, 4, 4, mesh.shape["heads"]), ("seq_0", "seq_1", "seq_2", "heads")
    )
    placed = (
        P(SEQ, "heads", None),
        P(SEQ, "heads", None),
        P(SEQ, "heads", None),
        P(SEQ, "heads"),
        P(SEQ, "heads"),
        P(),
        P("heads", None),
    )
    return jax.shard_map(
        body, mesh=finer, in_specs=placed, out_specs=P(SEQ_HEADS, None), check_vma=False
    )
```

```python
import jax
import jax.numpy as jnp
from jax import lax
from jax.experimental import pallas as pl
from jax.experimental.pallas import tpu as pltpu
from jax.sharding import Mesh
from jax.sharding import PartitionSpec as P

SEQ = ("seq_0", "seq_1", "seq_2")
SEQ_HEADS = ("seq_0", "seq_1", "seq_2", "heads")
F32 = jnp.float32
BF16 = jnp.bfloat16
norm_eps = 1e-12
unit_eps = 1e-06

NN = (((1,), (0,)), ((), ()))
NT = (((1,), (1,)), ((), ()))
TN = (((0,), (0,)), ((), ()))


def dot(a, b, dims=NN):
    return lax.dot_general(a, b, dims, preferred_element_type=F32)


def split(x):
    high = x.astype(BF16)
    low = (x - high.astype(F32)).astype(BF16)
    return high, low


def dot_split(a, b, dims=NN):
    return dot(a[0], b[0], dims) + (dot(a[0], b[1], dims) + dot(a[1], b[0], dims))


def spread(part):
    half = part.shape[0]
    zero = jnp.zeros((half, half), part.dtype)
    top = jnp.concatenate([part[:, :half], zero], axis=1)
    bottom = jnp.concatenate([zero, part[:, half:]], axis=1)
    return jnp.concatenate([top, bottom], axis=0)


def unit_lower_inverses(lowers, row, col):
    size = row.shape[0]
    half = size // 2
    r = row[:half, :]
    c = col[:half, :] % half
    base = 8
    unit = jnp.where(r == c, 1.0, 0.0)
    compact = [jnp.concatenate([x[:half, :half], x[half:, half:]], axis=1) for x in lowers]
    diag = [jnp.where(r // base == c // base, x, 0.0) for x in compact]
    s1 = [x.astype(BF16) for x in diag]
    d2 = [dot(x, spread(x)) for x in s1]
    s2 = [x.astype(BF16) for x in d2]
    d3 = [dot(x, spread(y)) for x, y in zip(s1, s2)]
    d4 = [dot(x, spread(x)).astype(BF16) for x in s2]
    inv = [unit - x + y - z for x, y, z in zip(diag, d2, d3)]
    inv = [x + dot(x.astype(BF16), spread(y)) for x, y in zip(inv, d4)]
    width = base
    while width < half:
        across = (r // (2 * width) == c // (2 * width)) & (r // width != c // width)
        off = [jnp.where(across, x, 0.0).astype(BF16) for x in compact]
        si = [x.astype(BF16) for x in inv]
        step = [dot(x, spread(y)).astype(BF16) for x, y in zip(si, off)]
        inv = [x - dot(y, spread(z)) for x, y, z in zip(inv, step, si)]
        width *= 2
    si = [x.astype(BF16) for x in inv]
    parts = [split(x) for x in lowers]
    corner = [dot(x[:, half:], y[0][half:, :half]).astype(BF16) for x, y in zip(si, parts)]
    corner = [(-dot(x, y[:, :half])).astype(BF16) for x, y in zip(corner, si)]
    zero = jnp.zeros((half, half), BF16)
    rough = [
        jnp.concatenate(
            [
                jnp.concatenate([x[:, :half], zero], axis=1),
                jnp.concatenate([y, x[:, half:]], axis=1),
            ],
            axis=0,
        )
        for x, y in zip(si, corner)
    ]
    eye = jnp.where(row == col, 1.0, 0.0)
    residual = [
        (eye - x.astype(F32)) - (dot(y[0], x) + dot(y[1], x)) for x, y in zip(rough, parts)
    ]
    short = [x.astype(BF16) for x in residual]
    series = [(x + dot(y, y)).astype(BF16) for x, y in zip(residual, short)]
    return [x.astype(F32) + dot(x, y) for x, y in zip(rough, series)]


def column(table, head):
    lane = lax.broadcasted_iota(jnp.int32, table.shape, 1)
    return jnp.sum(jnp.where(lane == head, table, 0.0), axis=1, keepdims=True)


def unpack_inputs(k_ref, v_ref, w_ref, d_ref, k32, v32, rows, cols):
    k32[...] = k_ref[...].astype(F32)
    v32[...] = v_ref[...].astype(F32)
    size = d_ref.shape[1]
    row = lax.broadcasted_iota(jnp.int32, (size, size), 0)
    col = lax.broadcasted_iota(jnp.int32, (size, size), 1)
    tri = jnp.where(row <= col, 1.0, 0.0).astype(BF16)
    rest = d_ref[...]
    summed = jnp.zeros_like(rest)
    for _ in range(3):
        part = rest.astype(BF16)
        summed = summed + dot(part, tri)
        rest = rest - part.astype(F32)
    rows[0] = -summed
    rows[1] = w_ref[...]
    cols[0] = rows[0].T
    cols[1] = rows[1].T


def key_parts(k32, pair, pairs, size):
    kf = k32[pl.ds(pair, size, stride=pairs), :]
    k2 = kf * kf
    rk_col = lax.rsqrt(jnp.sum(k2, axis=1, keepdims=True) + unit_eps)
    ones = jnp.ones((8, kf.shape[1]), BF16)
    high, low = split(k2)
    total = dot(ones, high, NT) + dot(ones, low, NT)
    rk_row = lax.rsqrt(total[0:1, :] + unit_eps)
    return kf, kf.astype(BF16), rk_col, rk_row


def decay_ratios(rows, cols, head):
    g_row = rows[0, pl.ds(head, 1), :]
    g_col = column(cols[0], head)
    return g_row, g_col, jnp.exp(jnp.minimum(g_col - g_row, 0.0))


def state_maps(chosen, k32, v32, rows, cols, maps_ref, solved_ref):
    heads, width, _ = maps_ref.shape
    size = rows.shape[2]
    pairs = k32.shape[0] // size
    group = heads // pairs
    row = lax.broadcasted_iota(jnp.int32, (size, size), 0)
    col = lax.broadcasted_iota(jnp.int32, (size, size), 1)
    eye_k = jnp.where(row[:width, :width] == col[:width, :width], 1.0, 0.0)
    keyed = [key_parts(k32, pair, pairs, size) for pair in chosen]
    dots = [dot(k, k, NT) * rk_col * rk_row for _, k, rk_col, rk_row in keyed]
    todo = [(pair * group + member, n) for n, pair in enumerate(chosen) for member in range(group)]
    lowers = []
    for head, n in todo:
        _, _, ratios = decay_ratios(rows, cols, head)
        lowers.append(jnp.where(row > col, column(cols[1], head) * ratios * dots[n], 0.0))
    inverses = unit_lower_inverses(lowers, row, col)
    scaled = [split(x * rows[1, pl.ds(head, 1), :]) for x, (head, _) in zip(inverses, todo)]
    tails = []
    for inv, (head, n) in zip(scaled, todo):
        kf, _, rk_col, _ = keyed[n]
        g_col = column(cols[0], head)
        keys = split(kf * (jnp.exp(g_col) * rk_col))
        v = v32[pl.ds(head, size, stride=heads), :].astype(BF16)
        right = jnp.concatenate([keys[0], v], axis=1)
        both = dot(inv[0], right) + dot(inv[1], right)
        on_keys = both[:, :width] + dot(inv[0], keys[1])
        solved = jnp.concatenate([on_keys, both[:, width:]], axis=1)
        solved_ref[head] = solved
        g_end = rows[0, pl.ds(head, 1), :][:, size - 1 : size]
        tails.append((g_end, split((jnp.exp(g_end - g_col) * rk_col) * solved)))
    turned = [kf.T.astype(BF16) for kf, _, _, _ in keyed]
    for (g_end, tail), (head, n) in zip(tails, todo):
        moved = dot(turned[n], tail[0]) + dot(turned[n], tail[1])
        maps_ref[head, :, :width] = jnp.exp(g_end) * eye_k - moved[:, :width]
        maps_ref[head, :, width:] = moved[:, width:]


def pair_outputs(pair, q32, k32, rows, cols, solved_ref, own_ref, reach_ref):
    heads, size, width = own_ref.shape
    pairs = k32.shape[0] // size
    group = heads // pairs
    row = lax.broadcasted_iota(jnp.int32, (size, size), 0)
    col = lax.broadcasted_iota(jnp.int32, (size, size), 1)
    kf, k, rk_col, rk_row = key_parts(k32, pair, pairs, size)
    qf = q32[pl.ds(pair, size, stride=pairs), :]
    rq_col = lax.rsqrt(jnp.sum(qf * qf, axis=1, keepdims=True) + unit_eps)
    query_dots = dot(qf.astype(BF16), k, NT) * rq_col * rk_row
    unit_q = qf * rq_col
    for member in range(group):
        head = pair * group + member
        g_row, g_col, ratios = decay_ratios(rows, cols, head)
        mixing = split(jnp.where(row >= col, ratios * query_dots, 0.0))
        mixed = dot_split(mixing, split(solved_ref[head]))
        reach_ref[head] = jnp.exp(g_col) * unit_q - mixed[:, :width]
        own_ref[head] = mixed[:, width:]


def remote(src, dst, send, recv, target):
    return pltpu.make_async_remote_copy(
        src_ref=src,
        dst_ref=dst,
        send_sem=send,
        recv_sem=recv,
        device_id=target,
        device_id_type=pl.DeviceIdType.MESH,
    )


def layer_kernel(
    q_ref, k_ref, v_ref, w_ref, d_ref, gain_ref, weight_hbm, out_ref,
    q32, k32, v32, rows, cols, maps_ref, solved_ref, own_ref, reach_ref,
    arrived, prefix, lower_map, plane, lent, states, incoming, passing, entering,
    weight, flat, parts, from_core, to_chip, from_chip, result,
    send_maps, recv_maps, send_pair, recv_pair, send_chain, recv_chain, send_lent, recv_lent, send_down, recv_down,
    load_sem, send_core, recv_core, send_chip, recv_chip, store_sem,
):
    load = pltpu.make_async_copy(weight_hbm, weight, load_sem)
    load.start()
    width = maps_ref.shape[1]
    z = lax.axis_index("seq_0")
    x = lax.axis_index("seq_1")
    y = lax.axis_index("seq_2")
    upper = x // 2
    side = x % 2
    place = side * 4 + y
    mine = ((side + upper) % 2) * 4 + y
    mirror = 3 - x
    me = lax.axis_index("heads")
    chip = me // 2
    core = me % 2
    other_core = {"heads": chip * 2 + 1 - core}
    other_chip = {"heads": (1 - chip) * 2 + core}

    def peer(step):
        p = (place + step) % 8
        target = {"seq_1": upper * 2 + p // 4, "seq_2": p % 4}
        head = ((p // 4 + upper) % 2) * 4 + p % 4
        return p, target, head

    def beside(dz, at):
        return {"seq_0": (z + dz + 4) % 4, "seq_1": at}

    barrier = pltpu.get_barrier_semaphore()
    greeted = [peer(step)[1] for step in range(1, 8)]
    greeted += [{"seq_1": mirror}]
    greeted += [beside(dz, at) for dz in (1, -1) for at in (x, mirror)]
    greeted += [beside(2, x), other_core, other_chip]
    for target in greeted:
        pl.semaphore_signal(barrier, inc=1, device_id=target, device_id_type=pl.DeviceIdType.MESH)

    unpack_inputs(k_ref, v_ref, w_ref, d_ref, k32, v32, rows, cols)

    def send_map(head):
        p = ((head // 4 + upper) % 2) * 4 + head % 4
        target = {"seq_1": upper * 2 + p // 4, "seq_2": p % 4}
        return remote(
            maps_ref.at[head], arrived.at[place], send_maps.at[head], recv_maps.at[place], target
        )

    def some_heads(step, carry):
        part = (mine // 4 + step) % 2
        state_maps([part * 2, part * 2 + 1], k32, v32, rows, cols, maps_ref, solved_ref)

        @pl.when(step == 1)
        def _():
            pl.semaphore_wait(barrier, len(greeted))

        for member in range(4):
            head = part * 4 + (mine + 1 + member) % 4

            @pl.when(head != mine)
            def _():
                send_map(head).start()

        return carry

    lax.fori_loop(1, 3, some_heads, 0)
    arrived[place] = maps_ref[mine]

    q32[...] = q_ref[...].astype(F32)

    def one_output(pair, carry):
        pair_outputs(pair, q32, k32, rows, cols, solved_ref, own_ref, reach_ref)
        return carry

    lax.fori_loop(0, 4, one_output, 0)

    def wait_map(s):
        @pl.when(place != s)
        def _():
            remote(
                maps_ref.at[0], arrived.at[s], send_maps.at[0], recv_maps.at[s], {"seq_1": mirror}
            ).wait_recv()

    def then(later, running):
        moved = dot_split(split(later[:, :width]), split(running))
        return jnp.concatenate([moved[:, :width], moved[:, width:] + later[:, width:]], axis=1)

    pairs_of = []
    for s in range(0, 8, 2):
        wait_map(s)
        wait_map(s + 1)
        pairs_of.append(then(arrived[s + 1], arrived[s]))
    low_half = then(pairs_of[1], pairs_of[0])
    high_half = then(pairs_of[3], pairs_of[2])
    prefix[7] = then(high_half, low_half)
    prefix[1] = pairs_of[0]
    prefix[3] = low_half

    pair = [
        remote(
            prefix.at[7, :, pl.ds(part * width, width)],
            lower_map.at[:, pl.ds(part * width, width)],
            send_pair.at[part],
            recv_pair.at[part],
            {"seq_1": mirror},
        )
        for part in (1, 0)
    ]
    def pass_on(n, target):
        return [
            remote(
                passing.at[piece], incoming.at[piece], send_chain.at[n, i], recv_chain.at[i], target
            )
            for i, piece in enumerate(pieces)
        ]

    pieces = [pl.ds(i * (width // 2), width // 2) for i in range(2)]
    to_next = pass_on(0, beside(1, x))
    to_last = pass_on(1, beside(2, x))
    to_next_lower = pass_on(2, beside(1, mirror))
    across = pass_on(0, {"seq_1": mirror})
    lend = remote(plane, lent, send_lent, recv_lent, beside(1, x))

    def carry_over(total, copies):
        through = split(total[:, :width])
        offset = total[:, width:].T
        for i, piece in enumerate(pieces):
            to_next[i].wait_recv()
            passing[piece, :] = (
                dot_split(split(incoming[piece, :]), through, NT)
                + offset[i * (width // 2) : (i + 1) * (width // 2), :]
            )
            copies[i].start()

    @pl.when(upper == 0)
    def _():
        for copy in pair:
            copy.start()

    def rest_of_prefixes():
        prefix[0] = arrived[0]
        prefix[2] = then(arrived[2], prefix[1])
        prefix[4] = then(arrived[4], prefix[3])
        prefix[5] = then(arrived[5], prefix[4])
        prefix[6] = then(arrived[6], prefix[5])

    rest_of_prefixes()

    @pl.when(upper == 1)
    def _():
        pair[0].wait_recv()

    @pl.when((upper == 1) & (z == 0))
    def _():
        passing[...] = (
            dot_split(split(lower_map[:, width:].T), split(prefix[7, :, :width]), NT)
            + prefix[7, :, width:].T
        )
        for copy in to_next + to_next_lower:
            copy.start()

    @pl.when(upper == 1)
    def _():
        pair[1].wait_recv()

    @pl.when((upper == 1) & (z > 0) & (z < 3))
    def _():
        plane[...] = then(prefix[7], lower_map[...])

    @pl.when((upper == 1) & (z == 2))
    def _():
        lend.start()

    @pl.when(z == 0)
    def _():
        incoming[...] = jnp.zeros_like(incoming)

    @pl.when((z == 2) | ((upper == 0) & (z > 0)))
    def _():
        for copy in to_next:
            copy.wait_recv()

    @pl.when((upper == 1) & (z == 1))
    def _():
        carry_over(plane[...], to_last)
        for copy in to_next_lower + to_next:
            copy.start()

    @pl.when((upper == 1) & (z == 3))
    def _():
        lend.wait_recv()
        carry_over(lent[...], across)
        incoming[...] = passing[...]

    @pl.when(upper == 0)
    def _():
        states[0] = incoming[...].T

    @pl.when(upper == 1)
    def _():
        states[0] = (
            dot_split(split(lower_map[:, :width]), split(incoming[...]), NT) + lower_map[:, width:]
        )

    ahead = split(states[0])
    for s in range(1, 8):
        states[s] = dot_split(split(prefix[s - 1, :, :width]), ahead) + prefix[s - 1, :, width:]

    def send_state(step):
        p, target, head = peer(step)
        return remote(
            states.at[p], entering.at[mine], send_down.at[step], recv_down.at[mine], target
        )

    for step in range(1, 8):
        send_state(step).start()
    entering[mine] = states[place]
    heads, size, _ = own_ref.shape
    half = size // 2
    quarter = size // 4
    chunks, _, span = to_chip.shape

    def emit(side):
        here = pl.ds(pl.multiple_of(side * half, half), half)
        value = [
            own_ref[head, here, :]
            + dot_split(split(reach_ref[head, here, :]), split(entering[head]))
            for head in range(heads)
        ]
        mean = [jnp.mean(x * x, axis=1, keepdims=True) for x in value]
        for head in range(heads):
            normed = value[head] * lax.rsqrt(mean[head] + norm_eps) * gain_ref[...]
            flat[:, head * width : (head + 1) * width] = normed.astype(BF16)

    def core_copy(way, c):
        return remote(
            parts.at[way, c, 1 - core],
            from_core.at[way, c],
            send_core.at[way, c],
            recv_core.at[way, c],
            other_core,
        )

    def chip_copy(c):
        return remote(
            to_chip.at[c], from_chip.at[c], send_chip.at[c], recv_chip.at[c], other_chip
        )

    def store_copy(c):
        return pltpu.make_async_copy(
            result.at[c], out_ref.at[:, pl.ds(c * span, span)], store_sem.at[c]
        )

    def project(way):
        for c in range(chunks):
            part = dot(flat[...], weight[:, c * span : (c + 1) * span])
            parts[way, c, 0] = part[:quarter]
            parts[way, c, 1] = part[quarter:]
            core_copy(way, c).start()

    for step in range(1, 8):
        p = (place + 8 - step) % 8
        head = ((p // 4 + upper) % 2) * 4 + p % 4
        remote(
            states.at[0], entering.at[head], send_down.at[0], recv_down.at[head], {"seq_1": mirror}
        ).wait_recv()
    emit(1 - chip)
    load.wait()
    project(0)
    for c in range(chunks):
        core_copy(0, c).wait_recv()
        to_chip[c] = parts[0, c, core] + from_core[0, c]
        chip_copy(c).start()
    emit(chip)
    project(1)
    for c in range(chunks):
        core_copy(1, c).wait_recv()
    for c in range(chunks):
        chip_copy(c).wait_recv()
        total = parts[1, c, core] + from_core[1, c] + from_chip[c]
        result[c] = total.astype(BF16)
        store_copy(c).start()

    for step in range(1, 8):
        p, target, head = peer(step)
        send_map(head).wait_send()
        send_state(step).wait_send()

    @pl.when(upper == 0)
    def _():
        for copy in pair:
            copy.wait_send()

    @pl.when((upper == 1) & (z < 2))
    def _():
        for copy in to_next + to_next_lower:
            copy.wait_send()

    @pl.when((upper == 1) & (z == 1))
    def _():
        for copy in to_last:
            copy.wait_send()

    @pl.when((upper == 1) & (z == 2))
    def _():
        lend.wait_send()

    @pl.when((upper == 1) & (z == 3))
    def _():
        for copy in across:
            copy.wait_send()

    for c in range(chunks):
        core_copy(0, c).wait_send()
        core_copy(1, c).wait_send()
        chip_copy(c).wait_send()
        store_copy(c).wait()


def body(queries, key_vecs, values, strength, decay_rate, norm_gain, w_out):
    size, pairs, width = queries.shape
    heads = values.shape[1]
    depth, model = w_out.shape
    chunks = 8
    span = model // chunks
    quarter = size // 4
    dma = pltpu.SemaphoreType.DMA
    vmem = pl.BlockSpec(memory_space=pltpu.VMEM)
    return pl.pallas_call(
        layer_kernel,
        out_shape=jax.ShapeDtypeStruct((quarter, model), BF16),
        in_specs=[vmem] * 6 + [pl.BlockSpec(memory_space=pl.ANY)],
        out_specs=pl.BlockSpec(memory_space=pl.ANY),
        scratch_shapes=[
            pltpu.VMEM((size * pairs, width), F32),
            pltpu.VMEM((size * pairs, width), F32),
            pltpu.VMEM((size * heads, width), F32),
            pltpu.VMEM((2, heads, size), F32),
            pltpu.VMEM((2, size, heads), F32),
            pltpu.VMEM((heads, width, 2 * width), F32),
            pltpu.VMEM((heads, size, 2 * width), F32),
            pltpu.VMEM((heads, size, width), F32),
            pltpu.VMEM((heads, size, width), F32),
            pltpu.VMEM((8, width, 2 * width), F32),
            pltpu.VMEM((8, width, 2 * width), F32),
            pltpu.VMEM((width, 2 * width), F32),
            pltpu.VMEM((width, 2 * width), F32),
            pltpu.VMEM((width, 2 * width), F32),
            pltpu.VMEM((8, width, width), F32),
            pltpu.VMEM((width, width), F32),
            pltpu.VMEM((width, width), F32),
            pltpu.VMEM((heads, width, width), F32),
            pltpu.VMEM((depth, model), BF16),
            pltpu.VMEM((size // 2, depth), BF16),
            pltpu.VMEM((2, chunks, 2, quarter, span), F32),
            pltpu.VMEM((2, chunks, quarter, span), F32),
            pltpu.VMEM((chunks, quarter, span), F32),
            pltpu.VMEM((chunks, quarter, span), F32),
            pltpu.VMEM((chunks, quarter, span), BF16),
            dma((8,)),
            dma((8,)),
            dma((2,)),
            dma((2,)),
            dma((3, 2)),
            dma((2,)),
            dma,
            dma,
            dma((8,)),
            dma((8,)),
            dma,
            dma((2, chunks)),
            dma((2, chunks)),
            dma((chunks,)),
            dma((chunks,)),
            dma((chunks,)),
        ],
        compiler_params=pltpu.CompilerParams(collective_id=0, has_side_effects=True),
        name="layer",
    )(
        queries.reshape(size * pairs, width),
        key_vecs.reshape(size * pairs, width),
        values.reshape(size * heads, width),
        strength.T,
        decay_rate.T,
        norm_gain.reshape(1, width),
        w_out,
    )


def solution(mesh):
    finer = Mesh(
        mesh.devices.reshape(4, 4, 4, mesh.shape["heads"]), ("seq_0", "seq_1", "seq_2", "heads")
    )
    placed = (
        P(SEQ, "heads", None),
        P(SEQ, "heads", None),
        P(SEQ, "heads", None),
        P(SEQ, "heads"),
        P(SEQ, "heads"),
        P(),
        P("heads", None),
    )
    return jax.shard_map(
        body, mesh=finer, in_specs=placed, out_specs=P(SEQ_HEADS, None), check_vma=False
    )
```

```python
import jax
import jax.numpy as jnp
from jax import lax
from jax.experimental import pallas as pl
from jax.experimental.pallas import tpu as pltpu
from jax.sharding import Mesh
from jax.sharding import PartitionSpec as P

SEQ = ("seq_0", "seq_1", "seq_2")
SEQ_HEADS = ("seq_0", "seq_1", "seq_2", "heads")
F32 = jnp.float32
BF16 = jnp.bfloat16
norm_eps = 1e-12
unit_eps = 1e-06

NN = (((1,), (0,)), ((), ()))
NT = (((1,), (1,)), ((), ()))
TN = (((0,), (0,)), ((), ()))


def dot(a, b, dims=NN):
    return lax.dot_general(a, b, dims, preferred_element_type=F32)


def split(x):
    high = x.astype(BF16)
    low = (x - high.astype(F32)).astype(BF16)
    return high, low


def dot_split(a, b, dims=NN):
    return dot(a[0], b[0], dims) + (dot(a[0], b[1], dims) + dot(a[1], b[0], dims))


def spread(part):
    half = part.shape[0]
    zero = jnp.zeros((half, half), part.dtype)
    top = jnp.concatenate([part[:, :half], zero], axis=1)
    bottom = jnp.concatenate([zero, part[:, half:]], axis=1)
    return jnp.concatenate([top, bottom], axis=0)


def unit_lower_inverses(lowers, row, col):
    size = row.shape[0]
    half = size // 2
    r = row[:half, :]
    c = col[:half, :] % half
    base = 8
    unit = jnp.where(r == c, 1.0, 0.0)
    compact = [jnp.concatenate([x[:half, :half], x[half:, half:]], axis=1) for x in lowers]
    diag = [jnp.where(r // base == c // base, x, 0.0) for x in compact]
    s1 = [x.astype(BF16) for x in diag]
    d2 = [dot(x, spread(x)) for x in s1]
    s2 = [x.astype(BF16) for x in d2]
    d3 = [dot(x, spread(y)) for x, y in zip(s1, s2)]
    d4 = [dot(x, spread(x)).astype(BF16) for x in s2]
    inv = [unit - x + y - z for x, y, z in zip(diag, d2, d3)]
    inv = [x + dot(x.astype(BF16), spread(y)) for x, y in zip(inv, d4)]
    width = base
    while width < half:
        across = (r // (2 * width) == c // (2 * width)) & (r // width != c // width)
        off = [jnp.where(across, x, 0.0).astype(BF16) for x in compact]
        si = [x.astype(BF16) for x in inv]
        step = [dot(x, spread(y)).astype(BF16) for x, y in zip(si, off)]
        inv = [x - dot(y, spread(z)) for x, y, z in zip(inv, step, si)]
        width *= 2
    si = [x.astype(BF16) for x in inv]
    parts = [split(x) for x in lowers]
    corner = [dot(x[:, half:], y[0][half:, :half]).astype(BF16) for x, y in zip(si, parts)]
    corner = [(-dot(x, y[:, :half])).astype(BF16) for x, y in zip(corner, si)]
    zero = jnp.zeros((half, half), BF16)
    rough = [
        jnp.concatenate(
            [
                jnp.concatenate([x[:, :half], zero], axis=1),
                jnp.concatenate([y, x[:, half:]], axis=1),
            ],
            axis=0,
        )
        for x, y in zip(si, corner)
    ]
    eye = jnp.where(row == col, 1.0, 0.0)
    residual = [
        (eye - x.astype(F32)) - (dot(y[0], x) + dot(y[1], x)) for x, y in zip(rough, parts)
    ]
    short = [x.astype(BF16) for x in residual]
    series = [(x + dot(y, y)).astype(BF16) for x, y in zip(residual, short)]
    return [x.astype(F32) + dot(x, y) for x, y in zip(rough, series)]


def column(table, head):
    lane = lax.broadcasted_iota(jnp.int32, table.shape, 1)
    return jnp.sum(jnp.where(lane == head, table, 0.0), axis=1, keepdims=True)


def unpack_inputs(k_ref, v_ref, w_ref, d_ref, k32, v32, rows, cols):
    k32[...] = k_ref[...].astype(F32)
    v32[...] = v_ref[...].astype(F32)
    size = d_ref.shape[1]
    row = lax.broadcasted_iota(jnp.int32, (size, size), 0)
    col = lax.broadcasted_iota(jnp.int32, (size, size), 1)
    tri = jnp.where(row <= col, 1.0, 0.0).astype(BF16)
    rest = d_ref[...]
    summed = jnp.zeros_like(rest)
    for _ in range(3):
        part = rest.astype(BF16)
        summed = summed + dot(part, tri)
        rest = rest - part.astype(F32)
    rows[0] = -summed
    rows[1] = w_ref[...]
    cols[0] = rows[0].T
    cols[1] = rows[1].T


def key_parts(k32, pair, pairs, size):
    kf = k32[pl.ds(pair, size, stride=pairs), :]
    k2 = kf * kf
    rk_col = lax.rsqrt(jnp.sum(k2, axis=1, keepdims=True) + unit_eps)
    ones = jnp.ones((8, kf.shape[1]), BF16)
    high, low = split(k2)
    total = dot(ones, high, NT) + dot(ones, low, NT)
    rk_row = lax.rsqrt(total[0:1, :] + unit_eps)
    return kf, kf.astype(BF16), rk_col, rk_row


def decay_ratios(rows, cols, head):
    g_row = rows[0, pl.ds(head, 1), :]
    g_col = column(cols[0], head)
    return g_row, g_col, jnp.exp(jnp.minimum(g_col - g_row, 0.0))


def state_maps(chosen, k32, v32, rows, cols, maps_ref, solved_ref):
    heads, width, _ = maps_ref.shape
    size = rows.shape[2]
    pairs = k32.shape[0] // size
    group = heads // pairs
    row = lax.broadcasted_iota(jnp.int32, (size, size), 0)
    col = lax.broadcasted_iota(jnp.int32, (size, size), 1)
    eye_k = jnp.where(row[:width, :width] == col[:width, :width], 1.0, 0.0)
    keyed = [key_parts(k32, pair, pairs, size) for pair in chosen]
    dots = [dot(k, k, NT) * rk_col * rk_row for _, k, rk_col, rk_row in keyed]
    todo = [(pair * group + member, n) for n, pair in enumerate(chosen) for member in range(group)]
    lowers = []
    for head, n in todo:
        _, _, ratios = decay_ratios(rows, cols, head)
        lowers.append(jnp.where(row > col, column(cols[1], head) * ratios * dots[n], 0.0))
    inverses = unit_lower_inverses(lowers, row, col)
    scaled = [split(x * rows[1, pl.ds(head, 1), :]) for x, (head, _) in zip(inverses, todo)]
    tails = []
    for inv, (head, n) in zip(scaled, todo):
        kf, _, rk_col, _ = keyed[n]
        g_col = column(cols[0], head)
        keys = split(kf * (jnp.exp(g_col) * rk_col))
        v = v32[pl.ds(head, size, stride=heads), :].astype(BF16)
        right = jnp.concatenate([keys[0], v], axis=1)
        both = dot(inv[0], right) + dot(inv[1], right)
        on_keys = both[:, :width] + dot(inv[0], keys[1])
        solved = jnp.concatenate([on_keys, both[:, width:]], axis=1)
        solved_ref[head] = solved
        g_end = rows[0, pl.ds(head, 1), :][:, size - 1 : size]
        tails.append((g_end, split((jnp.exp(g_end - g_col) * rk_col) * solved)))
    turned = [kf.T.astype(BF16) for kf, _, _, _ in keyed]
    for (g_end, tail), (head, n) in zip(tails, todo):
        moved = dot(turned[n], tail[0]) + dot(turned[n], tail[1])
        maps_ref[head, :, :width] = jnp.exp(g_end) * eye_k - moved[:, :width]
        maps_ref[head, :, width:] = moved[:, width:]


def pair_outputs(pair, q32, k32, rows, cols, solved_ref, own_ref, reach_ref):
    heads, size, width = own_ref.shape
    pairs = k32.shape[0] // size
    group = heads // pairs
    row = lax.broadcasted_iota(jnp.int32, (size, size), 0)
    col = lax.broadcasted_iota(jnp.int32, (size, size), 1)
    kf, k, rk_col, rk_row = key_parts(k32, pair, pairs, size)
    qf = q32[pl.ds(pair, size, stride=pairs), :]
    rq_col = lax.rsqrt(jnp.sum(qf * qf, axis=1, keepdims=True) + unit_eps)
    query_dots = dot(qf.astype(BF16), k, NT) * rq_col * rk_row
    unit_q = qf * rq_col
    for member in range(group):
        head = pair * group + member
        g_row, g_col, ratios = decay_ratios(rows, cols, head)
        mixing = split(jnp.where(row >= col, ratios * query_dots, 0.0))
        mixed = dot_split(mixing, split(solved_ref[head]))
        reach_ref[head] = jnp.exp(g_col) * unit_q - mixed[:, :width]
        own_ref[head] = mixed[:, width:]


def remote(src, dst, send, recv, target):
    return pltpu.make_async_remote_copy(
        src_ref=src,
        dst_ref=dst,
        send_sem=send,
        recv_sem=recv,
        device_id=target,
        device_id_type=pl.DeviceIdType.MESH,
    )


def layer_kernel(
    q_ref, k_ref, v_ref, w_ref, d_ref, gain_ref, weight_hbm, out_ref,
    q32, k32, v32, rows, cols, maps_ref, solved_ref, own_ref, reach_ref,
    arrived, prefix, lower_map, plane, lent, states, incoming, passing, entering,
    weight, flat, parts, from_core, to_chip, from_chip, result,
    send_maps, recv_maps, send_pair, recv_pair, send_chain, recv_chain, send_lent, recv_lent, send_down, recv_down,
    load_sem, send_core, recv_core, send_chip, recv_chip, store_sem,
):
    load = pltpu.make_async_copy(weight_hbm, weight, load_sem)
    load.start()
    width = maps_ref.shape[1]
    z = lax.axis_index("seq_0")
    x = lax.axis_index("seq_1")
    y = lax.axis_index("seq_2")
    upper = x // 2
    side = x % 2
    place = side * 4 + y
    mine = ((side + upper) % 2) * 4 + y
    mirror = 3 - x
    me = lax.axis_index("heads")
    chip = me // 2
    core = me % 2
    other_core = {"heads": chip * 2 + 1 - core}
    other_chip = {"heads": (1 - chip) * 2 + core}

    def peer(step):
        p = (place + step) % 8
        target = {"seq_1": upper * 2 + p // 4, "seq_2": p % 4}
        head = ((p // 4 + upper) % 2) * 4 + p % 4
        return p, target, head

    def beside(dz, at):
        return {"seq_0": (z + dz + 4) % 4, "seq_1": at}

    barrier = pltpu.get_barrier_semaphore()
    greeted = [peer(step)[1] for step in range(1, 8)]
    greeted += [{"seq_1": mirror}]
    greeted += [beside(dz, at) for dz in (1, -1) for at in (x, mirror)]
    greeted += [beside(2, x), other_core, other_chip]
    for target in greeted:
        pl.semaphore_signal(barrier, inc=1, device_id=target, device_id_type=pl.DeviceIdType.MESH)

    unpack_inputs(k_ref, v_ref, w_ref, d_ref, k32, v32, rows, cols)

    def send_map(head):
        p = ((head // 4 + upper) % 2) * 4 + head % 4
        target = {"seq_1": upper * 2 + p // 4, "seq_2": p % 4}
        return remote(
            maps_ref.at[head], arrived.at[place], send_maps.at[head], recv_maps.at[place], target
        )

    def some_heads(step, carry):
        part = (mine // 4 + step) % 2
        state_maps([part * 2, part * 2 + 1], k32, v32, rows, cols, maps_ref, solved_ref)

        @pl.when(step == 1)
        def _():
            pl.semaphore_wait(barrier, len(greeted))

        for member in range(4):
            head = part * 4 + (mine + 1 + member) % 4

            @pl.when(head != mine)
            def _():
                send_map(head).start()

        return carry

    lax.fori_loop(1, 3, some_heads, 0)
    arrived[place] = maps_ref[mine]

    q32[...] = q_ref[...].astype(F32)

    def one_output(pair, carry):
        pair_outputs(pair, q32, k32, rows, cols, solved_ref, own_ref, reach_ref)
        return carry

    lax.fori_loop(0, 4, one_output, 0)

    def wait_map(s):
        @pl.when(place != s)
        def _():
            remote(
                maps_ref.at[0], arrived.at[s], send_maps.at[0], recv_maps.at[s], {"seq_1": mirror}
            ).wait_recv()

    def then(later, running):
        moved = dot_split(split(later[:, :width]), split(running))
        return jnp.concatenate([moved[:, :width], moved[:, width:] + later[:, width:]], axis=1)

    for base in (side * 4, (1 - side) * 4):
        for i in range(4):
            wait_map(base + i)
        early = then(arrived[base + 1], arrived[base])
        late = then(arrived[base + 3], arrived[base + 2])
        prefix[base + 1] = early
        prefix[base + 3] = then(late, early)
    prefix[7] = then(prefix[7], prefix[3])

    pair = [
        remote(
            prefix.at[7, :, pl.ds(part * width, width)],
            lower_map.at[:, pl.ds(part * width, width)],
            send_pair.at[part],
            recv_pair.at[part],
            {"seq_1": mirror},
        )
        for part in (1, 0)
    ]
    def pass_on(n, target):
        return [
            remote(
                passing.at[piece], incoming.at[piece], send_chain.at[n, i], recv_chain.at[i], target
            )
            for i, piece in enumerate(pieces)
        ]

    pieces = [pl.ds(i * (width // 2), width // 2) for i in range(2)]
    to_next = pass_on(0, beside(1, x))
    to_last = pass_on(1, beside(2, x))
    to_next_lower = pass_on(2, beside(1, mirror))
    across = pass_on(0, {"seq_1": mirror})
    lend = remote(plane, lent, send_lent, recv_lent, beside(1, x))

    def carry_over(total, copies):
        through = split(total[:, :width])
        offset = total[:, width:].T
        for i, piece in enumerate(pieces):
            to_next[i].wait_recv()
            passing[piece, :] = (
                dot_split(split(incoming[piece, :]), through, NT)
                + offset[i * (width // 2) : (i + 1) * (width // 2), :]
            )
            copies[i].start()

    @pl.when(upper == 0)
    def _():
        for copy in pair:
            copy.start()

    def rest_of_prefixes():
        prefix[0] = arrived[0]
        prefix[2] = then(arrived[2], prefix[1])
        prefix[4] = then(arrived[4], prefix[3])
        prefix[5] = then(prefix[5], prefix[3])
        prefix[6] = then(arrived[6], prefix[5])

    rest_of_prefixes()

    @pl.when(upper == 1)
    def _():
        pair[0].wait_recv()

    @pl.when((upper == 1) & (z == 0))
    def _():
        passing[...] = (
            dot_split(split(lower_map[:, width:].T), split(prefix[7, :, :width]), NT)
            + prefix[7, :, width:].T
        )
        for copy in to_next + to_next_lower:
            copy.start()

    @pl.when(upper == 1)
    def _():
        pair[1].wait_recv()

    @pl.when((upper == 1) & (z > 0) & (z < 3))
    def _():
        plane[...] = then(prefix[7], lower_map[...])

    @pl.when((upper == 1) & (z == 2))
    def _():
        lend.start()

    @pl.when(z == 0)
    def _():
        incoming[...] = jnp.zeros_like(incoming)

    @pl.when((z == 2) | ((upper == 0) & (z > 0)))
    def _():
        for copy in to_next:
            copy.wait_recv()

    @pl.when((upper == 1) & (z == 1))
    def _():
        carry_over(plane[...], to_last)
        for copy in to_next_lower + to_next:
            copy.start()

    @pl.when((upper == 1) & (z == 3))
    def _():
        lend.wait_recv()
        carry_over(lent[...], across)
        incoming[...] = passing[...]

    @pl.when(upper == 0)
    def _():
        states[0] = incoming[...].T

    @pl.when(upper == 1)
    def _():
        states[0] = (
            dot_split(split(lower_map[:, :width]), split(incoming[...]), NT) + lower_map[:, width:]
        )

    ahead = split(states[0])
    for s in range(1, 8):
        states[s] = dot_split(split(prefix[s - 1, :, :width]), ahead) + prefix[s - 1, :, width:]

    def send_state(step):
        p, target, head = peer(step)
        return remote(
            states.at[p], entering.at[mine], send_down.at[step], recv_down.at[mine], target
        )

    for step in range(1, 8):
        send_state(step).start()
    entering[mine] = states[place]
    heads, size, _ = own_ref.shape
    half = size // 2
    quarter = size // 4
    chunks, _, span = to_chip.shape

    def emit(side):
        here = pl.ds(pl.multiple_of(side * half, half), half)
        value = [
            own_ref[head, here, :]
            + dot_split(split(reach_ref[head, here, :]), split(entering[head]))
            for head in range(heads)
        ]
        mean = [jnp.mean(x * x, axis=1, keepdims=True) for x in value]
        for head in range(heads):
            normed = value[head] * lax.rsqrt(mean[head] + norm_eps) * gain_ref[...]
            flat[:, head * width : (head + 1) * width] = normed.astype(BF16)

    def core_copy(way, c):
        return remote(
            parts.at[way, c, 1 - core],
            from_core.at[way, c],
            send_core.at[way, c],
            recv_core.at[way, c],
            other_core,
        )

    def chip_copy(c):
        return remote(
            to_chip.at[c], from_chip.at[c], send_chip.at[c], recv_chip.at[c], other_chip
        )

    def store_copy(c):
        return pltpu.make_async_copy(
            result.at[c], out_ref.at[:, pl.ds(c * span, span)], store_sem.at[c]
        )

    def project(way):
        for c in range(chunks):
            part = dot(flat[...], weight[:, c * span : (c + 1) * span])
            parts[way, c, 0] = part[:quarter]
            parts[way, c, 1] = part[quarter:]
            core_copy(way, c).start()

    for step in range(1, 8):
        p = (place + 8 - step) % 8
        head = ((p // 4 + upper) % 2) * 4 + p % 4
        remote(
            states.at[0], entering.at[head], send_down.at[0], recv_down.at[head], {"seq_1": mirror}
        ).wait_recv()
    emit(1 - chip)
    load.wait()
    project(0)
    for c in range(chunks):
        core_copy(0, c).wait_recv()
        to_chip[c] = parts[0, c, core] + from_core[0, c]
        chip_copy(c).start()
    emit(chip)
    project(1)
    for c in range(chunks):
        core_copy(1, c).wait_recv()
    for c in range(chunks):
        chip_copy(c).wait_recv()
        total = parts[1, c, core] + from_core[1, c] + from_chip[c]
        result[c] = total.astype(BF16)
        store_copy(c).start()

    for step in range(1, 8):
        p, target, head = peer(step)
        send_map(head).wait_send()
        send_state(step).wait_send()

    @pl.when(upper == 0)
    def _():
        for copy in pair:
            copy.wait_send()

    @pl.when((upper == 1) & (z < 2))
    def _():
        for copy in to_next + to_next_lower:
            copy.wait_send()

    @pl.when((upper == 1) & (z == 1))
    def _():
        for copy in to_last:
            copy.wait_send()

    @pl.when((upper == 1) & (z == 2))
    def _():
        lend.wait_send()

    @pl.when((upper == 1) & (z == 3))
    def _():
        for copy in across:
            copy.wait_send()

    for c in range(chunks):
        core_copy(0, c).wait_send()
        core_copy(1, c).wait_send()
        chip_copy(c).wait_send()
        store_copy(c).wait()


def body(queries, key_vecs, values, strength, decay_rate, norm_gain, w_out):
    size, pairs, width = queries.shape
    heads = values.shape[1]
    depth, model = w_out.shape
    chunks = 8
    span = model // chunks
    quarter = size // 4
    dma = pltpu.SemaphoreType.DMA
    vmem = pl.BlockSpec(memory_space=pltpu.VMEM)
    return pl.pallas_call(
        layer_kernel,
        out_shape=jax.ShapeDtypeStruct((quarter, model), BF16),
        in_specs=[vmem] * 6 + [pl.BlockSpec(memory_space=pl.ANY)],
        out_specs=pl.BlockSpec(memory_space=pl.ANY),
        scratch_shapes=[
            pltpu.VMEM((size * pairs, width), F32),
            pltpu.VMEM((size * pairs, width), F32),
            pltpu.VMEM((size * heads, width), F32),
            pltpu.VMEM((2, heads, size), F32),
            pltpu.VMEM((2, size, heads), F32),
            pltpu.VMEM((heads, width, 2 * width), F32),
            pltpu.VMEM((heads, size, 2 * width), F32),
            pltpu.VMEM((heads, size, width), F32),
            pltpu.VMEM((heads, size, width), F32),
            pltpu.VMEM((8, width, 2 * width), F32),
            pltpu.VMEM((8, width, 2 * width), F32),
            pltpu.VMEM((width, 2 * width), F32),
            pltpu.VMEM((width, 2 * width), F32),
            pltpu.VMEM((width, 2 * width), F32),
            pltpu.VMEM((8, width, width), F32),
            pltpu.VMEM((width, width), F32),
            pltpu.VMEM((width, width), F32),
            pltpu.VMEM((heads, width, width), F32),
            pltpu.VMEM((depth, model), BF16),
            pltpu.VMEM((size // 2, depth), BF16),
            pltpu.VMEM((2, chunks, 2, quarter, span), F32),
            pltpu.VMEM((2, chunks, quarter, span), F32),
            pltpu.VMEM((chunks, quarter, span), F32),
            pltpu.VMEM((chunks, quarter, span), F32),
            pltpu.VMEM((chunks, quarter, span), BF16),
            dma((8,)),
            dma((8,)),
            dma((2,)),
            dma((2,)),
            dma((3, 2)),
            dma((2,)),
            dma,
            dma,
            dma((8,)),
            dma((8,)),
            dma,
            dma((2, chunks)),
            dma((2, chunks)),
            dma((chunks,)),
            dma((chunks,)),
            dma((chunks,)),
        ],
        compiler_params=pltpu.CompilerParams(collective_id=0, has_side_effects=True),
        name="layer",
    )(
        queries.reshape(size * pairs, width),
        key_vecs.reshape(size * pairs, width),
        values.reshape(size * heads, width),
        strength.T,
        decay_rate.T,
        norm_gain.reshape(1, width),
        w_out,
    )


def solution(mesh):
    finer = Mesh(
        mesh.devices.reshape(4, 4, 4, mesh.shape["heads"]), ("seq_0", "seq_1", "seq_2", "heads")
    )
    placed = (
        P(SEQ, "heads", None),
        P(SEQ, "heads", None),
        P(SEQ, "heads", None),
        P(SEQ, "heads"),
        P(SEQ, "heads"),
        P(),
        P("heads", None),
    )
    return jax.shard_map(
        body, mesh=finer, in_specs=placed, out_specs=P(SEQ_HEADS, None), check_vma=False
    )
```

```python
import jax
import jax.numpy as jnp
from jax import lax
from jax.experimental import pallas as pl
from jax.experimental.pallas import tpu as pltpu
from jax.sharding import Mesh
from jax.sharding import PartitionSpec as P

SEQ = ("seq_0", "seq_1", "seq_2")
SEQ_HEADS = ("seq_0", "seq_1", "seq_2", "heads")
F32 = jnp.float32
BF16 = jnp.bfloat16
norm_eps = 1e-12
unit_eps = 1e-06

NN = (((1,), (0,)), ((), ()))
NT = (((1,), (1,)), ((), ()))
TN = (((0,), (0,)), ((), ()))


def dot(a, b, dims=NN):
    return lax.dot_general(a, b, dims, preferred_element_type=F32)


def split(x):
    high = x.astype(BF16)
    low = (x - high.astype(F32)).astype(BF16)
    return high, low


def dot_split(a, b, dims=NN):
    return dot(a[0], b[0], dims) + (dot(a[0], b[1], dims) + dot(a[1], b[0], dims))


def spread(part):
    half = part.shape[0]
    zero = jnp.zeros((half, half), part.dtype)
    top = jnp.concatenate([part[:, :half], zero], axis=1)
    bottom = jnp.concatenate([zero, part[:, half:]], axis=1)
    return jnp.concatenate([top, bottom], axis=0)


def unit_lower_inverses(lowers, row, col):
    size = row.shape[0]
    half = size // 2
    r = row[:half, :]
    c = col[:half, :] % half
    base = 8
    unit = jnp.where(r == c, 1.0, 0.0)
    compact = [jnp.concatenate([x[:half, :half], x[half:, half:]], axis=1) for x in lowers]
    diag = [jnp.where(r // base == c // base, x, 0.0) for x in compact]
    s1 = [x.astype(BF16) for x in diag]
    d2 = [dot(x, spread(x)) for x in s1]
    s2 = [x.astype(BF16) for x in d2]
    d3 = [dot(x, spread(y)) for x, y in zip(s1, s2)]
    d4 = [dot(x, spread(x)).astype(BF16) for x in s2]
    inv = [unit - x + y - z for x, y, z in zip(diag, d2, d3)]
    inv = [x + dot(x.astype(BF16), spread(y)) for x, y in zip(inv, d4)]
    width = base
    while width < half:
        across = (r // (2 * width) == c // (2 * width)) & (r // width != c // width)
        off = [jnp.where(across, x, 0.0).astype(BF16) for x in compact]
        si = [x.astype(BF16) for x in inv]
        step = [dot(x, spread(y)).astype(BF16) for x, y in zip(si, off)]
        inv = [x - dot(y, spread(z)) for x, y, z in zip(inv, step, si)]
        width *= 2
    si = [x.astype(BF16) for x in inv]
    parts = [split(x) for x in lowers]
    corner = [dot(x[:, half:], y[0][half:, :half]).astype(BF16) for x, y in zip(si, parts)]
    corner = [(-dot(x, y[:, :half])).astype(BF16) for x, y in zip(corner, si)]
    zero = jnp.zeros((half, half), BF16)
    rough = [
        jnp.concatenate(
            [
                jnp.concatenate([x[:, :half], zero], axis=1),
                jnp.concatenate([y, x[:, half:]], axis=1),
            ],
            axis=0,
        )
        for x, y in zip(si, corner)
    ]
    eye = jnp.where(row == col, 1.0, 0.0)
    residual = [
        (eye - x.astype(F32)) - (dot(y[0], x) + dot(y[1], x)) for x, y in zip(rough, parts)
    ]
    short = [x.astype(BF16) for x in residual]
    series = [(x + dot(y, y)).astype(BF16) for x, y in zip(residual, short)]
    return [x.astype(F32) + dot(x, y) for x, y in zip(rough, series)]


def column(table, head):
    lane = lax.broadcasted_iota(jnp.int32, table.shape, 1)
    return jnp.sum(jnp.where(lane == head, table, 0.0), axis=1, keepdims=True)


def unpack_inputs(k_ref, v_ref, w_ref, d_ref, k32, v32, rows, cols):
    k32[...] = k_ref[...].astype(F32)
    v32[...] = v_ref[...].astype(F32)
    size = d_ref.shape[1]
    row = lax.broadcasted_iota(jnp.int32, (size, size), 0)
    col = lax.broadcasted_iota(jnp.int32, (size, size), 1)
    tri = jnp.where(row <= col, 1.0, 0.0).astype(BF16)
    rest = d_ref[...]
    summed = jnp.zeros_like(rest)
    for _ in range(3):
        part = rest.astype(BF16)
        summed = summed + dot(part, tri)
        rest = rest - part.astype(F32)
    rows[0] = -summed
    rows[1] = w_ref[...]
    cols[0] = rows[0].T
    cols[1] = rows[1].T


def key_parts(k32, pair, pairs, size):
    kf = k32[pl.ds(pair, size, stride=pairs), :]
    k2 = kf * kf
    rk_col = lax.rsqrt(jnp.sum(k2, axis=1, keepdims=True) + unit_eps)
    ones = jnp.ones((8, kf.shape[1]), BF16)
    high, low = split(k2)
    total = dot(ones, high, NT) + dot(ones, low, NT)
    rk_row = lax.rsqrt(total[0:1, :] + unit_eps)
    return kf, kf.astype(BF16), rk_col, rk_row


def decay_ratios(rows, cols, head):
    g_row = rows[0, pl.ds(head, 1), :]
    g_col = column(cols[0], head)
    return g_row, g_col, jnp.exp(jnp.minimum(g_col - g_row, 0.0))


def state_maps(chosen, k32, v32, rows, cols, maps_ref, solved_ref):
    heads, width, _ = maps_ref.shape
    size = rows.shape[2]
    pairs = k32.shape[0] // size
    group = heads // pairs
    row = lax.broadcasted_iota(jnp.int32, (size, size), 0)
    col = lax.broadcasted_iota(jnp.int32, (size, size), 1)
    eye_k = jnp.where(row[:width, :width] == col[:width, :width], 1.0, 0.0)
    keyed = [key_parts(k32, pair, pairs, size) for pair in chosen]
    dots = [dot(k, k, NT) * rk_col * rk_row for _, k, rk_col, rk_row in keyed]
    todo = [(pair * group + member, n) for n, pair in enumerate(chosen) for member in range(group)]
    lowers = []
    for head, n in todo:
        _, _, ratios = decay_ratios(rows, cols, head)
        lowers.append(jnp.where(row > col, column(cols[1], head) * ratios * dots[n], 0.0))
    inverses = unit_lower_inverses(lowers, row, col)
    scaled = [split(x * rows[1, pl.ds(head, 1), :]) for x, (head, _) in zip(inverses, todo)]
    tails = []
    for inv, (head, n) in zip(scaled, todo):
        kf, _, rk_col, _ = keyed[n]
        g_col = column(cols[0], head)
        keys = split(kf * (jnp.exp(g_col) * rk_col))
        v = v32[pl.ds(head, size, stride=heads), :].astype(BF16)
        right = jnp.concatenate([keys[0], v], axis=1)
        both = dot(inv[0], right) + dot(inv[1], right)
        on_keys = both[:, :width] + dot(inv[0], keys[1])
        solved = jnp.concatenate([on_keys, both[:, width:]], axis=1)
        solved_ref[head] = solved
        g_end = rows[0, pl.ds(head, 1), :][:, size - 1 : size]
        tails.append((g_end, split((jnp.exp(g_end - g_col) * rk_col) * solved)))
    turned = [kf.T.astype(BF16) for kf, _, _, _ in keyed]
    for (g_end, tail), (head, n) in zip(tails, todo):
        moved = dot(turned[n], tail[0]) + dot(turned[n], tail[1])
        maps_ref[head, :, :width] = jnp.exp(g_end) * eye_k - moved[:, :width]
        maps_ref[head, :, width:] = moved[:, width:]


def pair_outputs(pair, q32, k32, rows, cols, solved_ref, own_ref, reach_ref):
    heads, size, width = own_ref.shape
    pairs = k32.shape[0] // size
    group = heads // pairs
    row = lax.broadcasted_iota(jnp.int32, (size, size), 0)
    col = lax.broadcasted_iota(jnp.int32, (size, size), 1)
    kf, k, rk_col, rk_row = key_parts(k32, pair, pairs, size)
    qf = q32[pl.ds(pair, size, stride=pairs), :]
    rq_col = lax.rsqrt(jnp.sum(qf * qf, axis=1, keepdims=True) + unit_eps)
    query_dots = dot(qf.astype(BF16), k, NT) * rq_col * rk_row
    unit_q = qf * rq_col
    for member in range(group):
        head = pair * group + member
        g_row, g_col, ratios = decay_ratios(rows, cols, head)
        mixing = split(jnp.where(row >= col, ratios * query_dots, 0.0))
        mixed = dot_split(mixing, split(solved_ref[head]))
        reach_ref[0, head], reach_ref[1, head] = split(jnp.exp(g_col) * unit_q - mixed[:, :width])
        own_ref[head] = mixed[:, width:]


def remote(src, dst, send, recv, target):
    return pltpu.make_async_remote_copy(
        src_ref=src,
        dst_ref=dst,
        send_sem=send,
        recv_sem=recv,
        device_id=target,
        device_id_type=pl.DeviceIdType.MESH,
    )


def layer_kernel(
    q_ref, k_ref, v_ref, w_ref, d_ref, gain_ref, weight_hbm, out_ref,
    q32, k32, v32, rows, cols, maps_ref, solved_ref, own_ref, reach_ref,
    arrived, prefix, through, lower_map, plane, lent, states, incoming, passing, entering,
    weight, flat, parts, from_core, to_chip, from_chip, result,
    send_maps, recv_maps, send_pair, recv_pair, send_chain, recv_chain, send_lent, recv_lent, send_down, recv_down,
    load_sem, send_core, recv_core, send_chip, recv_chip, store_sem,
):
    load = pltpu.make_async_copy(weight_hbm, weight, load_sem)
    load.start()
    width = maps_ref.shape[1]
    z = lax.axis_index("seq_0")
    x = lax.axis_index("seq_1")
    y = lax.axis_index("seq_2")
    upper = x // 2
    side = x % 2
    place = side * 4 + y
    mine = ((side + upper) % 2) * 4 + y
    mirror = 3 - x
    me = lax.axis_index("heads")
    chip = me // 2
    core = me % 2
    other_core = {"heads": chip * 2 + 1 - core}
    other_chip = {"heads": (1 - chip) * 2 + core}

    def peer(step):
        p = (place + step) % 8
        target = {"seq_1": upper * 2 + p // 4, "seq_2": p % 4}
        head = ((p // 4 + upper) % 2) * 4 + p % 4
        return p, target, head

    def beside(dz, at):
        return {"seq_0": (z + dz + 4) % 4, "seq_1": at}

    barrier = pltpu.get_barrier_semaphore()
    greeted = [peer(step)[1] for step in range(1, 8)]
    greeted += [{"seq_1": mirror}]
    greeted += [beside(dz, at) for dz in (1, -1) for at in (x, mirror)]
    greeted += [beside(2, x), other_core, other_chip]
    for target in greeted:
        pl.semaphore_signal(barrier, inc=1, device_id=target, device_id_type=pl.DeviceIdType.MESH)

    unpack_inputs(k_ref, v_ref, w_ref, d_ref, k32, v32, rows, cols)

    def send_map(head):
        p = ((head // 4 + upper) % 2) * 4 + head % 4
        target = {"seq_1": upper * 2 + p // 4, "seq_2": p % 4}
        return remote(
            maps_ref.at[head], arrived.at[place], send_maps.at[head], recv_maps.at[place], target
        )

    def some_heads(step, carry):
        part = (mine // 4 + step) % 2
        state_maps([part * 2, part * 2 + 1], k32, v32, rows, cols, maps_ref, solved_ref)

        @pl.when(step == 1)
        def _():
            pl.semaphore_wait(barrier, len(greeted))

        for member in range(4):
            head = part * 4 + (mine + 1 + member) % 4

            @pl.when(head != mine)
            def _():
                send_map(head).start()

        return carry

    lax.fori_loop(1, 3, some_heads, 0)
    arrived[place] = maps_ref[mine]

    q32[...] = q_ref[...].astype(F32)

    def one_output(pair, carry):
        pair_outputs(pair, q32, k32, rows, cols, solved_ref, own_ref, reach_ref)
        return carry

    lax.fori_loop(0, 4, one_output, 0)

    def wait_map(s):
        @pl.when(place != s)
        def _():
            remote(
                maps_ref.at[0], arrived.at[s], send_maps.at[0], recv_maps.at[s], {"seq_1": mirror}
            ).wait_recv()

    def then(later, running):
        moved = dot_split(split(later[:, :width]), split(running))
        return jnp.concatenate([moved[:, :width], moved[:, width:] + later[:, width:]], axis=1)

    pairs_of = []
    for s in range(0, 8, 2):
        wait_map(s)
        wait_map(s + 1)
        pairs_of.append(then(arrived[s + 1], arrived[s]))
    low_half = then(pairs_of[1], pairs_of[0])
    high_half = then(pairs_of[3], pairs_of[2])
    prefix[7] = then(high_half, low_half)
    prefix[1] = pairs_of[0]
    prefix[3] = low_half

    pair = [
        remote(
            prefix.at[7, :, pl.ds(part * width, width)],
            lower_map.at[:, pl.ds(part * width, width)],
            send_pair.at[part],
            recv_pair.at[part],
            {"seq_1": mirror},
        )
        for part in (1, 0)
    ]
    def pass_on(n, target):
        return [
            remote(
                passing.at[piece], incoming.at[piece], send_chain.at[n, i], recv_chain.at[i], target
            )
            for i, piece in enumerate(pieces)
        ]

    pieces = [pl.ds(i * (width // 2), width // 2) for i in range(2)]
    to_next = pass_on(0, beside(1, x))
    to_last = pass_on(1, beside(2, x))
    to_next_lower = pass_on(2, beside(1, mirror))
    across = pass_on(0, {"seq_1": mirror})
    lend = remote(plane, lent, send_lent, recv_lent, beside(1, x))

    def carry_over(total, copies):
        moving = split(total[:, :width])
        offset = total[:, width:].T
        for i, piece in enumerate(pieces):
            to_next[i].wait_recv()
            passing[piece, :] = (
                dot_split(split(incoming[piece, :]), moving, NT)
                + offset[i * (width // 2) : (i + 1) * (width // 2), :]
            )
            copies[i].start()

    @pl.when(upper == 0)
    def _():
        for copy in pair:
            copy.start()

    def rest_of_prefixes():
        prefix[0] = arrived[0]
        prefix[2] = then(arrived[2], prefix[1])
        prefix[4] = then(arrived[4], prefix[3])
        prefix[5] = then(arrived[5], prefix[4])
        prefix[6] = then(arrived[6], prefix[5])

    rest_of_prefixes()
    for s in range(7):
        through[0, s], through[1, s] = split(prefix[s, :, :width])

    @pl.when(upper == 1)
    def _():
        pair[0].wait_recv()

    @pl.when((upper == 1) & (z == 0))
    def _():
        passing[...] = (
            dot_split(split(lower_map[:, width:].T), split(prefix[7, :, :width]), NT)
            + prefix[7, :, width:].T
        )
        for copy in to_next + to_next_lower:
            copy.start()

    @pl.when(upper == 1)
    def _():
        pair[1].wait_recv()

    @pl.when((upper == 1) & (z > 0) & (z < 3))
    def _():
        plane[...] = then(prefix[7], lower_map[...])

    @pl.when((upper == 1) & (z == 2))
    def _():
        lend.start()

    @pl.when(z == 0)
    def _():
        incoming[...] = jnp.zeros_like(incoming)

    @pl.when((z == 2) | ((upper == 0) & (z > 0)))
    def _():
        for copy in to_next:
            copy.wait_recv()

    @pl.when((upper == 1) & (z == 1))
    def _():
        carry_over(plane[...], to_last)
        for copy in to_next_lower + to_next:
            copy.start()

    @pl.when((upper == 1) & (z == 3))
    def _():
        lend.wait_recv()
        carry_over(lent[...], across)
        incoming[...] = passing[...]

    @pl.when(upper == 0)
    def _():
        states[0] = incoming[...].T

    @pl.when(upper == 1)
    def _():
        states[0] = (
            dot_split(split(lower_map[:, :width]), split(incoming[...]), NT) + lower_map[:, width:]
        )

    ahead = split(states[0])
    for s in range(1, 8):
        states[s] = (
            dot_split((through[0, s - 1], through[1, s - 1]), ahead) + prefix[s - 1, :, width:]
        )

    def send_state(step):
        p, target, head = peer(step)
        return remote(
            states.at[p], entering.at[mine], send_down.at[step], recv_down.at[mine], target
        )

    for step in range(1, 8):
        send_state(step).start()
    entering[mine] = states[place]
    heads, size, _ = own_ref.shape
    half = size // 2
    quarter = size // 4
    chunks, _, span = to_chip.shape

    def emit(side):
        here = pl.ds(pl.multiple_of(side * half, half), half)
        value = [
            own_ref[head, here, :]
            + dot_split(
                (reach_ref[0, head, here, :], reach_ref[1, head, here, :]), split(entering[head])
            )
            for head in range(heads)
        ]
        mean = [jnp.mean(x * x, axis=1, keepdims=True) for x in value]
        for head in range(heads):
            normed = value[head] * lax.rsqrt(mean[head] + norm_eps) * gain_ref[...]
            flat[:, head * width : (head + 1) * width] = normed.astype(BF16)

    def core_copy(way, c):
        return remote(
            parts.at[way, c, 1 - core],
            from_core.at[way, c],
            send_core.at[way, c],
            recv_core.at[way, c],
            other_core,
        )

    def chip_copy(c):
        return remote(
            to_chip.at[c], from_chip.at[c], send_chip.at[c], recv_chip.at[c], other_chip
        )

    def store_copy(c):
        return pltpu.make_async_copy(
            result.at[c], out_ref.at[:, pl.ds(c * span, span)], store_sem.at[c]
        )

    def project(way):
        for c in range(chunks):
            part = dot(flat[...], weight[:, c * span : (c + 1) * span])
            parts[way, c, 0] = part[:quarter]
            parts[way, c, 1] = part[quarter:]
            core_copy(way, c).start()

    for step in range(1, 8):
        p = (place + 8 - step) % 8
        head = ((p // 4 + upper) % 2) * 4 + p % 4
        remote(
            states.at[0], entering.at[head], send_down.at[0], recv_down.at[head], {"seq_1": mirror}
        ).wait_recv()
    emit(1 - chip)
    load.wait()
    project(0)
    for c in range(chunks):
        core_copy(0, c).wait_recv()
        to_chip[c] = parts[0, c, core] + from_core[0, c]
        chip_copy(c).start()
    emit(chip)
    project(1)
    for c in range(chunks):
        core_copy(1, c).wait_recv()
    for c in range(chunks):
        chip_copy(c).wait_recv()
        total = parts[1, c, core] + from_core[1, c] + from_chip[c]
        result[c] = total.astype(BF16)
        store_copy(c).start()

    for step in range(1, 8):
        p, target, head = peer(step)
        send_map(head).wait_send()
        send_state(step).wait_send()

    @pl.when(upper == 0)
    def _():
        for copy in pair:
            copy.wait_send()

    @pl.when((upper == 1) & (z < 2))
    def _():
        for copy in to_next + to_next_lower:
            copy.wait_send()

    @pl.when((upper == 1) & (z == 1))
    def _():
        for copy in to_last:
            copy.wait_send()

    @pl.when((upper == 1) & (z == 2))
    def _():
        lend.wait_send()

    @pl.when((upper == 1) & (z == 3))
    def _():
        for copy in across:
            copy.wait_send()

    for c in range(chunks):
        core_copy(0, c).wait_send()
        core_copy(1, c).wait_send()
        chip_copy(c).wait_send()
        store_copy(c).wait()


def body(queries, key_vecs, values, strength, decay_rate, norm_gain, w_out):
    size, pairs, width = queries.shape
    heads = values.shape[1]
    depth, model = w_out.shape
    chunks = 8
    span = model // chunks
    quarter = size // 4
    dma = pltpu.SemaphoreType.DMA
    vmem = pl.BlockSpec(memory_space=pltpu.VMEM)
    return pl.pallas_call(
        layer_kernel,
        out_shape=jax.ShapeDtypeStruct((quarter, model), BF16),
        in_specs=[vmem] * 6 + [pl.BlockSpec(memory_space=pl.ANY)],
        out_specs=pl.BlockSpec(memory_space=pl.ANY),
        scratch_shapes=[
            pltpu.VMEM((size * pairs, width), F32),
            pltpu.VMEM((size * pairs, width), F32),
            pltpu.VMEM((size * heads, width), F32),
            pltpu.VMEM((2, heads, size), F32),
            pltpu.VMEM((2, size, heads), F32),
            pltpu.VMEM((heads, width, 2 * width), F32),
            pltpu.VMEM((heads, size, 2 * width), F32),
            pltpu.VMEM((heads, size, width), F32),
            pltpu.VMEM((2, heads, size, width), BF16),
            pltpu.VMEM((8, width, 2 * width), F32),
            pltpu.VMEM((8, width, 2 * width), F32),
            pltpu.VMEM((2, 7, width, width), BF16),
            pltpu.VMEM((width, 2 * width), F32),
            pltpu.VMEM((width, 2 * width), F32),
            pltpu.VMEM((width, 2 * width), F32),
            pltpu.VMEM((8, width, width), F32),
            pltpu.VMEM((width, width), F32),
            pltpu.VMEM((width, width), F32),
            pltpu.VMEM((heads, width, width), F32),
            pltpu.VMEM((depth, model), BF16),
            pltpu.VMEM((size // 2, depth), BF16),
            pltpu.VMEM((2, chunks, 2, quarter, span), F32),
            pltpu.VMEM((2, chunks, quarter, span), F32),
            pltpu.VMEM((chunks, quarter, span), F32),
            pltpu.VMEM((chunks, quarter, span), F32),
            pltpu.VMEM((chunks, quarter, span), BF16),
            dma((8,)),
            dma((8,)),
            dma((2,)),
            dma((2,)),
            dma((3, 2)),
            dma((2,)),
            dma,
            dma,
            dma((8,)),
            dma((8,)),
            dma,
            dma((2, chunks)),
            dma((2, chunks)),
            dma((chunks,)),
            dma((chunks,)),
            dma((chunks,)),
        ],
        compiler_params=pltpu.CompilerParams(collective_id=0, has_side_effects=True),
        name="layer",
    )(
        queries.reshape(size * pairs, width),
        key_vecs.reshape(size * pairs, width),
        values.reshape(size * heads, width),
        strength.T,
        decay_rate.T,
        norm_gain.reshape(1, width),
        w_out,
    )


def solution(mesh):
    finer = Mesh(
        mesh.devices.reshape(4, 4, 4, mesh.shape["heads"]), ("seq_0", "seq_1", "seq_2", "heads")
    )
    placed = (
        P(SEQ, "heads", None),
        P(SEQ, "heads", None),
        P(SEQ, "heads", None),
        P(SEQ, "heads"),
        P(SEQ, "heads"),
        P(),
        P("heads", None),
    )
    return jax.shard_map(
        body, mesh=finer, in_specs=placed, out_specs=P(SEQ_HEADS, None), check_vma=False
    )
```
